256 devices in a mesh: row: 8 (over x, core), col: 32 (over y, z).
Axes of the slice: x: 4, y: 4, z: 8, core: 2. Of those that a mesh axis runs over, the one named last changes fastest.
Arguments:
- velocity_start: float32 [2, 512, 4096], P(None, 'row', 'col'), may hold values from -3 to 3
- stress_start: float32 [3, 512, 4096], P(None, 'row', 'col'), may hold values from -3 to 3
- wind_stress: float32 [2, 512, 4096], P(None, 'row', 'col'), may hold values from -6 to 6
- ocean_current: float32 [2, 512, 4096], P(None, 'row', 'col'), may hold values from -3 to 3
- ice_area: float32 [5, 512, 4096], P(None, 'row', 'col'), may hold values from 0.15 to 0.2
- ice_volume: float32 [5, 512, 4096], P(None, 'row', 'col'), may hold values from 0.05 to 0.6
- inverse_width: float32 [512, 4096], P('row', 'col'), may hold values from 0.7 to 1.4
- inverse_height: float32 [512, 4096], P('row', 'col'), may hold values from 0.7 to 1.4
- land_block: int32 [128, 128], P('row', 'col'), may hold values 0 or 1
- ice_block: int32 [128, 128], P('row', 'col'), may hold values 0 or 1
- writer: int32 [32], replicated, may hold values from 0 to 7
Outputs:
- velocity: float32 [2, 512, 4096], P(None, 'row', 'col')
- stress: float32 [3, 512, 4096], P(None, 'row', 'col')
- restart: float32 [8, 10, 512, 4096], P('row', None, None, 'col')
The draws below stay inside these ranges and needn't reach their ends.
All inputs are finite; a program needn't handle non-finite values. No bound on the sum of `land_block` or of `ice_block` on one device may be relied on, other than what follows from the above.
Results may differ from the reference program's by a relative error of at most 0.00002.
Values sent between devices are 32-bit elements; how exact they have to be, the bound alone decides.
No kernel may reach another device: no remote copies, remote signals or barrier semaphores. Data moves between devices by JAX's collectives and lax.ppermute only.
A program may use at most 64 MiB of HBM per device.

```python
import math
import jax
import jax.numpy as jnp
from jax import lax

CX = 128
NCAT = 5
SUB = 12
NY = 512
NX = 4096
NBY = 128
NBX = 128
GROUPS = 32
SLOTS = 8


def place_ends(array, key, least, high):
    spot = [jax.random.randint(jax.random.fold_in(key, axis), (), 0, length) for axis, length in enumerate(array.shape)]
    longest = array.shape.index(max(array.shape))
    neighbour = spot[:longest] + [(spot[longest] + 1) % array.shape[longest]] + spot[longest + 1:]
    return array.at[tuple(spot)].set(least).at[tuple(neighbour)].set(high)


def block_scale(rng, extent, pieces, least, largest):
    gain, own = 1.0, jax.random.fold_in(rng, 6)
    for axis_at, shards_of in pieces:
        draws = jnp.exp(jax.random.uniform(jax.random.fold_in(own, axis_at), (shards_of,), jnp.float32, least / len(pieces), largest / len(pieces)))
        gain = gain * jnp.repeat(draws, extent[axis_at] // shards_of).reshape([-1 if axis == axis_at else 1 for axis in range(len(extent))])
    return gain


def centred(stream_key, shape, scale, reach, cuts=(), held_as=jnp.bfloat16):
    array = jax.random.normal(stream_key, shape, jnp.float32) * scale
    if len(cuts) > 0:
        array = block_scale(stream_key, shape, cuts, -0.22, 0.18) * array
    return jnp.clip(array, min=-reach, max=reach).astype(held_as)


def setup_inputs(seed: int = 0) -> dict:
    splits = jax.random.split(jax.random.key(seed), 12)
    velocity_start = centred(splits[0], (2, NY, NX), 0.5, 3.0, ((1, 8), (2, 32)), jnp.float32)
    stress_start = centred(splits[1], (3, NY, NX), 0.5, 3.0, ((1, 8), (2, 32)), jnp.float32)
    wind_stress = centred(splits[2], (2, NY, NX), 1.0, 6.0, ((1, 8), (2, 32)), jnp.float32)
    ocean_current = centred(splits[3], (2, NY, NX), 0.5, 3.0, ((1, 8), (2, 32)), jnp.float32)
    ice_area = jnp.clip(0.15 + 0.049999997 * jax.random.uniform(splits[4], (NCAT, NY, NX), jnp.float32) ** block_scale(splits[4], (NCAT, NY, NX), ((1, 8), (2, 32)), -0.2, 0.2), 0.15, 0.2)
    ice_volume = jnp.clip(0.05 + 0.55 * jax.random.uniform(splits[5], (NCAT, NY, NX), jnp.float32) ** block_scale(splits[5], (NCAT, NY, NX), ((1, 8), (2, 32)), -0.2, 0.2), 0.05, 0.6)
    inverse_width = jnp.clip(jnp.exp(math.log(1.4) - 0.6931472 * jax.random.uniform(splits[6], (NY, NX), jnp.float32) ** block_scale(splits[6], (NY, NX), ((0, 8), (1, 32)), -0.2, 0.2)), 0.7, 1.4)
    inverse_height = jnp.clip(jnp.exp(math.log(1.4) - 0.6931472 * jax.random.uniform(splits[7], (NY, NX), jnp.float32) ** block_scale(splits[7], (NY, NX), ((0, 8), (1, 32)), -0.2, 0.2)), 0.7, 1.4)
    land_block = place_ends((jax.random.randint(splits[8], (NBY, NBX), 0, 4) < 3).astype(jnp.int32), jax.random.fold_in(splits[8], 1), 0, 1)
    ice_block = place_ends((jax.random.randint(splits[9], (NBY, NBX), 0, 3) < 2).astype(jnp.int32), jax.random.fold_in(splits[9], 1), 0, 1)
    writer = place_ends(jax.random.randint(splits[10], (GROUPS,), 0, SLOTS), jax.random.fold_in(splits[10], 1), 0, SLOTS - 1).astype(jnp.int32)
    return {"velocity_start": velocity_start, "stress_start": stress_start, "wind_stress": wind_stress, "ocean_current": ocean_current, "ice_area": ice_area, "ice_volume": ice_volume, "inverse_width": inverse_width, "inverse_height": inverse_height, "land_block": land_block, "ice_block": ice_block, "writer": writer}


strength_scale = 4.0
hibler_decay = 20.0
mass_rate = 16.0
water_drag = 1.0
coriolis = 0.5
relax_rate = 0.5
ellipse_square = 4.0
delta_margin = 0.5

def expand_blocks(blocks, height, breadth):
    counted = blocks.astype(jnp.float32)
    block_rows, block_cols = counted.shape
    spread = jnp.broadcast_to(counted[:, None, :, None], (block_rows, height // block_rows, block_cols, breadth // block_cols))
    return spread.reshape(height, breadth)

def stress_update(stresses, strength, across_scale, along_scale, north_east, north_west, south_east, south_west):
    grad_ux = 0.5 * across_scale * (north_east[0] + south_east[0] - (north_west[0] + south_west[0]))
    grad_vy = 0.5 * along_scale * (north_east[1] + north_west[1] - (south_east[1] + south_west[1]))
    grad_uy = 0.5 * along_scale * (north_east[0] + north_west[0] - (south_east[0] + south_west[0]))
    grad_vx = 0.5 * across_scale * (north_east[1] + south_east[1] - (north_west[1] + south_west[1]))
    divergence = grad_ux + grad_vy
    tension = grad_ux - grad_vy
    shearing = grad_uy + grad_vx
    deform = jnp.sqrt(divergence * divergence + (tension * tension + shearing * shearing) / ellipse_square)
    viscous = strength / (deform + delta_margin)
    normal_sum = (stresses[0] + relax_rate * viscous * (divergence - deform)) / (1.0 + relax_rate)
    normal_diff = (stresses[1] + relax_rate * viscous * tension / ellipse_square) / (1.0 + relax_rate)
    shear_new = (stresses[2] + relax_rate * viscous * shearing / (2.0 * ellipse_square)) / (1.0 + relax_rate)
    return jnp.stack([normal_sum, normal_diff, shear_new])

def normal_xx(stresses):
    return 0.5 * (stresses[0] + stresses[1])

def normal_yy(stresses):
    return 0.5 * (stresses[0] - stresses[1])

def stress_force(across_scale, along_scale, south_west, south_east, north_west, north_east):
    force_x = 0.5 * across_scale * (normal_xx(south_east) + normal_xx(north_east) - (normal_xx(south_west) + normal_xx(north_west))) + 0.5 * along_scale * (north_west[2] + north_east[2] - (south_west[2] + south_east[2]))
    force_y = 0.5 * across_scale * (south_east[2] + north_east[2] - (south_west[2] + north_west[2])) + 0.5 * along_scale * (normal_yy(north_west) + normal_yy(north_east) - (normal_yy(south_west) + normal_yy(south_east)))
    return (force_x, force_y)

def momentum(velocity, force_x, force_y, inertia, turning, wind_stress, ocean_current, land_cells, ice_cells):
    damped = inertia + water_drag
    right_x = inertia * velocity[0] + force_x + wind_stress[0] + water_drag * ocean_current[0]
    right_y = inertia * velocity[1] + force_y + wind_stress[1] + water_drag * ocean_current[1]
    denominator = damped * damped + turning * turning
    next_u = (damped * right_x + turning * right_y) / denominator
    next_v = (damped * right_y - turning * right_x) / denominator
    moving = jnp.stack([next_u, next_v])
    return land_cells * (ice_cells * moving + (1.0 - ice_cells) * ocean_current)

def shift_south(stacked):
    return jnp.concatenate([jnp.zeros_like(stacked[:, :1]), stacked[:, :-1]], axis=1)

def fold_north(stacked):
    return jnp.concatenate([stacked[:, 1:], stacked[:, -1:, ::-1]], axis=1)

def reference(velocity_start, stress_start, wind_stress, ocean_current, ice_area, ice_volume, inverse_width, inverse_height, land_block, ice_block, writer):
    height, breadth = inverse_width.shape
    land_cells = expand_blocks(land_block, height, breadth)
    ice_cells = expand_blocks(ice_block, height, breadth)
    area_total = lax.optimization_barrier(jnp.sum(ice_area, axis=0))
    volume_total = lax.optimization_barrier(jnp.sum(ice_volume, axis=0))
    strength = strength_scale * volume_total * jnp.exp(-hibler_decay * (1.0 - area_total)) * land_cells
    inertia = mass_rate * (1.0 + volume_total)
    turning = coriolis * (1.0 + volume_total)
    velocity = velocity_start
    stresses = stress_start
    for subcycle in range(SUB):
        west_side = jnp.roll(velocity, 1, axis=2)
        south_side = shift_south(velocity)
        south_west = shift_south(west_side)
        stresses = stress_update(stresses, strength, inverse_width, inverse_height, velocity, west_side, south_side, south_west)
        east_side = jnp.roll(stresses, -1, axis=2)
        north_side = fold_north(stresses)
        north_east = jnp.roll(north_side, -1, axis=2)
        force_x, force_y = stress_force(inverse_width, inverse_height, stresses, east_side, north_side, north_east)
        velocity = momentum(velocity, force_x, force_y, inertia, turning, wind_stress, ocean_current, land_cells, ice_cells)
    snapshot = jnp.concatenate([ice_area, ice_volume], axis=0)
    strip_owner = writer[jnp.arange(NX, dtype=jnp.int32) // CX]
    slot_index = jnp.arange(SLOTS, dtype=jnp.int32)
    chosen = slot_index[:, None, None, None] == strip_owner[None, None, None, :]
    restart = jnp.where(chosen, snapshot[None], jnp.zeros((), snapshot.dtype))
    return (velocity, stresses, restart)
```

```python
import jax
import jax.numpy as jnp
from jax import lax
from jax.experimental import pallas as pl
from jax.experimental.pallas import tpu as pltpu
from jax.sharding import PartitionSpec as P


SUB = 12
ROWS = 64
LANES = 128
HALO = 16
PAD = 8
TALL = PAD + HALO + ROWS + HALO + PAD
TOP = PAD + HALO + ROWS

U, V, S1, S2, S12, STR, HW, HH, INE, AA, KU, KV = range(12)
SENT = 12
BB, HWV, HHV, DU, SU, DV, SV, DP, DS, AS, AM = range(12, 23)
HELD = 23
MOVING = (U, V, INE, AA, KU, KV)
NEGATED = (U, V, KU, KV)
MESSAGE = SENT * HALO + SENT // 2 * 8


def lane_index():
    return lax.broadcasted_iota(jnp.int32, (8, LANES), 1)


def row_index():
    return lax.broadcasted_iota(jnp.int32, (8, LANES), 0)


def turned(value, steps):
    steps = steps % LANES
    return value if steps == 0 else pltpu.roll(value, steps, 1)


def west(main, side, first):
    a, b = turned(main, 1), turned(side, 1)
    return jnp.where(first, b, a), jnp.where(first, a, b)


def east(main, side, last):
    a, b = turned(main, -1), turned(side, -1)
    return jnp.where(last, b, a), jnp.where(last, a, b)


def expanded(blocks_t):
    rows = lax.broadcasted_iota(jnp.int32, (ROWS, 16), 0) // 4
    pick_rows = (rows == lax.broadcasted_iota(jnp.int32, (ROWS, 16), 1)).astype(jnp.float32)
    lanes = lax.broadcasted_iota(jnp.int32, (4, LANES), 1) // 32
    pick_lanes = (lanes == lax.broadcasted_iota(jnp.int32, (4, LANES), 0)).astype(jnp.float32)
    half = lax.dot_general(
        pick_rows, blocks_t, (((1,), (1,)), ((), ())), preferred_element_type=jnp.float32
    )
    return lax.dot_general(
        half, pick_lanes, (((1,), (0,)), ((), ())), preferred_element_type=jnp.float32
    )


def prepare_kernel(
    vel_hbm,
    stress_hbm,
    wind_hbm,
    ocean_hbm,
    area_hbm,
    volume_hbm,
    wide_hbm,
    high_hbm,
    land_hbm,
    ice_hbm,
    fields,
    to_west,
    to_east,
    snap,
    vel,
    stress,
    wind,
    ocean,
    wide,
    high,
    land_t,
    ice_t,
    sems,
):
    area, volume = snap.at[0:5], snap.at[5:10]
    moves = (
        (area_hbm, area),
        (volume_hbm, volume),
        (land_hbm, land_t),
        (ice_hbm, ice_t),
        (ocean_hbm, ocean),
        (wind_hbm, wind),
        (stress_hbm, stress),
        (vel_hbm, vel),
        (wide_hbm, wide),
        (high_hbm, high),
    )
    copies = [pltpu.make_async_copy(a, b, sems.at[n]) for n, (a, b) in enumerate(moves)]
    for copy in copies:
        copy.start()
    for copy in copies:
        copy.wait()
    land = expanded(land_t[...].astype(jnp.float32))
    ice = expanded(ice_t[...].astype(jnp.float32))
    area_total = area[0] + area[1] + area[2] + area[3] + area[4]
    volume_total = volume[0] + volume[1] + volume[2] + volume[3] + volume[4]
    fields[U] = vel[0]
    fields[V] = vel[1]
    fields[S1] = 0.5 * stress[0]
    fields[S2] = 0.5 * stress[1]
    fields[S12] = stress[2]
    fields[STR] = (4.0 / 6.0) * volume_total * jnp.exp(-20.0 * (1.0 - area_total)) * land
    fields[HW] = 0.5 * wide[...]
    fields[HH] = 0.5 * high[...]
    inertia = 16.0 * (1.0 + volume_total)
    turning = 0.5 * (1.0 + volume_total)
    damped = inertia + 1.0
    scale = land * ice / (damped * damped + turning * turning)
    still = land * (1.0 - ice)
    fx = wind[0] + ocean[0]
    fy = wind[1] + ocean[1]
    fields[INE] = inertia
    fields[AA] = scale
    fields[KU] = scale * (damped * fx + turning * fy) + still * ocean[0]
    fields[KV] = scale * (damped * fy - turning * fx) + still * ocean[1]
    lane = lane_index()
    for f in range(SENT):
        left = right = None
        for g in range(8):
            part = fields[f, 8 * g : 8 * g + 8]
            inside = (lane >= 16 * g) & (lane < 16 * g + 16)
            a = turned(part, 16 * g)
            b = turned(part, 16 * g - 112)
            left = a if g == 0 else jnp.where(inside, a, left)
            right = b if g == 0 else jnp.where(inside, b, right)
        to_west[8 * f : 8 * f + 8] = left
        to_east[8 * f : 8 * f + 8] = right


def rows_kernel(fields, from_west, from_east, to_north, to_south):
    lane = lane_index()
    for f in range(SENT):
        to_north[HALO * f : HALO * f + HALO] = fields[f, ROWS - HALO : ROWS]
        to_south[HALO * f : HALO * f + HALO] = fields[f, 0:HALO]
    for pair in range(SENT // 2):
        north = south = None
        for member in range(2):
            f = 2 * pair + member
            base = 64 * member
            a = from_west[8 * f : 8 * f + 8]
            b = from_east[8 * f : 8 * f + 8]
            here = lane >= base
            there = lane >= base + 32
            n = jnp.where(there, turned(b, base + 32 - 96), turned(a, base - 96))
            s = jnp.where(there, turned(b, base + 32), turned(a, base))
            north = n if member == 0 else jnp.where(here, n, north)
            south = s if member == 0 else jnp.where(here, s, south)
        at = SENT * HALO + 8 * pair
        to_north[at : at + 8] = north
        to_south[at : at + 8] = south


def stencil_kernel(fields, from_west, from_east, from_south, from_north, from_fold, vel, stress, held):
    is_top = lax.axis_index("row") == 7
    lane = lane_index()
    row = row_index()
    first = lane == 0
    last = lane == LANES - 1
    low = lane < 64
    top_rows = jnp.where(is_top, 1, 0) + jnp.zeros((8, LANES), jnp.int32)

    def side_rows(message, f, a):
        at = SENT * HALO + 8 * (f // 2)
        base = 64 * (f % 2)
        corner = message[at : at + 8]
        return jnp.where(low, turned(corner, -(base + 32 + 16 * a)), turned(corner, 112 - base - 16 * a))

    for f in range(SENT):
        a, b = from_west[8 * f : 8 * f + 8], from_east[8 * f : 8 * f + 8]
        for g in range(8):
            at = PAD + HALO + 8 * g
            held[f, 0, at : at + 8] = fields[f, 8 * g : 8 * g + 8]
            held[f, 1, at : at + 8] = jnp.where(low, turned(b, -16 * g), turned(a, 112 - 16 * g))
        for g in range(2):
            at = PAD + 8 * g
            held[f, 0, at : at + 8] = from_south[HALO * f + 8 * g : HALO * f + 8 * g + 8]
            held[f, 1, at : at + 8] = side_rows(from_south, f, g)

    @pl.when(jnp.logical_not(is_top))
    def _():
        for f in range(SENT):
            for g in range(2):
                at = TOP + 8 * g
                held[f, 0, at : at + 8] = from_north[HALO * f + 8 * g : HALO * f + 8 * g + 8]
                held[f, 1, at : at + 8] = side_rows(from_north, f, g)

    @pl.when(is_top)
    def _():
        def rotated(value):
            value = jnp.take_along_axis(value, LANES - 1 - lane, axis=1)
            return jnp.take_along_axis(value, 7 - row, axis=0)

        for f in range(SENT):
            for g in range(2):
                source = 1 - g
                main = rotated(from_fold[HALO * f + 8 * source : HALO * f + 8 * source + 8])
                side = rotated(side_rows(from_fold, f, source))
                if f in MOVING:
                    main, side = east(main, side, last)
                    if f in NEGATED:
                        main, side = -main, -side
                    at = TOP + 8 * g
                else:
                    at = TOP + 1 + 8 * g
                held[f, 0, at : at + 8] = main
                held[f, 1, at : at + 8] = side
                if f in (HW, HH):
                    main, side = east(main, side, last)
                    own = HWV if f == HW else HHV
                    held[own, 0, TOP + 8 * g : TOP + 8 * g + 8] = main
                    held[own, 1, TOP + 8 * g : TOP + 8 * g + 8] = side

    def velocity_sums(at, um, us, vm, vs):
        wum, wus = west(um, us, first)
        wvm, wvs = west(vm, vs, first)
        for t, (x, wx, y, wy) in enumerate(((um, wum, vm, wvm), (us, wus, vs, wvs))):
            held[DU, t, at : at + 8] = x - wx
            held[SU, t, at : at + 8] = x + wx
            held[DV, t, at : at + 8] = y - wy
            held[SV, t, at : at + 8] = y + wy

    for g in range(12):
        at = PAD + 8 * g
        for t in range(2):
            scale = held[AA, t, at : at + 8]
            inertia = held[INE, t, at : at + 8]
            held[AA, t, at : at + 8] = (inertia + 1.0) * scale
            held[BB, t, at : at + 8] = (inertia * (1.0 / 32.0)) * scale
            if g < 10:
                held[HWV, t, at : at + 8] = held[HW, t, at : at + 8]
                held[HHV, t, at : at + 8] = held[HH, t, at : at + 8]
        velocity_sums(
            at,
            held[U, 0, at : at + 8],
            held[U, 1, at : at + 8],
            held[V, 0, at : at + 8],
            held[V, 1, at : at + 8],
        )

    @pl.when(jnp.logical_not(is_top))
    def _():
        for t in range(2):
            held[HWV, t, TOP : TOP + HALO] = held[HW, t, TOP : TOP + HALO]
            held[HHV, t, TOP : TOP + HALO] = held[HH, t, TOP : TOP + HALO]

    def stress_rows(at):
        fresh = []
        for t in range(2):
            here = lambda f: held[f, t, at : at + 8]
            below = lambda f: held[f, t, at - 1 : at + 7]
            hw, hh = here(HW), here(HH)
            gux = hw * (here(DU) + below(DU))
            guy = hh * (here(SU) - below(SU))
            gvx = hw * (here(DV) + below(DV))
            gvy = hh * (here(SV) - below(SV))
            divergence = gux + gvy
            tension = gux - gvy
            shearing = guy + gvx
            deform = jnp.sqrt(
                divergence * divergence + 0.25 * (tension * tension + shearing * shearing)
            )
            viscous = here(STR) / (deform + 0.5)
            quarter = 0.25 * viscous
            s1 = here(S1) * (2.0 / 3.0) + viscous * (divergence - deform)
            s2 = here(S2) * (2.0 / 3.0) + quarter * tension
            s12 = here(S12) * (2.0 / 3.0) + quarter * shearing
            held[S1, t, at : at + 8] = s1
            held[S2, t, at : at + 8] = s2
            held[S12, t, at : at + 8] = s12
            fresh.append((s1 + s2, s1 - s2, s12))
        (pm, mm, qm), (ps, ms, qs) = fresh
        epm, eps = east(pm, ps, last)
        emm, ems = east(mm, ms, last)
        eqm, eqs = east(qm, qs, last)
        for t, (p, ep, m, em, q, eq) in enumerate(
            ((pm, epm, mm, emm, qm, eqm), (ps, eps, ms, ems, qs, eqs))
        ):
            held[DP, t, at : at + 8] = ep - p
            held[AM, t, at : at + 8] = em + m
            held[DS, t, at : at + 8] = eq - q
            held[AS, t, at : at + 8] = eq + q

    def velocity_rows(at):
        fresh = []
        for t in range(2):
            here = lambda f: held[f, t, at : at + 8]

            def pair(f):
                own, above = here(f), held[f, t, at + 1 : at + 9]
                if at == TOP - 8:
                    above = jnp.where((row == 7) & (top_rows == 1), held[f, t, at + 2 : at + 10], above)
                if at == TOP:
                    own = jnp.where((row == 0) & (top_rows == 1), held[f, t, at - 1 : at + 7], own)
                return own, above

            hw, hh = here(HWV), here(HHV)
            dp, ndp = pair(DP)
            ds, nds = pair(DS)
            as_, nas = pair(AS)
            am, nam = pair(AM)
            inertia, a, b = here(INE), here(AA), here(BB)
            x = inertia * here(U) + (hw * (dp + ndp) + hh * (nas - as_))
            y = inertia * here(V) + (hw * (ds + nds) + hh * (nam - am))
            u = a * x + b * y + here(KU)
            v = a * y - b * x + here(KV)
            held[U, t, at : at + 8] = u
            held[V, t, at : at + 8] = v
            fresh.append((u, v))
        (um, vm), (us, vs) = fresh
        velocity_sums(at, um, us, vm, vs)

    def subcycle(lo, hi):
        def body(_, carry):
            for g in range(lo, hi):
                stress_rows(PAD + 8 * g)
            for g in range(lo, hi):
                velocity_rows(PAD + 8 * g)
            return carry

        return body

    lax.fori_loop(0, 5, subcycle(0, 12), 0)
    lax.fori_loop(5, SUB, subcycle(1, 11), 0)
    at = PAD + HALO
    vel[0] = held[U, 0, at : at + ROWS]
    vel[1] = held[V, 0, at : at + ROWS]
    stress[0] = 2.0 * held[S1, 0, at : at + ROWS]
    stress[1] = 2.0 * held[S2, 0, at : at + ROWS]
    stress[2] = held[S12, 0, at : at + ROWS]


def restart_kernel(writer, own, other, near, near_other, far, far_other, side, side_other, out, zero, sems):
    me = lax.axis_index("row")
    chip, core = me // 2, me % 2
    step = 1 - 2 * core
    behind = lax.rem(chip - step + 4, 4)
    ahead = lax.rem(chip + step + 4, 4)
    across = lax.rem(chip + 2, 4)
    blocks = (
        (own, me),
        (other, 2 * chip + 1 - core),
        (near, 2 * behind + core),
        (near_other, 2 * behind + 1 - core),
        (side, 2 * ahead + 1 - core),
        (side_other, 2 * ahead + core),
        (far, 2 * across + core),
        (far_other, 2 * across + 1 - core),
    )
    mine = writer[lax.axis_index("col")] == me

    @pl.when(mine)
    def _():
        copies = [
            pltpu.make_async_copy(ref, out.at[0, :, pl.ds(place * ROWS, ROWS), :], sems.at[n])
            for n, (ref, place) in enumerate(blocks)
        ]
        for copy in copies:
            copy.start()
        for copy in copies:
            copy.wait()

    @pl.when(jnp.logical_not(mine))
    def _():
        zero[...] = jnp.zeros_like(zero)
        copies = [
            pltpu.make_async_copy(zero, out.at[0, :, pl.ds(n * ROWS, ROWS), :], sems.at[n])
            for n in range(8)
        ]
        for copy in copies:
            copy.start()
        for copy in copies:
            copy.wait()


def vmem():
    return pl.BlockSpec(memory_space=pltpu.VMEM)


def shape(*dims):
    return jax.ShapeDtypeStruct(dims, jnp.float32)


def grant(mebibytes):
    return pltpu.CompilerParams(vmem_limit_bytes=mebibytes << 20)


def step(
    velocity_start,
    stress_start,
    wind_stress,
    ocean_current,
    ice_area,
    ice_volume,
    inverse_width,
    inverse_height,
    land_block,
    ice_block,
    writer,
):
    fields, to_west, to_east, snap = pl.pallas_call(
        prepare_kernel,
        out_shape=(
            shape(SENT, ROWS, LANES),
            shape(SENT * 8, LANES),
            shape(SENT * 8, LANES),
            shape(10, ROWS, LANES),
        ),
        in_specs=[pl.BlockSpec(memory_space=pltpu.HBM)] * 10,
        out_specs=(vmem(),) * 4,
        scratch_shapes=[
            pltpu.VMEM((2, ROWS, LANES), jnp.float32),
            pltpu.VMEM((3, ROWS, LANES), jnp.float32),
            pltpu.VMEM((2, ROWS, LANES), jnp.float32),
            pltpu.VMEM((2, ROWS, LANES), jnp.float32),
            pltpu.VMEM((ROWS, LANES), jnp.float32),
            pltpu.VMEM((ROWS, LANES), jnp.float32),
            pltpu.VMEM((4, 16), jnp.int32),
            pltpu.VMEM((4, 16), jnp.int32),
            pltpu.SemaphoreType.DMA((10,)),
        ],
        compiler_params=grant(8),
        name="prepare",
    )(
        *(
            pltpu.with_memory_space_constraint(value, pltpu.HBM)
            for value in (
                velocity_start,
                stress_start,
                wind_stress,
                ocean_current,
                ice_area,
                ice_volume,
                inverse_width,
                inverse_height,
                land_block.T,
                ice_block.T,
            )
        )
    )
    along = [(r, (r + 2 - 4 * (r % 2)) % 8) for r in range(8)]
    partner = [(r, r ^ 1) for r in range(8)]
    eastward = [(c, (c + 1) % 32) for c in range(32)]
    westward = [(c, (c - 1) % 32) for c in range(32)]
    folded = [(7 * 32 + c, 7 * 32 + 31 - c) for c in range(32)]

    from_west = lax.ppermute(to_east, "col", eastward)
    from_east = lax.ppermute(to_west, "col", westward)
    near = lax.ppermute(snap, "row", along)
    other = lax.ppermute(snap, "row", partner)
    near_other = lax.ppermute(other, "row", along)

    to_north, to_south = pl.pallas_call(
        rows_kernel,
        out_shape=(shape(MESSAGE, LANES),) * 2,
        in_specs=[vmem()] * 3,
        out_specs=(vmem(),) * 2,
        compiler_params=grant(8),
        cost_estimate=pl.CostEstimate(flops=1000000, bytes_accessed=1000000, transcendentals=0),
        name="rows",
    )(fields, from_west, from_east)
    from_south = lax.ppermute(to_north, "row", [(r, r + 1) for r in range(7)])
    from_north = lax.ppermute(to_south, "row", [(r + 1, r) for r in range(7)])
    from_fold = lax.ppermute(to_north, ("row", "col"), folded)
    far = lax.ppermute(near, "row", along)
    side = lax.ppermute(near, "row", partner)
    side_other = lax.ppermute(near_other, "row", partner)
    far_other = lax.ppermute(far, "row", partner)

    velocity, stress = pl.pallas_call(
        stencil_kernel,
        out_shape=(shape(2, ROWS, LANES), shape(3, ROWS, LANES)),
        in_specs=[vmem()] * 6,
        out_specs=(vmem(),) * 2,
        scratch_shapes=[pltpu.VMEM((HELD, 2, TALL, LANES), jnp.float32)],
        compiler_params=grant(16),
        cost_estimate=pl.CostEstimate(flops=40000000, bytes_accessed=2000000, transcendentals=0),
        name="stencil",
    )(fields, from_west, from_east, from_south, from_north, from_fold)

    restart = pl.pallas_call(
        restart_kernel,
        out_shape=shape(1, 10, 8 * ROWS, LANES),
        in_specs=[pl.BlockSpec(memory_space=pltpu.SMEM)] + [pl.BlockSpec(memory_space=pl.ANY)] * 8,
        out_specs=pl.BlockSpec(memory_space=pl.ANY),
        scratch_shapes=[pltpu.VMEM((10, ROWS, LANES), jnp.float32), pltpu.SemaphoreType.DMA((8,))],
        compiler_params=grant(4),
        name="restart",
    )(writer, snap, other, near, near_other, far, far_other, side, side_other)
    return (velocity, stress, restart)


def solution(mesh):
    return jax.shard_map(
        step,
        mesh=mesh,
        in_specs=(
            P(None, "row", "col"),
            P(None, "row", "col"),
            P(None, "row", "col"),
            P(None, "row", "col"),
            P(None, "row", "col"),
            P(None, "row", "col"),
            P("row", "col"),
            P("row", "col"),
            P("row", "col"),
            P("row", "col"),
            P(),
        ),
        out_specs=(P(None, "row", "col"), P(None, "row", "col"), P("row", None, None, "col")),
        check_vma=False,
    )
```

```python
import jax
import jax.numpy as jnp
from jax import lax
from jax.experimental import pallas as pl
from jax.experimental.pallas import tpu as pltpu
from jax.sharding import PartitionSpec as P


SUB = 12
ROWS = 64
LANES = 128
HALO = 16
PAD = 8
TALL = PAD + HALO + ROWS + HALO + PAD
TOP = PAD + HALO + ROWS

U, V, S1, S2, S12, STR, HW, HH, INE, AA, KU, KV = range(12)
SENT = 12
BB, HWV, HHV, DU, SU, DV, SV, DP, DS, AS, AM = range(12, 23)
HELD = 23
MOVING = (U, V, INE, AA, KU, KV)
NEGATED = (U, V, KU, KV)
MESSAGE = SENT * HALO + SENT // 2 * 8


def lane_index():
    return lax.broadcasted_iota(jnp.int32, (8, LANES), 1)


def row_index():
    return lax.broadcasted_iota(jnp.int32, (8, LANES), 0)


def turned(value, steps):
    steps = steps % LANES
    return value if steps == 0 else pltpu.roll(value, steps, 1)


def west(main, side, first):
    a, b = turned(main, 1), turned(side, 1)
    return jnp.where(first, b, a), jnp.where(first, a, b)


def east(main, side, last):
    a, b = turned(main, -1), turned(side, -1)
    return jnp.where(last, b, a), jnp.where(last, a, b)


def expanded(blocks_t):
    rows = lax.broadcasted_iota(jnp.int32, (ROWS, 16), 0) // 4
    pick_rows = (rows == lax.broadcasted_iota(jnp.int32, (ROWS, 16), 1)).astype(jnp.float32)
    lanes = lax.broadcasted_iota(jnp.int32, (4, LANES), 1) // 32
    pick_lanes = (lanes == lax.broadcasted_iota(jnp.int32, (4, LANES), 0)).astype(jnp.float32)
    half = lax.dot_general(
        pick_rows, blocks_t, (((1,), (1,)), ((), ())), preferred_element_type=jnp.float32
    )
    return lax.dot_general(
        half, pick_lanes, (((1,), (0,)), ((), ())), preferred_element_type=jnp.float32
    )


def prepare_kernel(
    vel_hbm,
    stress_hbm,
    wind_hbm,
    ocean_hbm,
    area_hbm,
    volume_hbm,
    wide_hbm,
    high_hbm,
    land_hbm,
    ice_hbm,
    fields,
    to_west,
    to_east,
    snap,
    vel,
    stress,
    wind,
    ocean,
    wide,
    high,
    land_t,
    ice_t,
    sems,
):
    area, volume = snap.at[0:5], snap.at[5:10]
    moves = (
        (area_hbm, area),
        (volume_hbm, volume),
        (land_hbm, land_t),
        (ice_hbm, ice_t),
        (ocean_hbm, ocean),
        (wind_hbm, wind),
        (stress_hbm, stress),
        (vel_hbm, vel),
        (wide_hbm, wide),
        (high_hbm, high),
    )
    copies = [pltpu.make_async_copy(a, b, sems.at[n]) for n, (a, b) in enumerate(moves)]
    for copy in copies:
        copy.start()
    for copy in copies:
        copy.wait()
    land = expanded(land_t[...].astype(jnp.float32))
    ice = expanded(ice_t[...].astype(jnp.float32))
    area_total = area[0] + area[1] + area[2] + area[3] + area[4]
    volume_total = volume[0] + volume[1] + volume[2] + volume[3] + volume[4]
    fields[U] = vel[0]
    fields[V] = vel[1]
    fields[S1] = 0.5 * stress[0]
    fields[S2] = 0.5 * stress[1]
    fields[S12] = stress[2]
    fields[STR] = (4.0 / 6.0) * volume_total * jnp.exp(-20.0 * (1.0 - area_total)) * land
    fields[HW] = 0.5 * wide[...]
    fields[HH] = 0.5 * high[...]
    inertia = 16.0 * (1.0 + volume_total)
    turning = 0.5 * (1.0 + volume_total)
    damped = inertia + 1.0
    scale = land * ice / (damped * damped + turning * turning)
    still = land * (1.0 - ice)
    fx = wind[0] + ocean[0]
    fy = wind[1] + ocean[1]
    fields[INE] = inertia
    fields[AA] = scale
    fields[KU] = scale * (damped * fx + turning * fy) + still * ocean[0]
    fields[KV] = scale * (damped * fy - turning * fx) + still * ocean[1]
    lane = lane_index()
    for f in range(SENT):
        left = right = None
        for g in range(8):
            part = fields[f, 8 * g : 8 * g + 8]
            inside = (lane >= 16 * g) & (lane < 16 * g + 16)
            a = turned(part, 16 * g)
            b = turned(part, 16 * g - 112)
            left = a if g == 0 else jnp.where(inside, a, left)
            right = b if g == 0 else jnp.where(inside, b, right)
        to_west[8 * f : 8 * f + 8] = left
        to_east[8 * f : 8 * f + 8] = right


def rows_kernel(fields, from_west, from_east, upward, downward):
    lane = lane_index()
    flipped = lax.axis_index("col") >= 16

    def fill(to_north, to_south):
        for f in range(SENT):
            to_north[HALO * f : HALO * f + HALO] = fields[f, ROWS - HALO : ROWS]
            to_south[HALO * f : HALO * f + HALO] = fields[f, 0:HALO]
        for pair in range(SENT // 2):
            north = south = None
            for member in range(2):
                f = 2 * pair + member
                base = 64 * member
                a = from_west[8 * f : 8 * f + 8]
                b = from_east[8 * f : 8 * f + 8]
                here = lane >= base
                there = lane >= base + 32
                n = jnp.where(there, turned(b, base + 32 - 96), turned(a, base - 96))
                s = jnp.where(there, turned(b, base + 32), turned(a, base))
                north = n if member == 0 else jnp.where(here, n, north)
                south = s if member == 0 else jnp.where(here, s, south)
            at = SENT * HALO + 8 * pair
            to_north[at : at + 8] = north
            to_south[at : at + 8] = south

    @pl.when(flipped)
    def _():
        fill(downward, upward)

    @pl.when(jnp.logical_not(flipped))
    def _():
        fill(upward, downward)


def stencil_masks():
    lane, row = lane_index(), row_index()
    is_top = lax.axis_index("row") == 7
    top_rows = (jnp.where(is_top, 1, 0) + jnp.zeros((8, LANES), jnp.int32)) == 1
    return lane == 0, lane == LANES - 1, row, top_rows


def assemble(fields, from_west, from_east, from_below, from_above, held):
    is_top = lax.axis_index("row") == 7
    flipped = jnp.where(lax.axis_index("col") >= 16, 1, 0) + jnp.zeros((8, LANES), jnp.int32) == 1
    lane = lane_index()
    row = row_index()
    first, last, low = lane == 0, lane == LANES - 1, lane < 64

    def south(at):
        return jnp.where(flipped, from_above[at : at + 8], from_below[at : at + 8])

    def north(at):
        return jnp.where(flipped, from_below[at : at + 8], from_above[at : at + 8])

    def side_rows(message, f, a):
        base = 64 * (f % 2)
        corner = message(SENT * HALO + 8 * (f // 2))
        return jnp.where(low, turned(corner, -(base + 32 + 16 * a)), turned(corner, 112 - base - 16 * a))

    for f in range(SENT):
        a, b = from_west[8 * f : 8 * f + 8], from_east[8 * f : 8 * f + 8]
        for g in range(8):
            at = PAD + HALO + 8 * g
            held[f, 0, at : at + 8] = fields[f, 8 * g : 8 * g + 8]
            held[f, 1, at : at + 8] = jnp.where(low, turned(b, -16 * g), turned(a, 112 - 16 * g))
        for g in range(2):
            at = PAD + 8 * g
            held[f, 0, at : at + 8] = south(HALO * f + 8 * g)
            held[f, 1, at : at + 8] = side_rows(south, f, g)

    @pl.when(jnp.logical_not(is_top))
    def _():
        for f in range(SENT):
            for g in range(2):
                at = TOP + 8 * g
                held[f, 0, at : at + 8] = north(HALO * f + 8 * g)
                held[f, 1, at : at + 8] = side_rows(north, f, g)

    @pl.when(is_top)
    def _():
        def rotated(value):
            value = jnp.take_along_axis(value, LANES - 1 - lane, axis=1)
            return jnp.take_along_axis(value, 7 - row, axis=0)

        for f in range(SENT):
            for g in range(2):
                source = 1 - g
                main = rotated(north(HALO * f + 8 * source))
                side = rotated(side_rows(north, f, source))
                if f in MOVING:
                    main, side = east(main, side, last)
                    if f in NEGATED:
                        main, side = -main, -side
                    at = TOP + 8 * g
                else:
                    at = TOP + 1 + 8 * g
                held[f, 0, at : at + 8] = main
                held[f, 1, at : at + 8] = side
                if f in (HW, HH):
                    main, side = east(main, side, last)
                    own = HWV if f == HW else HHV
                    held[own, 0, TOP + 8 * g : TOP + 8 * g + 8] = main
                    held[own, 1, TOP + 8 * g : TOP + 8 * g + 8] = side

    for g in range(12):
        at = PAD + 8 * g
        for t in range(2):
            scale = held[AA, t, at : at + 8]
            inertia = held[INE, t, at : at + 8]
            held[AA, t, at : at + 8] = (inertia + 1.0) * scale
            held[BB, t, at : at + 8] = (inertia * (1.0 / 32.0)) * scale
            if g < 10:
                held[HWV, t, at : at + 8] = held[HW, t, at : at + 8]
                held[HHV, t, at : at + 8] = held[HH, t, at : at + 8]
        velocity_sums(
            held,
            at,
            held[U, 0, at : at + 8],
            held[U, 1, at : at + 8],
            held[V, 0, at : at + 8],
            held[V, 1, at : at + 8],
            first,
        )

    @pl.when(jnp.logical_not(is_top))
    def _():
        for t in range(2):
            held[HWV, t, TOP : TOP + HALO] = held[HW, t, TOP : TOP + HALO]
            held[HHV, t, TOP : TOP + HALO] = held[HH, t, TOP : TOP + HALO]


def velocity_sums(held, at, um, us, vm, vs, first):
    wum, wus = west(um, us, first)
    wvm, wvs = west(vm, vs, first)
    for t, (x, wx, y, wy) in enumerate(((um, wum, vm, wvm), (us, wus, vs, wvs))):
        held[DU, t, at : at + 8] = x - wx
        held[SU, t, at : at + 8] = x + wx
        held[DV, t, at : at + 8] = y - wy
        held[SV, t, at : at + 8] = y + wy


def stress_rows(held, at, last):
    fresh = []
    for t in range(2):
        here = lambda f: held[f, t, at : at + 8]
        below = lambda f: held[f, t, at - 1 : at + 7]
        hw, hh = here(HW), here(HH)
        gux = hw * (here(DU) + below(DU))
        guy = hh * (here(SU) - below(SU))
        gvx = hw * (here(DV) + below(DV))
        gvy = hh * (here(SV) - below(SV))
        divergence = gux + gvy
        tension = gux - gvy
        shearing = guy + gvx
        deform = jnp.sqrt(
            divergence * divergence + 0.25 * (tension * tension + shearing * shearing)
        )
        viscous = here(STR) / (deform + 0.5)
        quarter = 0.25 * viscous
        s1 = here(S1) * (2.0 / 3.0) + viscous * (divergence - deform)
        s2 = here(S2) * (2.0 / 3.0) + quarter * tension
        s12 = here(S12) * (2.0 / 3.0) + quarter * shearing
        held[S1, t, at : at + 8] = s1
        held[S2, t, at : at + 8] = s2
        held[S12, t, at : at + 8] = s12
        fresh.append((s1 + s2, s1 - s2, s12))
    (pm, mm, qm), (ps, ms, qs) = fresh
    epm, eps = east(pm, ps, last)
    emm, ems = east(mm, ms, last)
    eqm, eqs = east(qm, qs, last)
    for t, (p, ep, m, em, q, eq) in enumerate(
        ((pm, epm, mm, emm, qm, eqm), (ps, eps, ms, ems, qs, eqs))
    ):
        held[DP, t, at : at + 8] = ep - p
        held[AM, t, at : at + 8] = em + m
        held[DS, t, at : at + 8] = eq - q
        held[AS, t, at : at + 8] = eq + q


def velocity_rows(held, at, first, row, top_rows):
    fresh = []
    for t in range(2):
        here = lambda f: held[f, t, at : at + 8]

        def pair(f):
            own, above = here(f), held[f, t, at + 1 : at + 9]
            if at == TOP - 8:
                above = jnp.where((row == 7) & top_rows, held[f, t, at + 2 : at + 10], above)
            if at == TOP:
                own = jnp.where((row == 0) & top_rows, held[f, t, at - 1 : at + 7], own)
            return own, above

        hw, hh = here(HWV), here(HHV)
        dp, ndp = pair(DP)
        ds, nds = pair(DS)
        as_, nas = pair(AS)
        am, nam = pair(AM)
        inertia, a, b = here(INE), here(AA), here(BB)
        x = inertia * here(U) + (hw * (dp + ndp) + hh * (nas - as_))
        y = inertia * here(V) + (hw * (ds + nds) + hh * (nam - am))
        u = a * x + b * y + here(KU)
        v = a * y - b * x + here(KV)
        held[U, t, at : at + 8] = u
        held[V, t, at : at + 8] = v
        fresh.append((u, v))
    (um, vm), (us, vs) = fresh
    velocity_sums(held, at, um, us, vm, vs, first)


def subcycles(held, start, stop, lo, hi):
    first, last, row, top_rows = stencil_masks()

    def body(_, carry):
        for g in range(lo, hi):
            stress_rows(held, PAD + 8 * g, last)
        for g in range(lo, hi):
            velocity_rows(held, PAD + 8 * g, first, row, top_rows)
        return carry

    lax.fori_loop(start, stop, body, 0)


def place_of(me, which):
    chip, core = me // 2, me % 2
    step = 1 - 2 * core
    if which >= 4:
        core = 1 - core
        which -= 4
        step = -step
    chips = (chip, lax.rem(chip - step + 4, 4), lax.rem(chip + step + 4, 4), lax.rem(chip + 2, 4))
    return (2 * chips[which] + core) * ROWS


def into(out, ref, place, sem):
    return pltpu.make_async_copy(ref, out.at[0, :, pl.ds(place, ROWS), :], sem)


def first_half_kernel(
    fields, from_west, from_east, from_below, from_above, snap, writer_hbm, held, out, flag, writer, zero, sems
):
    me = lax.axis_index("row")
    read = pltpu.make_async_copy(writer_hbm, writer, sems.at[8])
    read.start()
    zero[...] = jnp.zeros_like(zero)
    assemble(fields, from_west, from_east, from_below, from_above, held)
    read.wait()
    mine = writer[lax.axis_index("col")] == me
    flag[...] = jnp.where(mine, 1, 0) + jnp.zeros((8, LANES), jnp.int32)
    zeros = [into(out, zero, n * ROWS, sems.at[n]) for n in range(8)]
    own = into(out, snap, place_of(me, 0), sems.at[0])

    @pl.when(mine)
    def _():
        own.start()

    @pl.when(jnp.logical_not(mine))
    def _():
        for copy in zeros:
            copy.start()

    subcycles(held, 0, 5, 0, 12)

    @pl.when(mine)
    def _():
        own.wait()

    @pl.when(jnp.logical_not(mine))
    def _():
        for copy in zeros:
            copy.wait()


def second_half_kernel(state, out_in, flag, near, near_back, vel, stress, held, out, sems):
    me = lax.axis_index("row")
    mine = jnp.max(flag[...]) == 1
    copies = [
        into(out, near, place_of(me, 1), sems.at[0]),
        into(out, near_back, place_of(me, 2), sems.at[1]),
    ]

    @pl.when(mine)
    def _():
        for copy in copies:
            copy.start()

    subcycles(held, 5, SUB, 1, 11)
    at = PAD + HALO
    vel[0] = held[U, 0, at : at + ROWS]
    vel[1] = held[V, 0, at : at + ROWS]
    stress[0] = 2.0 * held[S1, 0, at : at + ROWS]
    stress[1] = 2.0 * held[S2, 0, at : at + ROWS]
    stress[2] = held[S12, 0, at : at + ROWS]

    @pl.when(mine)
    def _():
        for copy in copies:
            copy.wait()


def last_kernel(out_in, flag, far, partner, partner_far, out, sems):
    me = lax.axis_index("row")
    mine = jnp.max(flag[...]) == 1

    @pl.when(mine)
    def _():
        copies = [
            into(out, far, place_of(me, 3), sems.at[0]),
            into(out, partner.at[0], place_of(me, 4), sems.at[1]),
            into(out, partner.at[1], place_of(me, 5), sems.at[2]),
            into(out, partner.at[2], place_of(me, 6), sems.at[3]),
            into(out, partner_far, place_of(me, 7), sems.at[4]),
        ]
        for copy in copies:
            copy.start()
        for copy in copies:
            copy.wait()


def join_kernel(own, near, near_back, joined):
    joined[0] = own[...]
    joined[1] = near[...]
    joined[2] = near_back[...]


def vmem():
    return pl.BlockSpec(memory_space=pltpu.VMEM)


def shape(*dims):
    return jax.ShapeDtypeStruct(dims, jnp.float32)


def grant(mebibytes):
    return pltpu.CompilerParams(vmem_limit_bytes=mebibytes << 20)


def step(
    velocity_start,
    stress_start,
    wind_stress,
    ocean_current,
    ice_area,
    ice_volume,
    inverse_width,
    inverse_height,
    land_block,
    ice_block,
    writer,
):
    fields, to_west, to_east, snap = pl.pallas_call(
        prepare_kernel,
        out_shape=(
            shape(SENT, ROWS, LANES),
            shape(SENT * 8, LANES),
            shape(SENT * 8, LANES),
            shape(10, ROWS, LANES),
        ),
        in_specs=[pl.BlockSpec(memory_space=pltpu.HBM)] * 10,
        out_specs=(vmem(),) * 4,
        scratch_shapes=[
            pltpu.VMEM((2, ROWS, LANES), jnp.float32),
            pltpu.VMEM((3, ROWS, LANES), jnp.float32),
            pltpu.VMEM((2, ROWS, LANES), jnp.float32),
            pltpu.VMEM((2, ROWS, LANES), jnp.float32),
            pltpu.VMEM((ROWS, LANES), jnp.float32),
            pltpu.VMEM((ROWS, LANES), jnp.float32),
            pltpu.VMEM((4, 16), jnp.int32),
            pltpu.VMEM((4, 16), jnp.int32),
            pltpu.SemaphoreType.DMA((10,)),
        ],
        compiler_params=grant(8),
        name="prepare",
    )(
        *(
            pltpu.with_memory_space_constraint(value, pltpu.HBM)
            for value in (
                velocity_start,
                stress_start,
                wind_stress,
                ocean_current,
                ice_area,
                ice_volume,
                inverse_width,
                inverse_height,
                land_block.T,
                ice_block.T,
            )
        )
    )
    along = [(r, (r + 2 - 4 * (r % 2)) % 8) for r in range(8)]
    against = [(r, (r - 2 + 4 * (r % 2)) % 8) for r in range(8)]
    partner = [(r, r ^ 1) for r in range(8)]
    eastward = [(c, (c + 1) % 32) for c in range(32)]
    westward = [(c, (c - 1) % 32) for c in range(32)]
    upward = []
    for c in range(16):
        line = [32 * r + c for r in range(8)] + [32 * (7 - r) + 31 - c for r in range(8)]
        upward += list(zip(line[:-1], line[1:]))
    downward = [(b, a) for a, b in upward]

    near = lax.ppermute(snap, "row", along)
    from_west = lax.ppermute(to_east, "col", eastward)
    from_east = lax.ppermute(to_west, "col", westward)
    near_back = lax.ppermute(snap, "row", against)

    to_above, to_below = pl.pallas_call(
        rows_kernel,
        out_shape=(shape(MESSAGE, LANES),) * 2,
        in_specs=[vmem()] * 3,
        out_specs=(vmem(),) * 2,
        compiler_params=grant(8),
        cost_estimate=pl.CostEstimate(flops=1000000, bytes_accessed=1000000, transcendentals=0),
        name="rows",
    )(fields, from_west, from_east)
    from_below = lax.ppermute(to_above, ("row", "col"), upward)
    from_above = lax.ppermute(to_below, ("row", "col"), downward)
    far = lax.ppermute(near, "row", along)

    hbm = lambda: pl.BlockSpec(memory_space=pl.ANY)
    state, restart, flag = pl.pallas_call(
        first_half_kernel,
        out_shape=(
            shape(HELD, 2, TALL, LANES),
            shape(1, 10, 8 * ROWS, LANES),
            jax.ShapeDtypeStruct((8, LANES), jnp.int32),
        ),
        in_specs=[vmem()] * 5 + [hbm(), hbm()],
        out_specs=(vmem(), hbm(), vmem()),
        scratch_shapes=[
            pltpu.SMEM((32,), jnp.int32),
            pltpu.VMEM((10, ROWS, LANES), jnp.float32),
            pltpu.SemaphoreType.DMA((9,)),
        ],
        compiler_params=grant(16),
        cost_estimate=pl.CostEstimate(flops=20000000, bytes_accessed=2000000, transcendentals=0),
        name="first_half",
    )(
        fields,
        from_west,
        from_east,
        from_below,
        from_above,
        snap,
        pltpu.with_memory_space_constraint(writer, pltpu.HBM),
    )

    joined = pl.pallas_call(
        join_kernel,
        out_shape=shape(3, 10, ROWS, LANES),
        in_specs=[vmem()] * 3,
        out_specs=vmem(),
        compiler_params=grant(8),
        name="join",
    )(snap, near, near_back)
    partner_blocks = lax.ppermute(joined, "row", partner)

    velocity, stress, _, restart = pl.pallas_call(
        second_half_kernel,
        out_shape=(
            shape(2, ROWS, LANES),
            shape(3, ROWS, LANES),
            shape(HELD, 2, TALL, LANES),
            shape(1, 10, 8 * ROWS, LANES),
        ),
        in_specs=[vmem(), hbm(), vmem(), hbm(), hbm()],
        out_specs=(vmem(), vmem(), vmem(), hbm()),
        input_output_aliases={0: 2, 1: 3},
        scratch_shapes=[pltpu.SemaphoreType.DMA((2,))],
        compiler_params=grant(8),
        cost_estimate=pl.CostEstimate(flops=20000000, bytes_accessed=2000000, transcendentals=0),
        name="second_half",
    )(state, restart, flag, near, near_back)
    partner_far = lax.ppermute(far, "row", partner)

    restart = pl.pallas_call(
        last_kernel,
        out_shape=shape(1, 10, 8 * ROWS, LANES),
        in_specs=[hbm(), vmem(), hbm(), hbm(), hbm()],
        out_specs=hbm(),
        input_output_aliases={0: 0},
        scratch_shapes=[pltpu.SemaphoreType.DMA((5,))],
        compiler_params=grant(4),
        name="last",
    )(restart, flag, far, partner_blocks, partner_far)
    return (velocity, stress, restart)


def solution(mesh):
    return jax.shard_map(
        step,
        mesh=mesh,
        in_specs=(
            P(None, "row", "col"),
            P(None, "row", "col"),
            P(None, "row", "col"),
            P(None, "row", "col"),
            P(None, "row", "col"),
            P(None, "row", "col"),
            P("row", "col"),
            P("row", "col"),
            P("row", "col"),
            P("row", "col"),
            P(),
        ),
        out_specs=(P(None, "row", "col"), P(None, "row", "col"), P("row", None, None, "col")),
        check_vma=False,
    )
```

```python
import jax
import jax.numpy as jnp
from jax import lax
from jax.experimental import pallas as pl
from jax.experimental.pallas import tpu as pltpu
from jax.sharding import PartitionSpec as P


SUB = 12
SPLIT = 7
ROWS = 64
LANES = 128
HALO = 16
PAD = 8
TALL = PAD + HALO + ROWS + HALO + PAD
TOP = PAD + HALO + ROWS

U, V, S1, S2, S12, STR, HW, HH, INE, AA, KU, KV = range(12)
SENT = 12
BB, HWV, HHV, DU, SU, DV, SV, DP, DS, AS, AM = range(12, 23)
HELD = 23
MOVING = (U, V, INE, AA, KU, KV)
NEGATED = (U, V, KU, KV)
MESSAGE = SENT * HALO + SENT // 2 * 8


def lane_index():
    return lax.broadcasted_iota(jnp.int32, (8, LANES), 1)


def row_index():
    return lax.broadcasted_iota(jnp.int32, (8, LANES), 0)


def turned(value, steps):
    steps = steps % LANES
    return value if steps == 0 else pltpu.roll(value, steps, 1)


def west(main, side, first):
    a, b = turned(main, 1), turned(side, 1)
    return jnp.where(first, b, a), jnp.where(first, a, b)


def east(main, side, last):
    a, b = turned(main, -1), turned(side, -1)
    return jnp.where(last, b, a), jnp.where(last, a, b)


def expanded(blocks_t):
    rows = lax.broadcasted_iota(jnp.int32, (ROWS, 16), 0) // 4
    pick_rows = (rows == lax.broadcasted_iota(jnp.int32, (ROWS, 16), 1)).astype(jnp.float32)
    lanes = lax.broadcasted_iota(jnp.int32, (4, LANES), 1) // 32
    pick_lanes = (lanes == lax.broadcasted_iota(jnp.int32, (4, LANES), 0)).astype(jnp.float32)
    half = lax.dot_general(
        pick_rows, blocks_t, (((1,), (1,)), ((), ())), preferred_element_type=jnp.float32
    )
    return lax.dot_general(
        half, pick_lanes, (((1,), (0,)), ((), ())), preferred_element_type=jnp.float32
    )


def prepare_kernel(
    vel_hbm,
    stress_hbm,
    wind_hbm,
    ocean_hbm,
    area_hbm,
    volume_hbm,
    wide_hbm,
    high_hbm,
    land_hbm,
    ice_hbm,
    fields,
    to_west,
    to_east,
    snap,
    vel,
    stress,
    wind,
    ocean,
    wide,
    high,
    land_t,
    ice_t,
    sems,
):
    area, volume = snap.at[0:5], snap.at[5:10]
    moves = (
        (area_hbm, area),
        (volume_hbm, volume),
        (land_hbm, land_t),
        (ice_hbm, ice_t),
        (ocean_hbm, ocean),
        (wind_hbm, wind),
        (stress_hbm, stress),
        (vel_hbm, vel),
        (wide_hbm, wide),
        (high_hbm, high),
    )
    copies = [pltpu.make_async_copy(a, b, sems.at[n]) for n, (a, b) in enumerate(moves)]
    for copy in copies:
        copy.start()
    for copy in copies:
        copy.wait()
    land = expanded(land_t[...].astype(jnp.float32))
    ice = expanded(ice_t[...].astype(jnp.float32))
    area_total = area[0] + area[1] + area[2] + area[3] + area[4]
    volume_total = volume[0] + volume[1] + volume[2] + volume[3] + volume[4]
    fields[U] = vel[0]
    fields[V] = vel[1]
    fields[S1] = 0.5 * stress[0]
    fields[S2] = 0.5 * stress[1]
    fields[S12] = stress[2]
    fields[STR] = (4.0 / 6.0) * volume_total * jnp.exp(-20.0 * (1.0 - area_total)) * land
    fields[HW] = 0.5 * wide[...]
    fields[HH] = 0.5 * high[...]
    inertia = 16.0 * (1.0 + volume_total)
    turning = 0.5 * (1.0 + volume_total)
    damped = inertia + 1.0
    scale = land * ice / (damped * damped + turning * turning)
    still = land * (1.0 - ice)
    fx = wind[0] + ocean[0]
    fy = wind[1] + ocean[1]
    fields[INE] = inertia
    fields[AA] = scale
    fields[KU] = scale * (damped * fx + turning * fy) + still * ocean[0]
    fields[KV] = scale * (damped * fy - turning * fx) + still * ocean[1]
    lane = lane_index()
    for f in range(SENT):
        left = right = None
        for g in range(8):
            part = fields[f, 8 * g : 8 * g + 8]
            inside = (lane >= 16 * g) & (lane < 16 * g + 16)
            a = turned(part, 16 * g)
            b = turned(part, 16 * g - 112)
            left = a if g == 0 else jnp.where(inside, a, left)
            right = b if g == 0 else jnp.where(inside, b, right)
        to_west[8 * f : 8 * f + 8] = left
        to_east[8 * f : 8 * f + 8] = right


def rows_kernel(fields, from_west, from_east, upward, downward):
    lane = lane_index()
    flipped = lax.axis_index("col") >= 16

    def fill(to_north, to_south):
        for f in range(SENT):
            to_north[HALO * f : HALO * f + HALO] = fields[f, ROWS - HALO : ROWS]
            to_south[HALO * f : HALO * f + HALO] = fields[f, 0:HALO]
        for pair in range(SENT // 2):
            north = south = None
            for member in range(2):
                f = 2 * pair + member
                base = 64 * member
                a = from_west[8 * f : 8 * f + 8]
                b = from_east[8 * f : 8 * f + 8]
                here = lane >= base
                there = lane >= base + 32
                n = jnp.where(there, turned(b, base + 32 - 96), turned(a, base - 96))
                s = jnp.where(there, turned(b, base + 32), turned(a, base))
                north = n if member == 0 else jnp.where(here, n, north)
                south = s if member == 0 else jnp.where(here, s, south)
            at = SENT * HALO + 8 * pair
            to_north[at : at + 8] = north
            to_south[at : at + 8] = south

    @pl.when(flipped)
    def _():
        fill(downward, upward)

    @pl.when(jnp.logical_not(flipped))
    def _():
        fill(upward, downward)


def stencil_masks():
    lane, row = lane_index(), row_index()
    is_top = lax.axis_index("row") == 7
    top_rows = (jnp.where(is_top, 1, 0) + jnp.zeros((8, LANES), jnp.int32)) == 1
    return lane == 0, lane == LANES - 1, row, top_rows


def assemble(fields, from_west, from_east, from_below, from_above, held):
    is_top = lax.axis_index("row") == 7
    flipped = jnp.where(lax.axis_index("col") >= 16, 1, 0) + jnp.zeros((8, LANES), jnp.int32) == 1
    lane = lane_index()
    row = row_index()
    first, last, low = lane == 0, lane == LANES - 1, lane < 64

    def south(at):
        return jnp.where(flipped, from_above[at : at + 8], from_below[at : at + 8])

    def north(at):
        return jnp.where(flipped, from_below[at : at + 8], from_above[at : at + 8])

    def side_rows(message, f, a):
        base = 64 * (f % 2)
        corner = message(SENT * HALO + 8 * (f // 2))
        return jnp.where(low, turned(corner, -(base + 32 + 16 * a)), turned(corner, 112 - base - 16 * a))

    for f in range(SENT):
        a, b = from_west[8 * f : 8 * f + 8], from_east[8 * f : 8 * f + 8]
        for g in range(8):
            at = PAD + HALO + 8 * g
            held[f, 0, at : at + 8] = fields[f, 8 * g : 8 * g + 8]
            held[f, 1, at : at + 8] = jnp.where(low, turned(b, -16 * g), turned(a, 112 - 16 * g))
        for g in range(2):
            at = PAD + 8 * g
            held[f, 0, at : at + 8] = south(HALO * f + 8 * g)
            held[f, 1, at : at + 8] = side_rows(south, f, g)

    @pl.when(jnp.logical_not(is_top))
    def _():
        for f in range(SENT):
            for g in range(2):
                at = TOP + 8 * g
                held[f, 0, at : at + 8] = north(HALO * f + 8 * g)
                held[f, 1, at : at + 8] = side_rows(north, f, g)

    @pl.when(is_top)
    def _():
        def rotated(value):
            value = jnp.take_along_axis(value, LANES - 1 - lane, axis=1)
            return jnp.take_along_axis(value, 7 - row, axis=0)

        for f in range(SENT):
            for g in range(2):
                source = 1 - g
                main = rotated(north(HALO * f + 8 * source))
                side = rotated(side_rows(north, f, source))
                if f in MOVING:
                    main, side = east(main, side, last)
                    if f in NEGATED:
                        main, side = -main, -side
                    at = TOP + 8 * g
                else:
                    at = TOP + 1 + 8 * g
                held[f, 0, at : at + 8] = main
                held[f, 1, at : at + 8] = side
                if f in (HW, HH):
                    main, side = east(main, side, last)
                    own = HWV if f == HW else HHV
                    held[own, 0, TOP + 8 * g : TOP + 8 * g + 8] = main
                    held[own, 1, TOP + 8 * g : TOP + 8 * g + 8] = side

    for g in range(12):
        at = PAD + 8 * g
        for t in range(2):
            scale = held[AA, t, at : at + 8]
            inertia = held[INE, t, at : at + 8]
            held[AA, t, at : at + 8] = (inertia + 1.0) * scale
            held[BB, t, at : at + 8] = (inertia * (1.0 / 32.0)) * scale
            if g < 10:
                held[HWV, t, at : at + 8] = held[HW, t, at : at + 8]
                held[HHV, t, at : at + 8] = held[HH, t, at : at + 8]
        velocity_sums(
            held,
            at,
            held[U, 0, at : at + 8],
            held[U, 1, at : at + 8],
            held[V, 0, at : at + 8],
            held[V, 1, at : at + 8],
            first,
        )

    @pl.when(jnp.logical_not(is_top))
    def _():
        for t in range(2):
            held[HWV, t, TOP : TOP + HALO] = held[HW, t, TOP : TOP + HALO]
            held[HHV, t, TOP : TOP + HALO] = held[HH, t, TOP : TOP + HALO]


def velocity_sums(held, at, um, us, vm, vs, first):
    wum, wus = west(um, us, first)
    wvm, wvs = west(vm, vs, first)
    for t, (x, wx, y, wy) in enumerate(((um, wum, vm, wvm), (us, wus, vs, wvs))):
        held[DU, t, at : at + 8] = x - wx
        held[SU, t, at : at + 8] = x + wx
        held[DV, t, at : at + 8] = y - wy
        held[SV, t, at : at + 8] = y + wy


def stress_rows(held, at, last):
    fresh = []
    for t in range(2):
        here = lambda f: held[f, t, at : at + 8]
        below = lambda f: held[f, t, at - 1 : at + 7]
        hw, hh = here(HW), here(HH)
        gux = hw * (here(DU) + below(DU))
        guy = hh * (here(SU) - below(SU))
        gvx = hw * (here(DV) + below(DV))
        gvy = hh * (here(SV) - below(SV))
        divergence = gux + gvy
        tension = gux - gvy
        shearing = guy + gvx
        deform = jnp.sqrt(
            divergence * divergence + 0.25 * (tension * tension + shearing * shearing)
        )
        viscous = here(STR) / (deform + 0.5)
        quarter = 0.25 * viscous
        s1 = here(S1) * (2.0 / 3.0) + viscous * (divergence - deform)
        s2 = here(S2) * (2.0 / 3.0) + quarter * tension
        s12 = here(S12) * (2.0 / 3.0) + quarter * shearing
        held[S1, t, at : at + 8] = s1
        held[S2, t, at : at + 8] = s2
        held[S12, t, at : at + 8] = s12
        fresh.append((s1 + s2, s1 - s2, s12))
    (pm, mm, qm), (ps, ms, qs) = fresh
    epm, eps = east(pm, ps, last)
    emm, ems = east(mm, ms, last)
    eqm, eqs = east(qm, qs, last)
    for t, (p, ep, m, em, q, eq) in enumerate(
        ((pm, epm, mm, emm, qm, eqm), (ps, eps, ms, ems, qs, eqs))
    ):
        held[DP, t, at : at + 8] = ep - p
        held[AM, t, at : at + 8] = em + m
        held[DS, t, at : at + 8] = eq - q
        held[AS, t, at : at + 8] = eq + q


def velocity_rows(held, at, first, row, top_rows):
    fresh = []
    for t in range(2):
        here = lambda f: held[f, t, at : at + 8]

        def pair(f):
            own, above = here(f), held[f, t, at + 1 : at + 9]
            if at == TOP - 8:
                above = jnp.where((row == 7) & top_rows, held[f, t, at + 2 : at + 10], above)
            if at == TOP:
                own = jnp.where((row == 0) & top_rows, held[f, t, at - 1 : at + 7], own)
            return own, above

        hw, hh = here(HWV), here(HHV)
        dp, ndp = pair(DP)
        ds, nds = pair(DS)
        as_, nas = pair(AS)
        am, nam = pair(AM)
        inertia, a, b = here(INE), here(AA), here(BB)
        x = inertia * here(U) + (hw * (dp + ndp) + hh * (nas - as_))
        y = inertia * here(V) + (hw * (ds + nds) + hh * (nam - am))
        u = a * x + b * y + here(KU)
        v = a * y - b * x + here(KV)
        held[U, t, at : at + 8] = u
        held[V, t, at : at + 8] = v
        fresh.append((u, v))
    (um, vm), (us, vs) = fresh
    velocity_sums(held, at, um, us, vm, vs, first)


def subcycles(held, start, stop, lo, hi):
    first, last, row, top_rows = stencil_masks()

    def body(_, carry):
        for g in range(lo, hi):
            stress_rows(held, PAD + 8 * g, last)
        for g in range(lo, hi):
            velocity_rows(held, PAD + 8 * g, first, row, top_rows)
        return carry

    lax.fori_loop(start, stop, body, 0)


def place_of(me, which):
    chip, core = me // 2, me % 2
    step = 1 - 2 * core
    if which >= 4:
        core = 1 - core
        which -= 4
        step = -step
    chips = (chip, lax.rem(chip - step + 4, 4), lax.rem(chip + step + 4, 4), lax.rem(chip + 2, 4))
    return (2 * chips[which] + core) * ROWS


def into(out, ref, place, sem):
    return pltpu.make_async_copy(ref, out.at[0, :, pl.ds(place, ROWS), :], sem)


def first_half_kernel(
    fields, from_west, from_east, from_below, from_above, snap, writer_hbm, held, out, flag, writer, zero, sems
):
    me = lax.axis_index("row")
    read = pltpu.make_async_copy(writer_hbm, writer, sems.at[8])
    read.start()
    zero[...] = jnp.zeros_like(zero)
    assemble(fields, from_west, from_east, from_below, from_above, held)
    read.wait()
    mine = writer[lax.axis_index("col")] == me
    flag[...] = jnp.where(mine, 1, 0) + jnp.zeros((8, LANES), jnp.int32)
    zeros = [into(out, zero, n * ROWS, sems.at[n]) for n in range(8)]
    own = into(out, snap, place_of(me, 0), sems.at[0])

    @pl.when(mine)
    def _():
        own.start()

    @pl.when(jnp.logical_not(mine))
    def _():
        for copy in zeros:
            copy.start()

    subcycles(held, 0, 5, 0, 12)
    subcycles(held, 5, SPLIT, 1, 11)

    @pl.when(mine)
    def _():
        own.wait()

    @pl.when(jnp.logical_not(mine))
    def _():
        for copy in zeros:
            copy.wait()


def second_half_kernel(state, out_in, flag, near, near_back, far, vel, stress, held, out, sems):
    me = lax.axis_index("row")
    mine = jnp.max(flag[...]) == 1
    copies = [
        into(out, near, place_of(me, 1), sems.at[0]),
        into(out, near_back, place_of(me, 2), sems.at[1]),
        into(out, far, place_of(me, 3), sems.at[2]),
    ]

    @pl.when(mine)
    def _():
        for copy in copies:
            copy.start()

    subcycles(held, SPLIT, SUB, 1, 11)
    at = PAD + HALO
    vel[0] = held[U, 0, at : at + ROWS]
    vel[1] = held[V, 0, at : at + ROWS]
    stress[0] = 2.0 * held[S1, 0, at : at + ROWS]
    stress[1] = 2.0 * held[S2, 0, at : at + ROWS]
    stress[2] = held[S12, 0, at : at + ROWS]

    @pl.when(mine)
    def _():
        for copy in copies:
            copy.wait()


def last_kernel(out_in, flag, partner, out, sems):
    me = lax.axis_index("row")
    mine = jnp.max(flag[...]) == 1

    @pl.when(mine)
    def _():
        copies = [into(out, partner.at[n], place_of(me, 4 + n), sems.at[n]) for n in range(4)]
        for copy in copies:
            copy.start()
        for copy in copies:
            copy.wait()


def join_kernel(own, near, near_back, far, joined):
    for n, block in enumerate((own, near, near_back, far)):
        joined[n] = block[...]


def vmem():
    return pl.BlockSpec(memory_space=pltpu.VMEM)


def shape(*dims):
    return jax.ShapeDtypeStruct(dims, jnp.float32)


def grant(mebibytes):
    return pltpu.CompilerParams(vmem_limit_bytes=mebibytes << 20)


def step(
    velocity_start,
    stress_start,
    wind_stress,
    ocean_current,
    ice_area,
    ice_volume,
    inverse_width,
    inverse_height,
    land_block,
    ice_block,
    writer,
):
    fields, to_west, to_east, snap = pl.pallas_call(
        prepare_kernel,
        out_shape=(
            shape(SENT, ROWS, LANES),
            shape(SENT * 8, LANES),
            shape(SENT * 8, LANES),
            shape(10, ROWS, LANES),
        ),
        in_specs=[pl.BlockSpec(memory_space=pltpu.HBM)] * 10,
        out_specs=(vmem(),) * 4,
        scratch_shapes=[
            pltpu.VMEM((2, ROWS, LANES), jnp.float32),
            pltpu.VMEM((3, ROWS, LANES), jnp.float32),
            pltpu.VMEM((2, ROWS, LANES), jnp.float32),
            pltpu.VMEM((2, ROWS, LANES), jnp.float32),
            pltpu.VMEM((ROWS, LANES), jnp.float32),
            pltpu.VMEM((ROWS, LANES), jnp.float32),
            pltpu.VMEM((4, 16), jnp.int32),
            pltpu.VMEM((4, 16), jnp.int32),
            pltpu.SemaphoreType.DMA((10,)),
        ],
        compiler_params=grant(8),
        name="prepare",
    )(
        *(
            pltpu.with_memory_space_constraint(value, pltpu.HBM)
            for value in (
                velocity_start,
                stress_start,
                wind_stress,
                ocean_current,
                ice_area,
                ice_volume,
                inverse_width,
                inverse_height,
                land_block.T,
                ice_block.T,
            )
        )
    )
    along = [(r, (r + 2 - 4 * (r % 2)) % 8) for r in range(8)]
    against = [(r, (r - 2 + 4 * (r % 2)) % 8) for r in range(8)]
    partner = [(r, r ^ 1) for r in range(8)]
    eastward = [(c, (c + 1) % 32) for c in range(32)]
    westward = [(c, (c - 1) % 32) for c in range(32)]
    upward = []
    for c in range(16):
        line = [32 * r + c for r in range(8)] + [32 * (7 - r) + 31 - c for r in range(8)]
        upward += list(zip(line[:-1], line[1:]))
    downward = [(b, a) for a, b in upward]

    near = lax.ppermute(snap, "row", along)
    from_west = lax.ppermute(to_east, "col", eastward)
    from_east = lax.ppermute(to_west, "col", westward)
    near_back = lax.ppermute(snap, "row", against)

    to_above, to_below = pl.pallas_call(
        rows_kernel,
        out_shape=(shape(MESSAGE, LANES),) * 2,
        in_specs=[vmem()] * 3,
        out_specs=(vmem(),) * 2,
        compiler_params=grant(8),
        cost_estimate=pl.CostEstimate(flops=1000000, bytes_accessed=1000000, transcendentals=0),
        name="rows",
    )(fields, from_west, from_east)
    from_below = lax.ppermute(to_above, ("row", "col"), upward)
    from_above = lax.ppermute(to_below, ("row", "col"), downward)
    far = lax.ppermute(near, "row", along)

    hbm = lambda: pl.BlockSpec(memory_space=pl.ANY)
    state, restart, flag = pl.pallas_call(
        first_half_kernel,
        out_shape=(
            shape(HELD, 2, TALL, LANES),
            shape(1, 10, 8 * ROWS, LANES),
            jax.ShapeDtypeStruct((8, LANES), jnp.int32),
        ),
        in_specs=[vmem()] * 5 + [hbm(), hbm()],
        out_specs=(vmem(), hbm(), vmem()),
        scratch_shapes=[
            pltpu.SMEM((32,), jnp.int32),
            pltpu.VMEM((10, ROWS, LANES), jnp.float32),
            pltpu.SemaphoreType.DMA((9,)),
        ],
        compiler_params=grant(16),
        cost_estimate=pl.CostEstimate(flops=20000000, bytes_accessed=2000000, transcendentals=0),
        name="first_half",
    )(
        fields,
        from_west,
        from_east,
        from_below,
        from_above,
        snap,
        pltpu.with_memory_space_constraint(writer, pltpu.HBM),
    )

    joined = pl.pallas_call(
        join_kernel,
        out_shape=shape(4, 10, ROWS, LANES),
        in_specs=[vmem()] * 4,
        out_specs=vmem(),
        compiler_params=grant(8),
        name="join",
    )(snap, near, near_back, far)
    partner_blocks = lax.ppermute(joined, "row", partner)

    velocity, stress, _, restart = pl.pallas_call(
        second_half_kernel,
        out_shape=(
            shape(2, ROWS, LANES),
            shape(3, ROWS, LANES),
            shape(HELD, 2, TALL, LANES),
            shape(1, 10, 8 * ROWS, LANES),
        ),
        in_specs=[vmem(), hbm(), vmem(), hbm(), hbm(), hbm()],
        out_specs=(vmem(), vmem(), vmem(), hbm()),
        input_output_aliases={0: 2, 1: 3},
        scratch_shapes=[pltpu.SemaphoreType.DMA((3,))],
        compiler_params=grant(8),
        cost_estimate=pl.CostEstimate(flops=20000000, bytes_accessed=2000000, transcendentals=0),
        name="second_half",
    )(state, restart, flag, near, near_back, far)

    restart = pl.pallas_call(
        last_kernel,
        out_shape=shape(1, 10, 8 * ROWS, LANES),
        in_specs=[hbm(), vmem(), hbm()],
        out_specs=hbm(),
        input_output_aliases={0: 0},
        scratch_shapes=[pltpu.SemaphoreType.DMA((4,))],
        compiler_params=grant(4),
        name="last",
    )(restart, flag, partner_blocks)
    return (velocity, stress, restart)


def solution(mesh):
    return jax.shard_map(
        step,
        mesh=mesh,
        in_specs=(
            P(None, "row", "col"),
            P(None, "row", "col"),
            P(None, "row", "col"),
            P(None, "row", "col"),
            P(None, "row", "col"),
            P(None, "row", "col"),
            P("row", "col"),
            P("row", "col"),
            P("row", "col"),
            P("row", "col"),
            P(),
        ),
        out_specs=(P(None, "row", "col"), P(None, "row", "col"), P("row", None, None, "col")),
        check_vma=False,
    )
```

```python
import jax
import jax.numpy as jnp
from jax import lax
from jax.experimental import pallas as pl
from jax.experimental.pallas import tpu as pltpu
from jax.sharding import PartitionSpec as P


SUB = 12
SPLIT = 7
ROWS = 64
LANES = 128
HALO = 16
PAD = 8
TALL = PAD + HALO + ROWS + HALO + PAD
TOP = PAD + HALO + ROWS

U, V, S1, S2, S12, STR, HW, HH, INE, AA, KU, KV = range(12)
SENT = 12
BB, HWV, HHV, DU, SU, DV, SV, DP, DS, AS, AM = range(12, 23)
HELD = 23
MOVING = (U, V, INE, AA, KU, KV)
NEGATED = (U, V, KU, KV)
MESSAGE = SENT * HALO + SENT // 2 * 8


def lane_index():
    return lax.broadcasted_iota(jnp.int32, (8, LANES), 1)


def row_index():
    return lax.broadcasted_iota(jnp.int32, (8, LANES), 0)


def turned(value, steps):
    steps = steps % LANES
    return value if steps == 0 else pltpu.roll(value, steps, 1)


def west(main, side, first):
    a, b = turned(main, 1), turned(side, 1)
    return jnp.where(first, b, a), jnp.where(first, a, b)


def east(main, side, last):
    a, b = turned(main, -1), turned(side, -1)
    return jnp.where(last, b, a), jnp.where(last, a, b)


def expanded(blocks_t):
    rows = lax.broadcasted_iota(jnp.int32, (ROWS, 16), 0) // 4
    pick_rows = (rows == lax.broadcasted_iota(jnp.int32, (ROWS, 16), 1)).astype(jnp.float32)
    lanes = lax.broadcasted_iota(jnp.int32, (4, LANES), 1) // 32
    pick_lanes = (lanes == lax.broadcasted_iota(jnp.int32, (4, LANES), 0)).astype(jnp.float32)
    half = lax.dot_general(
        pick_rows, blocks_t, (((1,), (1,)), ((), ())), preferred_element_type=jnp.float32
    )
    return lax.dot_general(
        half, pick_lanes, (((1,), (0,)), ((), ())), preferred_element_type=jnp.float32
    )


def prepare_kernel(
    vel_hbm,
    stress_hbm,
    wind_hbm,
    ocean_hbm,
    area_hbm,
    volume_hbm,
    wide_hbm,
    high_hbm,
    land_hbm,
    ice_hbm,
    fields,
    to_west,
    to_east,
    snap,
    vel,
    stress,
    wind,
    ocean,
    wide,
    high,
    land_t,
    ice_t,
    sems,
):
    area, volume = snap.at[0:5], snap.at[5:10]
    moves = (
        (area_hbm, area),
        (volume_hbm, volume),
        (land_hbm, land_t),
        (ice_hbm, ice_t),
        (ocean_hbm, ocean),
        (wind_hbm, wind),
        (stress_hbm, stress),
        (vel_hbm, vel),
        (wide_hbm, wide),
        (high_hbm, high),
    )
    copies = [pltpu.make_async_copy(a, b, sems.at[n]) for n, (a, b) in enumerate(moves)]
    for copy in copies:
        copy.start()
    for copy in copies:
        copy.wait()
    land = expanded(land_t[...].astype(jnp.float32))
    ice = expanded(ice_t[...].astype(jnp.float32))
    area_total = area[0] + area[1] + area[2] + area[3] + area[4]
    volume_total = volume[0] + volume[1] + volume[2] + volume[3] + volume[4]
    fields[U] = vel[0]
    fields[V] = vel[1]
    fields[S1] = 0.5 * stress[0]
    fields[S2] = 0.5 * stress[1]
    fields[S12] = stress[2]
    fields[STR] = (4.0 / 6.0) * volume_total * jnp.exp(-20.0 * (1.0 - area_total)) * land
    fields[HW] = 0.5 * wide[...]
    fields[HH] = 0.5 * high[...]
    inertia = 16.0 * (1.0 + volume_total)
    turning = 0.5 * (1.0 + volume_total)
    damped = inertia + 1.0
    scale = land * ice / (damped * damped + turning * turning)
    still = land * (1.0 - ice)
    fx = wind[0] + ocean[0]
    fy = wind[1] + ocean[1]
    fields[INE] = inertia
    fields[AA] = scale
    fields[KU] = scale * (damped * fx + turning * fy) + still * ocean[0]
    fields[KV] = scale * (damped * fy - turning * fx) + still * ocean[1]
    lane = lane_index()
    for f in range(SENT):
        left = right = None
        for g in range(8):
            part = fields[f, 8 * g : 8 * g + 8]
            inside = (lane >= 16 * g) & (lane < 16 * g + 16)
            a = turned(part, 16 * g)
            b = turned(part, 16 * g - 112)
            left = a if g == 0 else jnp.where(inside, a, left)
            right = b if g == 0 else jnp.where(inside, b, right)
        to_west[8 * f : 8 * f + 8] = left
        to_east[8 * f : 8 * f + 8] = right


def rows_kernel(fields, from_west, from_east, outer, inner):
    lane = lane_index()
    odd = lax.axis_index("row") % 2 == 1

    def fill(to_north, to_south):
        for f in range(SENT):
            to_north[HALO * f : HALO * f + HALO] = fields[f, ROWS - HALO : ROWS]
            to_south[HALO * f : HALO * f + HALO] = fields[f, 0:HALO]
        for pair in range(SENT // 2):
            north = south = None
            for member in range(2):
                f = 2 * pair + member
                base = 64 * member
                a = from_west[8 * f : 8 * f + 8]
                b = from_east[8 * f : 8 * f + 8]
                here = lane >= base
                there = lane >= base + 32
                n = jnp.where(there, turned(b, base + 32 - 96), turned(a, base - 96))
                s = jnp.where(there, turned(b, base + 32), turned(a, base))
                north = n if member == 0 else jnp.where(here, n, north)
                south = s if member == 0 else jnp.where(here, s, south)
            at = SENT * HALO + 8 * pair
            to_north[at : at + 8] = north
            to_south[at : at + 8] = south

    @pl.when(odd)
    def _():
        fill(outer, inner)

    @pl.when(jnp.logical_not(odd))
    def _():
        fill(inner, outer)


def stencil_masks():
    lane, row = lane_index(), row_index()
    is_top = lax.axis_index("row") == 7
    top_rows = (jnp.where(is_top, 1, 0) + jnp.zeros((8, LANES), jnp.int32)) == 1
    return lane == 0, lane == LANES - 1, row, top_rows


def assemble(fields, from_west, from_east, from_outer, from_inner, held):
    is_top = lax.axis_index("row") == 7
    odd = lax.axis_index("row") % 2 + jnp.zeros((8, LANES), jnp.int32) == 1
    lane = lane_index()
    row = row_index()
    first, last, low = lane == 0, lane == LANES - 1, lane < 64

    def south(at):
        return jnp.where(odd, from_inner[at : at + 8], from_outer[at : at + 8])

    def north(at):
        return jnp.where(odd, from_outer[at : at + 8], from_inner[at : at + 8])

    def side_rows(message, f, a):
        base = 64 * (f % 2)
        corner = message(SENT * HALO + 8 * (f // 2))
        return jnp.where(low, turned(corner, -(base + 32 + 16 * a)), turned(corner, 112 - base - 16 * a))

    for f in range(SENT):
        a, b = from_west[8 * f : 8 * f + 8], from_east[8 * f : 8 * f + 8]
        for g in range(8):
            at = PAD + HALO + 8 * g
            held[f, 0, at : at + 8] = fields[f, 8 * g : 8 * g + 8]
            held[f, 1, at : at + 8] = jnp.where(low, turned(b, -16 * g), turned(a, 112 - 16 * g))
        for g in range(2):
            at = PAD + 8 * g
            held[f, 0, at : at + 8] = south(HALO * f + 8 * g)
            held[f, 1, at : at + 8] = side_rows(south, f, g)

    @pl.when(jnp.logical_not(is_top))
    def _():
        for f in range(SENT):
            for g in range(2):
                at = TOP + 8 * g
                held[f, 0, at : at + 8] = north(HALO * f + 8 * g)
                held[f, 1, at : at + 8] = side_rows(north, f, g)

    @pl.when(is_top)
    def _():
        def rotated(value):
            value = jnp.take_along_axis(value, LANES - 1 - lane, axis=1)
            return jnp.take_along_axis(value, 7 - row, axis=0)

        for f in range(SENT):
            for g in range(2):
                source = 1 - g
                main = rotated(north(HALO * f + 8 * source))
                side = rotated(side_rows(north, f, source))
                if f in MOVING:
                    main, side = east(main, side, last)
                    if f in NEGATED:
                        main, side = -main, -side
                    at = TOP + 8 * g
                else:
                    at = TOP + 1 + 8 * g
                held[f, 0, at : at + 8] = main
                held[f, 1, at : at + 8] = side
                if f in (HW, HH):
                    main, side = east(main, side, last)
                    own = HWV if f == HW else HHV
                    held[own, 0, TOP + 8 * g : TOP + 8 * g + 8] = main
                    held[own, 1, TOP + 8 * g : TOP + 8 * g + 8] = side

    for g in range(12):
        at = PAD + 8 * g
        for t in range(2):
            scale = held[AA, t, at : at + 8]
            inertia = held[INE, t, at : at + 8]
            held[AA, t, at : at + 8] = (inertia + 1.0) * scale
            held[BB, t, at : at + 8] = (inertia * (1.0 / 32.0)) * scale
            if g < 10:
                held[HWV, t, at : at + 8] = held[HW, t, at : at + 8]
                held[HHV, t, at : at + 8] = held[HH, t, at : at + 8]
        velocity_sums(
            held,
            at,
            held[U, 0, at : at + 8],
            held[U, 1, at : at + 8],
            held[V, 0, at : at + 8],
            held[V, 1, at : at + 8],
            first,
        )

    @pl.when(jnp.logical_not(is_top))
    def _():
        for t in range(2):
            held[HWV, t, TOP : TOP + HALO] = held[HW, t, TOP : TOP + HALO]
            held[HHV, t, TOP : TOP + HALO] = held[HH, t, TOP : TOP + HALO]


def velocity_sums(held, at, um, us, vm, vs, first):
    wum, wus = west(um, us, first)
    wvm, wvs = west(vm, vs, first)
    for t, (x, wx, y, wy) in enumerate(((um, wum, vm, wvm), (us, wus, vs, wvs))):
        held[DU, t, at : at + 8] = x - wx
        held[SU, t, at : at + 8] = x + wx
        held[DV, t, at : at + 8] = y - wy
        held[SV, t, at : at + 8] = y + wy


def stress_rows(held, at, last):
    fresh = []
    for t in range(2):
        here = lambda f: held[f, t, at : at + 8]
        below = lambda f: held[f, t, at - 1 : at + 7]
        hw, hh = here(HW), here(HH)
        gux = hw * (here(DU) + below(DU))
        guy = hh * (here(SU) - below(SU))
        gvx = hw * (here(DV) + below(DV))
        gvy = hh * (here(SV) - below(SV))
        divergence = gux + gvy
        tension = gux - gvy
        shearing = guy + gvx
        deform = jnp.sqrt(
            divergence * divergence + 0.25 * (tension * tension + shearing * shearing)
        )
        viscous = here(STR) / (deform + 0.5)
        quarter = 0.25 * viscous
        s1 = here(S1) * (2.0 / 3.0) + viscous * (divergence - deform)
        s2 = here(S2) * (2.0 / 3.0) + quarter * tension
        s12 = here(S12) * (2.0 / 3.0) + quarter * shearing
        held[S1, t, at : at + 8] = s1
        held[S2, t, at : at + 8] = s2
        held[S12, t, at : at + 8] = s12
        fresh.append((s1 + s2, s1 - s2, s12))
    (pm, mm, qm), (ps, ms, qs) = fresh
    epm, eps = east(pm, ps, last)
    emm, ems = east(mm, ms, last)
    eqm, eqs = east(qm, qs, last)
    for t, (p, ep, m, em, q, eq) in enumerate(
        ((pm, epm, mm, emm, qm, eqm), (ps, eps, ms, ems, qs, eqs))
    ):
        held[DP, t, at : at + 8] = ep - p
        held[AM, t, at : at + 8] = em + m
        held[DS, t, at : at + 8] = eq - q
        held[AS, t, at : at + 8] = eq + q


def velocity_rows(held, at, first, row, top_rows):
    fresh = []
    for t in range(2):
        here = lambda f: held[f, t, at : at + 8]

        def pair(f):
            own, above = here(f), held[f, t, at + 1 : at + 9]
            if at == TOP - 8:
                above = jnp.where((row == 7) & top_rows, held[f, t, at + 2 : at + 10], above)
            if at == TOP:
                own = jnp.where((row == 0) & top_rows, held[f, t, at - 1 : at + 7], own)
            return own, above

        hw, hh = here(HWV), here(HHV)
        dp, ndp = pair(DP)
        ds, nds = pair(DS)
        as_, nas = pair(AS)
        am, nam = pair(AM)
        inertia, a, b = here(INE), here(AA), here(BB)
        x = inertia * here(U) + (hw * (dp + ndp) + hh * (nas - as_))
        y = inertia * here(V) + (hw * (ds + nds) + hh * (nam - am))
        u = a * x + b * y + here(KU)
        v = a * y - b * x + here(KV)
        held[U, t, at : at + 8] = u
        held[V, t, at : at + 8] = v
        fresh.append((u, v))
    (um, vm), (us, vs) = fresh
    velocity_sums(held, at, um, us, vm, vs, first)


def subcycles(held, start, stop, lo, hi):
    first, last, row, top_rows = stencil_masks()

    def body(_, carry):
        for g in range(lo, hi):
            stress_rows(held, PAD + 8 * g, last)
        for g in range(lo, hi):
            velocity_rows(held, PAD + 8 * g, first, row, top_rows)
        return carry

    lax.fori_loop(start, stop, body, 0)


def place_of(me, which):
    chip, core = me // 2, me % 2
    step = 1 - 2 * core
    if which >= 4:
        core = 1 - core
        which -= 4
        step = -step
    chips = (chip, lax.rem(chip - step + 4, 4), lax.rem(chip + step + 4, 4), lax.rem(chip + 2, 4))
    return (2 * chips[which] + core) * ROWS


def into(out, ref, place, sem):
    return pltpu.make_async_copy(ref, out.at[0, :, pl.ds(place, ROWS), :], sem)


def first_half_kernel(
    fields, from_west, from_east, from_outer, from_inner, snap, writer_hbm, held, out, flag, writer, zero, sems
):
    me = lax.axis_index("row")
    read = pltpu.make_async_copy(writer_hbm, writer, sems.at[8])
    read.start()
    zero[...] = jnp.zeros_like(zero)
    assemble(fields, from_west, from_east, from_outer, from_inner, held)
    read.wait()
    mine = writer[lax.axis_index("col")] == me
    flag[...] = jnp.where(mine, 1, 0) + jnp.zeros((8, LANES), jnp.int32)
    zeros = [into(out, zero, n * ROWS, sems.at[n]) for n in range(8)]
    own = into(out, snap, place_of(me, 0), sems.at[0])

    @pl.when(mine)
    def _():
        own.start()

    @pl.when(jnp.logical_not(mine))
    def _():
        for copy in zeros:
            copy.start()

    subcycles(held, 0, 5, 0, 12)
    subcycles(held, 5, SPLIT, 1, 11)

    @pl.when(mine)
    def _():
        own.wait()

    @pl.when(jnp.logical_not(mine))
    def _():
        for copy in zeros:
            copy.wait()


def second_half_kernel(state, out_in, flag, near, near_back, far, vel, stress, held, out, sems):
    me = lax.axis_index("row")
    mine = jnp.max(flag[...]) == 1
    copies = [
        into(out, near, place_of(me, 1), sems.at[0]),
        into(out, near_back, place_of(me, 2), sems.at[1]),
        into(out, far, place_of(me, 3), sems.at[2]),
    ]

    @pl.when(mine)
    def _():
        for copy in copies:
            copy.start()

    subcycles(held, SPLIT, SUB, 1, 11)
    at = PAD + HALO
    vel[0] = held[U, 0, at : at + ROWS]
    vel[1] = held[V, 0, at : at + ROWS]
    stress[0] = 2.0 * held[S1, 0, at : at + ROWS]
    stress[1] = 2.0 * held[S2, 0, at : at + ROWS]
    stress[2] = held[S12, 0, at : at + ROWS]

    @pl.when(mine)
    def _():
        for copy in copies:
            copy.wait()


def last_kernel(out_in, flag, partner, out, sems):
    me = lax.axis_index("row")
    mine = jnp.max(flag[...]) == 1

    @pl.when(mine)
    def _():
        copies = [into(out, partner.at[n], place_of(me, 4 + n), sems.at[n]) for n in range(4)]
        for copy in copies:
            copy.start()
        for copy in copies:
            copy.wait()


def join_kernel(own, near, near_back, far, joined):
    for n, block in enumerate((own, near, near_back, far)):
        joined[n] = block[...]


def vmem():
    return pl.BlockSpec(memory_space=pltpu.VMEM)


def shape(*dims):
    return jax.ShapeDtypeStruct(dims, jnp.float32)


def grant(mebibytes):
    return pltpu.CompilerParams(vmem_limit_bytes=mebibytes << 20)


def step(
    velocity_start,
    stress_start,
    wind_stress,
    ocean_current,
    ice_area,
    ice_volume,
    inverse_width,
    inverse_height,
    land_block,
    ice_block,
    writer,
):
    fields, to_west, to_east, snap = pl.pallas_call(
        prepare_kernel,
        out_shape=(
            shape(SENT, ROWS, LANES),
            shape(SENT * 8, LANES),
            shape(SENT * 8, LANES),
            shape(10, ROWS, LANES),
        ),
        in_specs=[pl.BlockSpec(memory_space=pltpu.HBM)] * 10,
        out_specs=(vmem(),) * 4,
        scratch_shapes=[
            pltpu.VMEM((2, ROWS, LANES), jnp.float32),
            pltpu.VMEM((3, ROWS, LANES), jnp.float32),
            pltpu.VMEM((2, ROWS, LANES), jnp.float32),
            pltpu.VMEM((2, ROWS, LANES), jnp.float32),
            pltpu.VMEM((ROWS, LANES), jnp.float32),
            pltpu.VMEM((ROWS, LANES), jnp.float32),
            pltpu.VMEM((4, 16), jnp.int32),
            pltpu.VMEM((4, 16), jnp.int32),
            pltpu.SemaphoreType.DMA((10,)),
        ],
        compiler_params=grant(8),
        name="prepare",
    )(
        *(
            pltpu.with_memory_space_constraint(value, pltpu.HBM)
            for value in (
                velocity_start,
                stress_start,
                wind_stress,
                ocean_current,
                ice_area,
                ice_volume,
                inverse_width,
                inverse_height,
                land_block.T,
                ice_block.T,
            )
        )
    )
    along = [(r, (r + 2 - 4 * (r % 2)) % 8) for r in range(8)]
    against = [(r, (r - 2 + 4 * (r % 2)) % 8) for r in range(8)]
    partner = [(r, r ^ 1) for r in range(8)]
    eastward = [(c, (c + 1) % 32) for c in range(32)]
    westward = [(c, (c - 1) % 32) for c in range(32)]
    across = [(7 * 32 + c, 7 * 32 + 31 - c) for c in range(32)]
    for c in range(32):
        for r in (1, 3, 5):
            across += [(32 * r + c, 32 * r + 32 + c), (32 * r + 32 + c, 32 * r + c)]

    near = lax.ppermute(snap, "row", along)
    from_west = lax.ppermute(to_east, "col", eastward)
    from_east = lax.ppermute(to_west, "col", westward)
    near_back = lax.ppermute(snap, "row", against)

    outer, inner = pl.pallas_call(
        rows_kernel,
        out_shape=(shape(MESSAGE, LANES),) * 2,
        in_specs=[vmem()] * 3,
        out_specs=(vmem(),) * 2,
        compiler_params=grant(8),
        cost_estimate=pl.CostEstimate(flops=1000000, bytes_accessed=1000000, transcendentals=0),
        name="rows",
    )(fields, from_west, from_east)
    from_outer = lax.ppermute(outer, ("row", "col"), across)
    from_inner = lax.ppermute(inner, "row", partner)
    far = lax.ppermute(near, "row", along)

    hbm = lambda: pl.BlockSpec(memory_space=pl.ANY)
    state, restart, flag = pl.pallas_call(
        first_half_kernel,
        out_shape=(
            shape(HELD, 2, TALL, LANES),
            shape(1, 10, 8 * ROWS, LANES),
            jax.ShapeDtypeStruct((8, LANES), jnp.int32),
        ),
        in_specs=[vmem()] * 5 + [hbm(), hbm()],
        out_specs=(vmem(), hbm(), vmem()),
        scratch_shapes=[
            pltpu.SMEM((32,), jnp.int32),
            pltpu.VMEM((10, ROWS, LANES), jnp.float32),
            pltpu.SemaphoreType.DMA((9,)),
        ],
        compiler_params=grant(16),
        cost_estimate=pl.CostEstimate(flops=20000000, bytes_accessed=2000000, transcendentals=0),
        name="first_half",
    )(
        fields,
        from_west,
        from_east,
        from_outer,
        from_inner,
        snap,
        pltpu.with_memory_space_constraint(writer, pltpu.HBM),
    )

    joined = pl.pallas_call(
        join_kernel,
        out_shape=shape(4, 10, ROWS, LANES),
        in_specs=[vmem()] * 4,
        out_specs=vmem(),
        compiler_params=grant(8),
        name="join",
    )(snap, near, near_back, far)
    partner_blocks = lax.ppermute(joined, "row", partner)

    velocity, stress, _, restart = pl.pallas_call(
        second_half_kernel,
        out_shape=(
            shape(2, ROWS, LANES),
            shape(3, ROWS, LANES),
            shape(HELD, 2, TALL, LANES),
            shape(1, 10, 8 * ROWS, LANES),
        ),
        in_specs=[vmem(), hbm(), vmem(), hbm(), hbm(), hbm()],
        out_specs=(vmem(), vmem(), vmem(), hbm()),
        input_output_aliases={0: 2, 1: 3},
        scratch_shapes=[pltpu.SemaphoreType.DMA((3,))],
        compiler_params=grant(8),
        cost_estimate=pl.CostEstimate(flops=20000000, bytes_accessed=2000000, transcendentals=0),
        name="second_half",
    )(state, restart, flag, near, near_back, far)

    restart = pl.pallas_call(
        last_kernel,
        out_shape=shape(1, 10, 8 * ROWS, LANES),
        in_specs=[hbm(), vmem(), hbm()],
        out_specs=hbm(),
        input_output_aliases={0: 0},
        scratch_shapes=[pltpu.SemaphoreType.DMA((4,))],
        compiler_params=grant(4),
        name="last",
    )(restart, flag, partner_blocks)
    return (velocity, stress, restart)


def solution(mesh):
    return jax.shard_map(
        step,
        mesh=mesh,
        in_specs=(
            P(None, "row", "col"),
            P(None, "row", "col"),
            P(None, "row", "col"),
            P(None, "row", "col"),
            P(None, "row", "col"),
            P(None, "row", "col"),
            P("row", "col"),
            P("row", "col"),
            P("row", "col"),
            P("row", "col"),
            P(),
        ),
        out_specs=(P(None, "row", "col"), P(None, "row", "col"), P("row", None, None, "col")),
        check_vma=False,
    )
```

```python
import jax
import jax.numpy as jnp
from jax import lax
from jax.experimental import pallas as pl
from jax.experimental.pallas import tpu as pltpu
from jax.sharding import PartitionSpec as P


SUB = 12
SPLIT = 7
ROWS = 64
LANES = 128
HALO = 16
PAD = 8
TALL = PAD + HALO + ROWS + HALO + PAD
TOP = PAD + HALO + ROWS

U, V, S1, S2, S12, STR, HW, HH, INE, AA, KU, KV = range(12)
SENT = 12
BB, HWV, HHV, DU, SU, DV, SV, DP, DS, AS, AM = range(12, 23)
HELD = 23
MOVING = (U, V, INE, AA, KU, KV)
NEGATED = (U, V, KU, KV)
MESSAGE = SENT * HALO + SENT // 2 * 8


def lane_index():
    return lax.broadcasted_iota(jnp.int32, (8, LANES), 1)


def row_index():
    return lax.broadcasted_iota(jnp.int32, (8, LANES), 0)


def turned(value, steps):
    steps = steps % LANES
    return value if steps == 0 else pltpu.roll(value, steps, 1)


def west(main, side, first):
    a, b = turned(main, 1), turned(side, 1)
    return jnp.where(first, b, a), jnp.where(first, a, b)


def east(main, side, last):
    a, b = turned(main, -1), turned(side, -1)
    return jnp.where(last, b, a), jnp.where(last, a, b)


def expanded(blocks_t):
    rows = lax.broadcasted_iota(jnp.int32, (ROWS, 16), 0) // 4
    pick_rows = (rows == lax.broadcasted_iota(jnp.int32, (ROWS, 16), 1)).astype(jnp.float32)
    lanes = lax.broadcasted_iota(jnp.int32, (4, LANES), 1) // 32
    pick_lanes = (lanes == lax.broadcasted_iota(jnp.int32, (4, LANES), 0)).astype(jnp.float32)
    half = lax.dot_general(
        pick_rows, blocks_t, (((1,), (1,)), ((), ())), preferred_element_type=jnp.float32
    )
    return lax.dot_general(
        half, pick_lanes, (((1,), (0,)), ((), ())), preferred_element_type=jnp.float32
    )


def prepare_kernel(
    vel_hbm,
    stress_hbm,
    wind_hbm,
    ocean_hbm,
    area_hbm,
    volume_hbm,
    wide_hbm,
    high_hbm,
    land_hbm,
    ice_hbm,
    fields,
    to_west,
    to_east,
    snap,
    vel,
    stress,
    wind,
    ocean,
    wide,
    high,
    land_t,
    ice_t,
    sems,
):
    area, volume = snap.at[0:5], snap.at[5:10]
    moves = (
        (area_hbm, area),
        (volume_hbm, volume),
        (land_hbm, land_t),
        (ice_hbm, ice_t),
        (ocean_hbm, ocean),
        (wind_hbm, wind),
        (stress_hbm, stress),
        (vel_hbm, vel),
        (wide_hbm, wide),
        (high_hbm, high),
    )
    copies = [pltpu.make_async_copy(a, b, sems.at[n]) for n, (a, b) in enumerate(moves)]
    for copy in copies:
        copy.start()
    for copy in copies:
        copy.wait()
    land = expanded(land_t[...].astype(jnp.float32))
    ice = expanded(ice_t[...].astype(jnp.float32))
    area_total = area[0] + area[1] + area[2] + area[3] + area[4]
    volume_total = volume[0] + volume[1] + volume[2] + volume[3] + volume[4]
    fields[U] = vel[0]
    fields[V] = vel[1]
    fields[S1] = 0.5 * stress[0]
    fields[S2] = 0.5 * stress[1]
    fields[S12] = stress[2]
    fields[STR] = (4.0 / 6.0) * volume_total * jnp.exp(-20.0 * (1.0 - area_total)) * land
    fields[HW] = 0.5 * wide[...]
    fields[HH] = 0.5 * high[...]
    inertia = 16.0 * (1.0 + volume_total)
    turning = 0.5 * (1.0 + volume_total)
    damped = inertia + 1.0
    scale = land * ice / (damped * damped + turning * turning)
    still = land * (1.0 - ice)
    fx = wind[0] + ocean[0]
    fy = wind[1] + ocean[1]
    fields[INE] = inertia
    fields[AA] = scale
    fields[KU] = scale * (damped * fx + turning * fy) + still * ocean[0]
    fields[KV] = scale * (damped * fy - turning * fx) + still * ocean[1]
    lane = lane_index()
    for f in range(SENT):
        left = right = None
        for g in range(8):
            part = fields[f, 8 * g : 8 * g + 8]
            inside = (lane >= 16 * g) & (lane < 16 * g + 16)
            a = turned(part, 16 * g)
            b = turned(part, 16 * g - 112)
            left = a if g == 0 else jnp.where(inside, a, left)
            right = b if g == 0 else jnp.where(inside, b, right)
        to_west[8 * f : 8 * f + 8] = left
        to_east[8 * f : 8 * f + 8] = right


def rows_kernel(fields, from_west, from_east, outer, inner):
    lane = lane_index()
    odd = lax.axis_index("row") % 2 == 1

    def fill(to_north, to_south):
        for f in range(SENT):
            to_north[HALO * f : HALO * f + HALO] = fields[f, ROWS - HALO : ROWS]
            to_south[HALO * f : HALO * f + HALO] = fields[f, 0:HALO]
        for pair in range(SENT // 2):
            north = south = None
            for member in range(2):
                f = 2 * pair + member
                base = 64 * member
                a = from_west[8 * f : 8 * f + 8]
                b = from_east[8 * f : 8 * f + 8]
                here = lane >= base
                there = lane >= base + 32
                n = jnp.where(there, turned(b, base + 32 - 96), turned(a, base - 96))
                s = jnp.where(there, turned(b, base + 32), turned(a, base))
                north = n if member == 0 else jnp.where(here, n, north)
                south = s if member == 0 else jnp.where(here, s, south)
            at = SENT * HALO + 8 * pair
            to_north[at : at + 8] = north
            to_south[at : at + 8] = south

    @pl.when(odd)
    def _():
        fill(outer, inner)

    @pl.when(jnp.logical_not(odd))
    def _():
        fill(inner, outer)


def stencil_masks():
    lane, row = lane_index(), row_index()
    is_top = lax.axis_index("row") == 7
    top_rows = (jnp.where(is_top, 1, 0) + jnp.zeros((8, LANES), jnp.int32)) == 1
    return lane == 0, lane == LANES - 1, row, top_rows


def assemble(fields, from_west, from_east, from_outer, from_inner, held):
    is_top = lax.axis_index("row") == 7
    odd = lax.axis_index("row") % 2 + jnp.zeros((8, LANES), jnp.int32) == 1
    lane = lane_index()
    row = row_index()
    first, last, low = lane == 0, lane == LANES - 1, lane < 64

    bottom = lax.axis_index("row") + jnp.zeros((8, LANES), jnp.int32) == 0

    def south(at):
        value = jnp.where(odd, from_inner[at : at + 8], from_outer[at : at + 8])
        return jnp.where(bottom, 0.0, value)

    def north(at):
        return jnp.where(odd, from_outer[at : at + 8], from_inner[at : at + 8])

    def side_rows(message, f, a):
        base = 64 * (f % 2)
        corner = message(SENT * HALO + 8 * (f // 2))
        return jnp.where(low, turned(corner, -(base + 32 + 16 * a)), turned(corner, 112 - base - 16 * a))

    for f in range(SENT):
        a, b = from_west[8 * f : 8 * f + 8], from_east[8 * f : 8 * f + 8]
        for g in range(8):
            at = PAD + HALO + 8 * g
            held[f, 0, at : at + 8] = fields[f, 8 * g : 8 * g + 8]
            held[f, 1, at : at + 8] = jnp.where(low, turned(b, -16 * g), turned(a, 112 - 16 * g))
        for g in range(2):
            at = PAD + 8 * g
            held[f, 0, at : at + 8] = south(HALO * f + 8 * g)
            held[f, 1, at : at + 8] = side_rows(south, f, g)

    @pl.when(jnp.logical_not(is_top))
    def _():
        for f in range(SENT):
            for g in range(2):
                at = TOP + 8 * g
                held[f, 0, at : at + 8] = north(HALO * f + 8 * g)
                held[f, 1, at : at + 8] = side_rows(north, f, g)

    @pl.when(is_top)
    def _():
        def rotated(value):
            value = jnp.take_along_axis(value, LANES - 1 - lane, axis=1)
            return jnp.take_along_axis(value, 7 - row, axis=0)

        for f in range(SENT):
            for g in range(2):
                source = 1 - g
                main = rotated(north(HALO * f + 8 * source))
                side = rotated(side_rows(north, f, source))
                if f in MOVING:
                    main, side = east(main, side, last)
                    if f in NEGATED:
                        main, side = -main, -side
                    at = TOP + 8 * g
                else:
                    at = TOP + 1 + 8 * g
                held[f, 0, at : at + 8] = main
                held[f, 1, at : at + 8] = side
                if f in (HW, HH):
                    main, side = east(main, side, last)
                    own = HWV if f == HW else HHV
                    held[own, 0, TOP + 8 * g : TOP + 8 * g + 8] = main
                    held[own, 1, TOP + 8 * g : TOP + 8 * g + 8] = side

    for g in range(12):
        at = PAD + 8 * g
        for t in range(2):
            scale = held[AA, t, at : at + 8]
            inertia = held[INE, t, at : at + 8]
            held[AA, t, at : at + 8] = (inertia + 1.0) * scale
            held[BB, t, at : at + 8] = (inertia * (1.0 / 32.0)) * scale
            if g < 10:
                held[HWV, t, at : at + 8] = held[HW, t, at : at + 8]
                held[HHV, t, at : at + 8] = held[HH, t, at : at + 8]
        velocity_sums(
            held,
            at,
            held[U, 0, at : at + 8],
            held[U, 1, at : at + 8],
            held[V, 0, at : at + 8],
            held[V, 1, at : at + 8],
            first,
        )

    @pl.when(jnp.logical_not(is_top))
    def _():
        for t in range(2):
            held[HWV, t, TOP : TOP + HALO] = held[HW, t, TOP : TOP + HALO]
            held[HHV, t, TOP : TOP + HALO] = held[HH, t, TOP : TOP + HALO]


def velocity_sums(held, at, um, us, vm, vs, first):
    wum, wus = west(um, us, first)
    wvm, wvs = west(vm, vs, first)
    for t, (x, wx, y, wy) in enumerate(((um, wum, vm, wvm), (us, wus, vs, wvs))):
        held[DU, t, at : at + 8] = x - wx
        held[SU, t, at : at + 8] = x + wx
        held[DV, t, at : at + 8] = y - wy
        held[SV, t, at : at + 8] = y + wy


def stress_rows(held, at, last):
    fresh = []
    for t in range(2):
        here = lambda f: held[f, t, at : at + 8]
        below = lambda f: held[f, t, at - 1 : at + 7]
        hw, hh = here(HW), here(HH)
        gux = hw * (here(DU) + below(DU))
        guy = hh * (here(SU) - below(SU))
        gvx = hw * (here(DV) + below(DV))
        gvy = hh * (here(SV) - below(SV))
        divergence = gux + gvy
        tension = gux - gvy
        shearing = guy + gvx
        deform = jnp.sqrt(
            divergence * divergence + 0.25 * (tension * tension + shearing * shearing)
        )
        viscous = here(STR) / (deform + 0.5)
        quarter = 0.25 * viscous
        s1 = here(S1) * (2.0 / 3.0) + viscous * (divergence - deform)
        s2 = here(S2) * (2.0 / 3.0) + quarter * tension
        s12 = here(S12) * (2.0 / 3.0) + quarter * shearing
        held[S1, t, at : at + 8] = s1
        held[S2, t, at : at + 8] = s2
        held[S12, t, at : at + 8] = s12
        fresh.append((s1 + s2, s1 - s2, s12))
    (pm, mm, qm), (ps, ms, qs) = fresh
    epm, eps = east(pm, ps, last)
    emm, ems = east(mm, ms, last)
    eqm, eqs = east(qm, qs, last)
    for t, (p, ep, m, em, q, eq) in enumerate(
        ((pm, epm, mm, emm, qm, eqm), (ps, eps, ms, ems, qs, eqs))
    ):
        held[DP, t, at : at + 8] = ep - p
        held[AM, t, at : at + 8] = em + m
        held[DS, t, at : at + 8] = eq - q
        held[AS, t, at : at + 8] = eq + q


def velocity_rows(held, at, first, row, top_rows):
    fresh = []
    for t in range(2):
        here = lambda f: held[f, t, at : at + 8]

        def pair(f):
            own, above = here(f), held[f, t, at + 1 : at + 9]
            if at == TOP - 8:
                above = jnp.where((row == 7) & top_rows, held[f, t, at + 2 : at + 10], above)
            if at == TOP:
                own = jnp.where((row == 0) & top_rows, held[f, t, at - 1 : at + 7], own)
            return own, above

        hw, hh = here(HWV), here(HHV)
        dp, ndp = pair(DP)
        ds, nds = pair(DS)
        as_, nas = pair(AS)
        am, nam = pair(AM)
        inertia, a, b = here(INE), here(AA), here(BB)
        x = inertia * here(U) + (hw * (dp + ndp) + hh * (nas - as_))
        y = inertia * here(V) + (hw * (ds + nds) + hh * (nam - am))
        u = a * x + b * y + here(KU)
        v = a * y - b * x + here(KV)
        held[U, t, at : at + 8] = u
        held[V, t, at : at + 8] = v
        fresh.append((u, v))
    (um, vm), (us, vs) = fresh
    velocity_sums(held, at, um, us, vm, vs, first)


def subcycles(held, start, stop, lo, hi):
    first, last, row, top_rows = stencil_masks()

    def body(_, carry):
        for g in range(lo, hi):
            stress_rows(held, PAD + 8 * g, last)
        for g in range(lo, hi):
            velocity_rows(held, PAD + 8 * g, first, row, top_rows)
        return carry

    lax.fori_loop(start, stop, body, 0)


def place_of(me, which):
    chip, core = me // 2, me % 2
    step = 1 - 2 * core
    if which >= 4:
        core = 1 - core
        which -= 4
        step = -step
    chips = (chip, lax.rem(chip - step + 4, 4), lax.rem(chip + step + 4, 4), lax.rem(chip + 2, 4))
    return (2 * chips[which] + core) * ROWS


def into(out, ref, place, sem):
    return pltpu.make_async_copy(ref, out.at[0, :, pl.ds(place, ROWS), :], sem)


def first_half_kernel(
    fields, from_west, from_east, from_outer, from_inner, snap, writer_hbm, held, out, flag, writer, zero, sems
):
    me = lax.axis_index("row")
    read = pltpu.make_async_copy(writer_hbm, writer, sems.at[8])
    read.start()
    zero[...] = jnp.zeros_like(zero)
    assemble(fields, from_west, from_east, from_outer, from_inner, held)
    read.wait()
    mine = writer[lax.axis_index("col")] == me
    flag[...] = jnp.where(mine, 1, 0) + jnp.zeros((8, LANES), jnp.int32)
    zeros = [into(out, zero, n * ROWS, sems.at[n]) for n in range(8)]
    own = into(out, snap, place_of(me, 0), sems.at[0])

    @pl.when(mine)
    def _():
        own.start()

    @pl.when(jnp.logical_not(mine))
    def _():
        for copy in zeros:
            copy.start()

    subcycles(held, 0, 5, 0, 12)
    subcycles(held, 5, SPLIT, 1, 11)

    @pl.when(mine)
    def _():
        own.wait()

    @pl.when(jnp.logical_not(mine))
    def _():
        for copy in zeros:
            copy.wait()


def second_half_kernel(state, out_in, flag, near, near_back, far, vel, stress, held, out, sems):
    me = lax.axis_index("row")
    mine = jnp.max(flag[...]) == 1
    copies = [
        into(out, near, place_of(me, 1), sems.at[0]),
        into(out, near_back, place_of(me, 2), sems.at[1]),
        into(out, far, place_of(me, 3), sems.at[2]),
    ]

    @pl.when(mine)
    def _():
        for copy in copies:
            copy.start()

    subcycles(held, SPLIT, SUB, 1, 11)
    at = PAD + HALO
    vel[0] = held[U, 0, at : at + ROWS]
    vel[1] = held[V, 0, at : at + ROWS]
    stress[0] = 2.0 * held[S1, 0, at : at + ROWS]
    stress[1] = 2.0 * held[S2, 0, at : at + ROWS]
    stress[2] = held[S12, 0, at : at + ROWS]

    @pl.when(mine)
    def _():
        for copy in copies:
            copy.wait()


def last_kernel(out_in, flag, partner, out, sems):
    me = lax.axis_index("row")
    mine = jnp.max(flag[...]) == 1

    @pl.when(mine)
    def _():
        copies = [into(out, partner.at[n], place_of(me, 4 + n), sems.at[n]) for n in range(4)]
        for copy in copies:
            copy.start()
        for copy in copies:
            copy.wait()


def join_kernel(own, near, near_back, far, joined):
    for n, block in enumerate((own, near, near_back, far)):
        joined[n] = block[...]


def vmem():
    return pl.BlockSpec(memory_space=pltpu.VMEM)


def shape(*dims):
    return jax.ShapeDtypeStruct(dims, jnp.float32)


def grant(mebibytes):
    return pltpu.CompilerParams(vmem_limit_bytes=mebibytes << 20)


def step(
    velocity_start,
    stress_start,
    wind_stress,
    ocean_current,
    ice_area,
    ice_volume,
    inverse_width,
    inverse_height,
    land_block,
    ice_block,
    writer,
):
    fields, to_west, to_east, snap = pl.pallas_call(
        prepare_kernel,
        out_shape=(
            shape(SENT, ROWS, LANES),
            shape(SENT * 8, LANES),
            shape(SENT * 8, LANES),
            shape(10, ROWS, LANES),
        ),
        in_specs=[pl.BlockSpec(memory_space=pltpu.HBM)] * 10,
        out_specs=(vmem(),) * 4,
        scratch_shapes=[
            pltpu.VMEM((2, ROWS, LANES), jnp.float32),
            pltpu.VMEM((3, ROWS, LANES), jnp.float32),
            pltpu.VMEM((2, ROWS, LANES), jnp.float32),
            pltpu.VMEM((2, ROWS, LANES), jnp.float32),
            pltpu.VMEM((ROWS, LANES), jnp.float32),
            pltpu.VMEM((ROWS, LANES), jnp.float32),
            pltpu.VMEM((4, 16), jnp.int32),
            pltpu.VMEM((4, 16), jnp.int32),
            pltpu.SemaphoreType.DMA((10,)),
        ],
        compiler_params=grant(8),
        name="prepare",
    )(
        *(
            pltpu.with_memory_space_constraint(value, pltpu.HBM)
            for value in (
                velocity_start,
                stress_start,
                wind_stress,
                ocean_current,
                ice_area,
                ice_volume,
                inverse_width,
                inverse_height,
                land_block.T,
                ice_block.T,
            )
        )
    )
    along = [(r, (r + 2 - 4 * (r % 2)) % 8) for r in range(8)]
    against = [(r, (r - 2 + 4 * (r % 2)) % 8) for r in range(8)]
    partner = [(r, r ^ 1) for r in range(8)]
    eastward = [(c, (c + 1) % 32) for c in range(32)]
    westward = [(c, (c - 1) % 32) for c in range(32)]
    across = [(7 * 32 + c, 7 * 32 + 31 - c) for c in range(32)]
    across += [(c, c) for c in range(32)]
    for c in range(32):
        for r in (1, 3, 5):
            across += [(32 * r + c, 32 * r + 32 + c), (32 * r + 32 + c, 32 * r + c)]

    near = lax.ppermute(snap, "row", along)
    from_west = lax.ppermute(to_east, "col", eastward)
    from_east = lax.ppermute(to_west, "col", westward)
    near_back = lax.ppermute(snap, "row", against)

    outer, inner = pl.pallas_call(
        rows_kernel,
        out_shape=(shape(MESSAGE, LANES),) * 2,
        in_specs=[vmem()] * 3,
        out_specs=(vmem(),) * 2,
        compiler_params=grant(8),
        cost_estimate=pl.CostEstimate(flops=1000000, bytes_accessed=1000000, transcendentals=0),
        name="rows",
    )(fields, from_west, from_east)
    from_outer = lax.ppermute(outer, ("row", "col"), across)
    from_inner = lax.ppermute(inner, "row", partner)
    far = lax.ppermute(near, "row", along)

    hbm = lambda: pl.BlockSpec(memory_space=pl.ANY)
    state, restart, flag = pl.pallas_call(
        first_half_kernel,
        out_shape=(
            shape(HELD, 2, TALL, LANES),
            shape(1, 10, 8 * ROWS, LANES),
            jax.ShapeDtypeStruct((8, LANES), jnp.int32),
        ),
        in_specs=[vmem()] * 5 + [hbm(), hbm()],
        out_specs=(vmem(), hbm(), vmem()),
        scratch_shapes=[
            pltpu.SMEM((32,), jnp.int32),
            pltpu.VMEM((10, ROWS, LANES), jnp.float32),
            pltpu.SemaphoreType.DMA((9,)),
        ],
        compiler_params=grant(16),
        cost_estimate=pl.CostEstimate(flops=20000000, bytes_accessed=2000000, transcendentals=0),
        name="first_half",
    )(
        fields,
        from_west,
        from_east,
        from_outer,
        from_inner,
        snap,
        pltpu.with_memory_space_constraint(writer, pltpu.HBM),
    )

    joined = pl.pallas_call(
        join_kernel,
        out_shape=shape(4, 10, ROWS, LANES),
        in_specs=[vmem()] * 4,
        out_specs=vmem(),
        compiler_params=grant(8),
        name="join",
    )(snap, near, near_back, far)
    partner_blocks = lax.ppermute(joined, "row", partner)

    velocity, stress, _, restart = pl.pallas_call(
        second_half_kernel,
        out_shape=(
            shape(2, ROWS, LANES),
            shape(3, ROWS, LANES),
            shape(HELD, 2, TALL, LANES),
            shape(1, 10, 8 * ROWS, LANES),
        ),
        in_specs=[vmem(), hbm(), vmem(), hbm(), hbm(), hbm()],
        out_specs=(vmem(), vmem(), vmem(), hbm()),
        input_output_aliases={0: 2, 1: 3},
        scratch_shapes=[pltpu.SemaphoreType.DMA((3,))],
        compiler_params=grant(8),
        cost_estimate=pl.CostEstimate(flops=20000000, bytes_accessed=2000000, transcendentals=0),
        name="second_half",
    )(state, restart, flag, near, near_back, far)

    restart = pl.pallas_call(
        last_kernel,
        out_shape=shape(1, 10, 8 * ROWS, LANES),
        in_specs=[hbm(), vmem(), hbm()],
        out_specs=hbm(),
        input_output_aliases={0: 0},
        scratch_shapes=[pltpu.SemaphoreType.DMA((4,))],
        compiler_params=grant(4),
        name="last",
    )(restart, flag, partner_blocks)
    return (velocity, stress, restart)


def solution(mesh):
    return jax.shard_map(
        step,
        mesh=mesh,
        in_specs=(
            P(None, "row", "col"),
            P(None, "row", "col"),
            P(None, "row", "col"),
            P(None, "row", "col"),
            P(None, "row", "col"),
            P(None, "row", "col"),
            P("row", "col"),
            P("row", "col"),
            P("row", "col"),
            P("row", "col"),
            P(),
        ),
        out_specs=(P(None, "row", "col"), P(None, "row", "col"), P("row", None, None, "col")),
        check_vma=False,
    )
```

```python
import jax
import jax.numpy as jnp
from jax import lax
from jax.experimental import pallas as pl
from jax.experimental.pallas import tpu as pltpu
from jax.sharding import PartitionSpec as P


SUB = 12
SPLIT = 7
ROWS = 64
LANES = 128
HALO = 16
PAD = 8
TALL = PAD + HALO + ROWS + HALO + PAD
TOP = PAD + HALO + ROWS
BAND = 24
SHORT = PAD + BAND + PAD

U, V, S1, S2, S12, STR, HW, HH, INE, AA, KU, KV = range(12)
SENT = 12
BB, HWV, HHV, DU, SU, DV, SV, DP, DS, AS, AM = range(12, 23)
HELD = 23
MOVING = (U, V, INE, AA, KU, KV)
NEGATED = (U, V, KU, KV)
MESSAGE = SENT * HALO + SENT // 2 * 8


def lane_index():
    return lax.broadcasted_iota(jnp.int32, (8, LANES), 1)


def row_index():
    return lax.broadcasted_iota(jnp.int32, (8, LANES), 0)


def turned(value, steps):
    steps = steps % LANES
    return value if steps == 0 else pltpu.roll(value, steps, 1)


def west(values, blocks, lane):
    side = values[0]
    out = turned(side, 1)
    mains = []
    for main, b in zip(values[1:], blocks):
        out = jnp.where(lane == 32 * b + 16, turned(main, 32 * b + 17), out)
        mains.append(jnp.where(lane == 0, turned(side, -(32 * b + 15)), turned(main, 1)))
    return [out] + mains


def east(values, blocks, lane):
    side = values[0]
    out = turned(side, -1)
    mains = []
    for main, b in zip(values[1:], blocks):
        out = jnp.where(lane == 32 * b + 15, turned(main, 32 * b + 15), out)
        mains.append(jnp.where(lane == LANES - 1, turned(side, 111 - 32 * b), turned(main, -1)))
    return [out] + mains


def expanded(blocks_t):
    rows = lax.broadcasted_iota(jnp.int32, (ROWS, 16), 0) // 4
    pick_rows = (rows == lax.broadcasted_iota(jnp.int32, (ROWS, 16), 1)).astype(jnp.float32)
    lanes = lax.broadcasted_iota(jnp.int32, (4, LANES), 1) // 32
    pick_lanes = (lanes == lax.broadcasted_iota(jnp.int32, (4, LANES), 0)).astype(jnp.float32)
    half = lax.dot_general(
        pick_rows, blocks_t, (((1,), (1,)), ((), ())), preferred_element_type=jnp.float32
    )
    return lax.dot_general(
        half, pick_lanes, (((1,), (0,)), ((), ())), preferred_element_type=jnp.float32
    )


def prepare_kernel(
    vel_hbm,
    stress_hbm,
    wind_hbm,
    ocean_hbm,
    area_hbm,
    volume_hbm,
    wide_hbm,
    high_hbm,
    land_hbm,
    ice_hbm,
    fields,
    to_west,
    to_east,
    snap,
    vel,
    stress,
    wind,
    ocean,
    wide,
    high,
    land_t,
    ice_t,
    sems,
):
    area, volume = snap.at[0:5], snap.at[5:10]
    moves = (
        (area_hbm, area),
        (volume_hbm, volume),
        (land_hbm, land_t),
        (ice_hbm, ice_t),
        (ocean_hbm, ocean),
        (wind_hbm, wind),
        (stress_hbm, stress),
        (vel_hbm, vel),
        (wide_hbm, wide),
        (high_hbm, high),
    )
    copies = [pltpu.make_async_copy(a, b, sems.at[n]) for n, (a, b) in enumerate(moves)]
    for copy in copies:
        copy.start()
    for copy in copies:
        copy.wait()
    land = expanded(land_t[...].astype(jnp.float32))
    ice = expanded(ice_t[...].astype(jnp.float32))
    area_total = area[0] + area[1] + area[2] + area[3] + area[4]
    volume_total = volume[0] + volume[1] + volume[2] + volume[3] + volume[4]
    fields[U] = vel[0]
    fields[V] = vel[1]
    fields[S1] = 0.5 * stress[0]
    fields[S2] = 0.5 * stress[1]
    fields[S12] = stress[2]
    fields[STR] = (4.0 / 6.0) * volume_total * jnp.exp(-20.0 * (1.0 - area_total)) * land
    fields[HW] = 0.5 * wide[...]
    fields[HH] = 0.5 * high[...]
    inertia = 16.0 * (1.0 + volume_total)
    turning = 0.5 * (1.0 + volume_total)
    damped = inertia + 1.0
    scale = land * ice / (damped * damped + turning * turning)
    still = land * (1.0 - ice)
    fx = wind[0] + ocean[0]
    fy = wind[1] + ocean[1]
    fields[INE] = inertia
    fields[AA] = scale
    fields[KU] = scale * (damped * fx + turning * fy) + still * ocean[0]
    fields[KV] = scale * (damped * fy - turning * fx) + still * ocean[1]
    lane = lane_index()
    for f in range(SENT):
        left = right = None
        for g in range(8):
            part = fields[f, 8 * g : 8 * g + 8]
            inside = (lane >= 16 * g) & (lane < 16 * g + 16)
            a = turned(part, 16 * g)
            b = turned(part, 16 * g - 112)
            left = a if g == 0 else jnp.where(inside, a, left)
            right = b if g == 0 else jnp.where(inside, b, right)
        to_west[8 * f : 8 * f + 8] = left
        to_east[8 * f : 8 * f + 8] = right


def rows_kernel(fields, from_west, from_east, outer, inner):
    lane = lane_index()
    odd = lax.axis_index("row") % 2 == 1

    def fill(to_north, to_south):
        for f in range(SENT):
            to_north[HALO * f : HALO * f + HALO] = fields[f, ROWS - HALO : ROWS]
            to_south[HALO * f : HALO * f + HALO] = fields[f, 0:HALO]
        for pair in range(SENT // 2):
            north = south = None
            for member in range(2):
                f = 2 * pair + member
                base = 64 * member
                a = from_west[8 * f : 8 * f + 8]
                b = from_east[8 * f : 8 * f + 8]
                here = lane >= base
                there = lane >= base + 32
                n = jnp.where(there, turned(b, base + 32 - 96), turned(a, base - 96))
                s = jnp.where(there, turned(b, base + 32), turned(a, base))
                north = n if member == 0 else jnp.where(here, n, north)
                south = s if member == 0 else jnp.where(here, s, south)
            at = SENT * HALO + 8 * pair
            to_north[at : at + 8] = north
            to_south[at : at + 8] = south

    @pl.when(odd)
    def _():
        fill(outer, inner)

    @pl.when(jnp.logical_not(odd))
    def _():
        fill(inner, outer)


def assemble(fields, from_west, from_east, from_outer, from_inner, main, side):
    is_top = lax.axis_index("row") == 7
    odd = lax.axis_index("row") % 2 + jnp.zeros((8, LANES), jnp.int32) == 1
    bottom = lax.axis_index("row") + jnp.zeros((8, LANES), jnp.int32) == 0
    lane, row = lane_index(), row_index()

    def south(at):
        value = jnp.where(odd, from_inner[at : at + 8], from_outer[at : at + 8])
        return jnp.where(bottom, 0.0, value)

    def north(at):
        return jnp.where(odd, from_outer[at : at + 8], from_inner[at : at + 8])

    def rotated(value):
        value = jnp.take_along_axis(value, LANES - 1 - lane, axis=1)
        return jnp.take_along_axis(value, 7 - row, axis=0)

    for f in range(SENT):
        base = 64 * (f % 2)
        corner_at = SENT * HALO + 8 * (f // 2)
        west_side, east_side = from_west[8 * f : 8 * f + 8], from_east[8 * f : 8 * f + 8]
        south_side, north_side = south(corner_at), north(corner_at)
        for g in range(8):
            main[f, PAD + HALO + 8 * g : PAD + HALO + 8 * g + 8] = fields[f, 8 * g : 8 * g + 8]
        for g in range(2):
            main[f, PAD + 8 * g : PAD + 8 * g + 8] = south(HALO * f + 8 * g)
            main[f, TOP + 8 * g : TOP + 8 * g + 8] = north(HALO * f + 8 * g)
        for j in range(3):
            value = None
            for b in range(4):
                g = 3 * b + j
                if g < 2:
                    parts = (south_side, base + 16 * g), (south_side, base + 32 + 16 * g)
                elif g < 10:
                    parts = (west_side, 16 * (g - 2)), (east_side, 16 * (g - 2))
                else:
                    parts = (north_side, base + 16 * (g - 10)), (north_side, base + 32 + 16 * (g - 10))
                for n, (part, origin) in enumerate(parts):
                    to = 32 * b + 16 * n
                    part = turned(part, to - origin)
                    value = part if value is None else jnp.where(lane >= to, part, value)
            side[f, PAD + 8 * j : PAD + 8 * j + 8] = value

    def ghost(f, g):
        a = 1 - g
        base = 64 * (f % 2)
        corner = north(SENT * HALO + 8 * (f // 2))
        both = jnp.where(lane < 16, turned(corner, -base - 16 * a), turned(corner, -base - 16 - 16 * a))
        return rotated(both), rotated(north(HALO * f + 8 * a))

    def put_ghost(f, g, shift, tiles):
        side_value, main_value = tiles
        at, low = TOP + shift + 8 * g, PAD + 8 + shift + 8 * g
        main[f, at : at + 8] = main_value
        side[f, low : low + 8] = jnp.where(lane >= 96, side_value, side[f, low : low + 8])

    @pl.when(is_top)
    def _():
        for f in range(SENT):
            for g in range(2):
                tiles = ghost(f, g)
                if f in MOVING:
                    tiles = east(tiles, (3,), lane)
                    if f in NEGATED:
                        tiles = [-value for value in tiles]
                put_ghost(f, g, 0 if f in MOVING else 1, tiles)

    for ref, tall in ((main, TALL), (side, SHORT)):
        for at in range(PAD, tall - PAD, 8):
            rows = slice(at, at + 8)
            inertia, scale = ref[INE, rows], ref[AA, rows]
            ref[AA, rows] = (inertia + 1.0) * scale
            ref[BB, rows] = (inertia * (1.0 / 32.0)) * scale
            ref[HWV, rows] = ref[HW, rows]
            ref[HHV, rows] = ref[HH, rows]

    @pl.when(is_top)
    def _():
        for f, own in ((HW, HWV), (HH, HHV)):
            for g in range(2):
                put_ghost(own, g, 0, east(ghost(f, g), (3,), lane))

    for j in range(3):
        tiles = unit(main, side, j, 0, 12)
        u = [ref[U, at : at + 8] for ref, at in tiles]
        v = [ref[V, at : at + 8] for ref, at in tiles]
        velocity_sums(side, tiles, blocks_of(j, 0, 12), j, u, v, lane)


def blocks_of(j, lo, hi):
    return [b for b in range(4) if lo <= 3 * b + j < hi]


def unit(main, side, j, lo, hi):
    return [(side, PAD + 8 * j)] + [(main, PAD + 8 * (3 * b + j)) for b in blocks_of(j, lo, hi)]


def velocity_sums(side, tiles, blocks, j, u, v, lane):
    wu = west(u, blocks, lane)
    wv = west(v, blocks, lane)
    for (ref, at), x, wx, y, wy in zip(tiles, u, wu, v, wv):
        made = ((DU, x - wx), (SU, x + wx), (DV, y - wy), (SV, y + wy))
        for f, value in made:
            ref[f, at : at + 8] = value
            if ref is side and j == 2:
                side[f, 0:PAD] = turned(value, 32)


def stress_rows(main, side, j, lo, hi, lane):
    tiles, blocks = unit(main, side, j, lo, hi), blocks_of(j, lo, hi)
    ps, ms, qs = [], [], []
    for ref, at in tiles:
        here = lambda f: ref[f, at : at + 8]
        below = lambda f: ref[f, at - 1 : at + 7]
        hw, hh = here(HW), here(HH)
        gux = hw * (here(DU) + below(DU))
        guy = hh * (here(SU) - below(SU))
        gvx = hw * (here(DV) + below(DV))
        gvy = hh * (here(SV) - below(SV))
        divergence = gux + gvy
        tension = gux - gvy
        shearing = guy + gvx
        deform = jnp.sqrt(
            divergence * divergence + 0.25 * (tension * tension + shearing * shearing)
        )
        viscous = here(STR) / (deform + 0.5)
        quarter = 0.25 * viscous
        s1 = here(S1) * (2.0 / 3.0) + viscous * (divergence - deform)
        s2 = here(S2) * (2.0 / 3.0) + quarter * tension
        s12 = here(S12) * (2.0 / 3.0) + quarter * shearing
        ref[S1, at : at + 8] = s1
        ref[S2, at : at + 8] = s2
        ref[S12, at : at + 8] = s12
        ps.append(s1 + s2)
        ms.append(s1 - s2)
        qs.append(s12)
    for values, minus, plus in ((ps, DP, None), (ms, None, AM), (qs, DS, AS)):
        for (ref, at), value, shifted in zip(tiles, values, east(values, blocks, lane)):
            for f, made in ((minus, shifted - value), (plus, shifted + value)):
                if f is not None:
                    ref[f, at : at + 8] = made
                    if ref is side and j == 0:
                        side[f, PAD + BAND : SHORT] = turned(made, -32)


def velocity_rows(main, side, j, lo, hi, lane, row, top_rows):
    tiles, blocks = unit(main, side, j, lo, hi), blocks_of(j, lo, hi)
    us, vs = [], []
    for ref, at in tiles:
        here = lambda f: ref[f, at : at + 8]
        below_fold = at == (PAD if ref is side else TOP - 8)
        above_fold = at == (PAD + 8 if ref is side else TOP)
        affected = top_rows & (lane >= 96) if ref is side else top_rows

        def pair(f):
            own, above = here(f), ref[f, at + 1 : at + 9]
            if below_fold:
                above = jnp.where((row == 7) & affected, ref[f, at + 2 : at + 10], above)
            if above_fold:
                own = jnp.where((row == 0) & affected, ref[f, at - 1 : at + 7], own)
            return own, above

        hw, hh = here(HWV), here(HHV)
        dp, ndp = pair(DP)
        ds, nds = pair(DS)
        as_, nas = pair(AS)
        am, nam = pair(AM)
        inertia, a, b = here(INE), here(AA), here(BB)
        x = inertia * here(U) + (hw * (dp + ndp) + hh * (nas - as_))
        y = inertia * here(V) + (hw * (ds + nds) + hh * (nam - am))
        u = a * x + b * y + here(KU)
        v = a * y - b * x + here(KV)
        ref[U, at : at + 8] = u
        ref[V, at : at + 8] = v
        us.append(u)
        vs.append(v)
    velocity_sums(side, tiles, blocks, j, us, vs, lane)


def subcycles(main, side, start, stop, lo, hi):
    lane, row = lane_index(), row_index()
    is_top = lax.axis_index("row") == 7
    top_rows = (jnp.where(is_top, 1, 0) + jnp.zeros((8, LANES), jnp.int32)) == 1

    def body(_, carry):
        for j in range(3):
            stress_rows(main, side, j, lo, hi, lane)
        for j in range(3):
            velocity_rows(main, side, j, lo, hi, lane, row, top_rows)
        return carry

    lax.fori_loop(start, stop, body, 0)


def place_of(me, which):
    chip, core = me // 2, me % 2
    step = 1 - 2 * core
    if which >= 4:
        core = 1 - core
        which -= 4
        step = -step
    chips = (chip, lax.rem(chip - step + 4, 4), lax.rem(chip + step + 4, 4), lax.rem(chip + 2, 4))
    return (2 * chips[which] + core) * ROWS


def into(out, ref, place, sem):
    return pltpu.make_async_copy(ref, out.at[0, :, pl.ds(place, ROWS), :], sem)


def first_half_kernel(
    fields, from_west, from_east, from_outer, from_inner, snap, writer_hbm, main, side, out, flag, writer, zero, sems
):
    me = lax.axis_index("row")
    read = pltpu.make_async_copy(writer_hbm, writer, sems.at[8])
    read.start()
    zero[...] = jnp.zeros_like(zero)
    assemble(fields, from_west, from_east, from_outer, from_inner, main, side)
    read.wait()
    mine = writer[lax.axis_index("col")] == me
    flag[...] = jnp.where(mine, 1, 0) + jnp.zeros((8, LANES), jnp.int32)
    zeros = [into(out, zero, n * ROWS, sems.at[n]) for n in range(8)]
    own = into(out, snap, place_of(me, 0), sems.at[0])

    @pl.when(mine)
    def _():
        own.start()

    @pl.when(jnp.logical_not(mine))
    def _():
        for copy in zeros:
            copy.start()

    subcycles(main, side, 0, 5, 0, 12)
    subcycles(main, side, 5, SPLIT, 1, 11)

    @pl.when(mine)
    def _():
        own.wait()

    @pl.when(jnp.logical_not(mine))
    def _():
        for copy in zeros:
            copy.wait()


def second_half_kernel(
    main_in, side_in, out_in, flag, near, near_back, far, vel, stress, main, side, out, sems
):
    me = lax.axis_index("row")
    mine = jnp.max(flag[...]) == 1
    copies = [
        into(out, near, place_of(me, 1), sems.at[0]),
        into(out, near_back, place_of(me, 2), sems.at[1]),
        into(out, far, place_of(me, 3), sems.at[2]),
    ]

    @pl.when(mine)
    def _():
        for copy in copies:
            copy.start()

    subcycles(main, side, SPLIT, SUB, 1, 11)
    at = PAD + HALO
    vel[0] = main[U, at : at + ROWS]
    vel[1] = main[V, at : at + ROWS]
    stress[0] = 2.0 * main[S1, at : at + ROWS]
    stress[1] = 2.0 * main[S2, at : at + ROWS]
    stress[2] = main[S12, at : at + ROWS]

    @pl.when(mine)
    def _():
        for copy in copies:
            copy.wait()


def last_kernel(out_in, flag, partner, out, sems):
    me = lax.axis_index("row")
    mine = jnp.max(flag[...]) == 1

    @pl.when(mine)
    def _():
        copies = [into(out, partner.at[n], place_of(me, 4 + n), sems.at[n]) for n in range(4)]
        for copy in copies:
            copy.start()
        for copy in copies:
            copy.wait()


def join_kernel(own, near, near_back, far, joined):
    for n, block in enumerate((own, near, near_back, far)):
        joined[n] = block[...]


def vmem():
    return pl.BlockSpec(memory_space=pltpu.VMEM)


def shape(*dims):
    return jax.ShapeDtypeStruct(dims, jnp.float32)


def grant(mebibytes):
    return pltpu.CompilerParams(vmem_limit_bytes=mebibytes << 20)


def step(
    velocity_start,
    stress_start,
    wind_stress,
    ocean_current,
    ice_area,
    ice_volume,
    inverse_width,
    inverse_height,
    land_block,
    ice_block,
    writer,
):
    fields, to_west, to_east, snap = pl.pallas_call(
        prepare_kernel,
        out_shape=(
            shape(SENT, ROWS, LANES),
            shape(SENT * 8, LANES),
            shape(SENT * 8, LANES),
            shape(10, ROWS, LANES),
        ),
        in_specs=[pl.BlockSpec(memory_space=pltpu.HBM)] * 10,
        out_specs=(vmem(),) * 4,
        scratch_shapes=[
            pltpu.VMEM((2, ROWS, LANES), jnp.float32),
            pltpu.VMEM((3, ROWS, LANES), jnp.float32),
            pltpu.VMEM((2, ROWS, LANES), jnp.float32),
            pltpu.VMEM((2, ROWS, LANES), jnp.float32),
            pltpu.VMEM((ROWS, LANES), jnp.float32),
            pltpu.VMEM((ROWS, LANES), jnp.float32),
            pltpu.VMEM((4, 16), jnp.int32),
            pltpu.VMEM((4, 16), jnp.int32),
            pltpu.SemaphoreType.DMA((10,)),
        ],
        compiler_params=grant(8),
        name="prepare",
    )(
        *(
            pltpu.with_memory_space_constraint(value, pltpu.HBM)
            for value in (
                velocity_start,
                stress_start,
                wind_stress,
                ocean_current,
                ice_area,
                ice_volume,
                inverse_width,
                inverse_height,
                land_block.T,
                ice_block.T,
            )
        )
    )
    along = [(r, (r + 2 - 4 * (r % 2)) % 8) for r in range(8)]
    against = [(r, (r - 2 + 4 * (r % 2)) % 8) for r in range(8)]
    partner = [(r, r ^ 1) for r in range(8)]
    eastward = [(c, (c + 1) % 32) for c in range(32)]
    westward = [(c, (c - 1) % 32) for c in range(32)]
    across = [(7 * 32 + c, 7 * 32 + 31 - c) for c in range(32)]
    across += [(c, c) for c in range(32)]
    for c in range(32):
        for r in (1, 3, 5):
            across += [(32 * r + c, 32 * r + 32 + c), (32 * r + 32 + c, 32 * r + c)]

    near = lax.ppermute(snap, "row", along)
    from_west = lax.ppermute(to_east, "col", eastward)
    from_east = lax.ppermute(to_west, "col", westward)
    near_back = lax.ppermute(snap, "row", against)

    outer, inner = pl.pallas_call(
        rows_kernel,
        out_shape=(shape(MESSAGE, LANES),) * 2,
        in_specs=[vmem()] * 3,
        out_specs=(vmem(),) * 2,
        compiler_params=grant(8),
        cost_estimate=pl.CostEstimate(flops=1000000, bytes_accessed=1000000, transcendentals=0),
        name="rows",
    )(fields, from_west, from_east)
    from_outer = lax.ppermute(outer, ("row", "col"), across)
    from_inner = lax.ppermute(inner, "row", partner)
    far = lax.ppermute(near, "row", along)

    hbm = lambda: pl.BlockSpec(memory_space=pl.ANY)
    main, packed, restart, flag = pl.pallas_call(
        first_half_kernel,
        out_shape=(
            shape(HELD, TALL, LANES),
            shape(HELD, SHORT, LANES),
            shape(1, 10, 8 * ROWS, LANES),
            jax.ShapeDtypeStruct((8, LANES), jnp.int32),
        ),
        in_specs=[vmem()] * 5 + [hbm(), hbm()],
        out_specs=(vmem(), vmem(), hbm(), vmem()),
        scratch_shapes=[
            pltpu.SMEM((32,), jnp.int32),
            pltpu.VMEM((10, ROWS, LANES), jnp.float32),
            pltpu.SemaphoreType.DMA((9,)),
        ],
        compiler_params=grant(16),
        cost_estimate=pl.CostEstimate(flops=20000000, bytes_accessed=2000000, transcendentals=0),
        name="first_half",
    )(
        fields,
        from_west,
        from_east,
        from_outer,
        from_inner,
        snap,
        pltpu.with_memory_space_constraint(writer, pltpu.HBM),
    )

    joined = pl.pallas_call(
        join_kernel,
        out_shape=shape(4, 10, ROWS, LANES),
        in_specs=[vmem()] * 4,
        out_specs=vmem(),
        compiler_params=grant(8),
        name="join",
    )(snap, near, near_back, far)
    partner_blocks = lax.ppermute(joined, "row", partner)

    velocity, stress, _, _, restart = pl.pallas_call(
        second_half_kernel,
        out_shape=(
            shape(2, ROWS, LANES),
            shape(3, ROWS, LANES),
            shape(HELD, TALL, LANES),
            shape(HELD, SHORT, LANES),
            shape(1, 10, 8 * ROWS, LANES),
        ),
        in_specs=[vmem(), vmem(), hbm(), vmem(), hbm(), hbm(), hbm()],
        out_specs=(vmem(), vmem(), vmem(), vmem(), hbm()),
        input_output_aliases={0: 2, 1: 3, 2: 4},
        scratch_shapes=[pltpu.SemaphoreType.DMA((3,))],
        compiler_params=grant(8),
        cost_estimate=pl.CostEstimate(flops=20000000, bytes_accessed=2000000, transcendentals=0),
        name="second_half",
    )(main, packed, restart, flag, near, near_back, far)

    restart = pl.pallas_call(
        last_kernel,
        out_shape=shape(1, 10, 8 * ROWS, LANES),
        in_specs=[hbm(), vmem(), hbm()],
        out_specs=hbm(),
        input_output_aliases={0: 0},
        scratch_shapes=[pltpu.SemaphoreType.DMA((4,))],
        compiler_params=grant(4),
        name="last",
    )(restart, flag, partner_blocks)
    return (velocity, stress, restart)


def solution(mesh):
    return jax.shard_map(
        step,
        mesh=mesh,
        in_specs=(
            P(None, "row", "col"),
            P(None, "row", "col"),
            P(None, "row", "col"),
            P(None, "row", "col"),
            P(None, "row", "col"),
            P(None, "row", "col"),
            P("row", "col"),
            P("row", "col"),
            P("row", "col"),
            P("row", "col"),
            P(),
        ),
        out_specs=(P(None, "row", "col"), P(None, "row", "col"), P("row", None, None, "col")),
        check_vma=False,
    )
```

```python
import jax
import jax.numpy as jnp
from jax import lax
from jax.experimental import pallas as pl
from jax.experimental.pallas import tpu as pltpu
from jax.sharding import PartitionSpec as P


SUB = 12
SPLIT = 7
ROWS = 64
LANES = 128
HALO = 16
PAD = 8
TALL = PAD + HALO + ROWS + HALO + PAD
TOP = PAD + HALO + ROWS

U, V, S1, S2, S12, STR, HW, HH, INE, AA, KU, KV = range(12)
SENT = 12
BB, HWV, HHV, DU, SU, DV, SV, DP, DS, AS, AM = range(12, 23)
HELD = 23
MOVING = (U, V, INE, AA, KU, KV)
NEGATED = (U, V, KU, KV)
MESSAGE = SENT * HALO + SENT // 2 * 8


def lane_index():
    return lax.broadcasted_iota(jnp.int32, (8, LANES), 1)


def row_index():
    return lax.broadcasted_iota(jnp.int32, (8, LANES), 0)


def turned(value, steps):
    steps = steps % LANES
    return value if steps == 0 else pltpu.roll(value, steps, 1)


def west(main, side, first):
    a, b = turned(main, 1), turned(side, 1)
    return jnp.where(first, b, a), jnp.where(first, a, b)


def east(main, side, last):
    a, b = turned(main, -1), turned(side, -1)
    return jnp.where(last, b, a), jnp.where(last, a, b)


def expanded(blocks_t):
    rows = lax.broadcasted_iota(jnp.int32, (ROWS, 16), 0) // 4
    pick_rows = (rows == lax.broadcasted_iota(jnp.int32, (ROWS, 16), 1)).astype(jnp.float32)
    lanes = lax.broadcasted_iota(jnp.int32, (4, LANES), 1) // 32
    pick_lanes = (lanes == lax.broadcasted_iota(jnp.int32, (4, LANES), 0)).astype(jnp.float32)
    half = lax.dot_general(
        pick_rows, blocks_t, (((1,), (1,)), ((), ())), preferred_element_type=jnp.float32
    )
    return lax.dot_general(
        half, pick_lanes, (((1,), (0,)), ((), ())), preferred_element_type=jnp.float32
    )


def prepare_kernel(
    vel_hbm,
    stress_hbm,
    wind_hbm,
    ocean_hbm,
    area_hbm,
    volume_hbm,
    wide_hbm,
    high_hbm,
    land_hbm,
    ice_hbm,
    writer_hbm,
    fields,
    to_west,
    to_east,
    snap,
    flag,
    blank,
    vel,
    stress,
    wind,
    ocean,
    wide,
    high,
    land_t,
    ice_t,
    writer,
    sems,
):
    area, volume = snap.at[0:5], snap.at[5:10]
    moves = (
        (area_hbm, area),
        (volume_hbm, volume),
        (land_hbm, land_t),
        (ice_hbm, ice_t),
        (ocean_hbm, ocean),
        (wind_hbm, wind),
        (stress_hbm, stress),
        (vel_hbm, vel),
        (wide_hbm, wide),
        (high_hbm, high),
        (writer_hbm, writer),
    )
    copies = [pltpu.make_async_copy(a, b, sems.at[n]) for n, (a, b) in enumerate(moves)]
    for copy in copies:
        copy.start()
    blank[...] = jnp.zeros_like(blank)
    for copy in copies:
        copy.wait()
    mine = writer[lax.axis_index("col")] == lax.axis_index("row")
    flag[...] = jnp.where(mine, 1, 0) + jnp.zeros((8, LANES), jnp.int32)
    land = expanded(land_t[...].astype(jnp.float32))
    ice = expanded(ice_t[...].astype(jnp.float32))
    area_total = area[0] + area[1] + area[2] + area[3] + area[4]
    volume_total = volume[0] + volume[1] + volume[2] + volume[3] + volume[4]
    fields[U] = vel[0]
    fields[V] = vel[1]
    fields[S1] = 0.5 * stress[0]
    fields[S2] = 0.5 * stress[1]
    fields[S12] = stress[2]
    fields[STR] = (4.0 / 6.0) * volume_total * jnp.exp(-20.0 * (1.0 - area_total)) * land
    fields[HW] = 0.5 * wide[...]
    fields[HH] = 0.5 * high[...]
    inertia = 16.0 * (1.0 + volume_total)
    turning = 0.5 * (1.0 + volume_total)
    damped = inertia + 1.0
    scale = land * ice / (damped * damped + turning * turning)
    still = land * (1.0 - ice)
    fx = wind[0] + ocean[0]
    fy = wind[1] + ocean[1]
    fields[INE] = inertia
    fields[AA] = scale
    fields[KU] = scale * (damped * fx + turning * fy) + still * ocean[0]
    fields[KV] = scale * (damped * fy - turning * fx) + still * ocean[1]
    lane = lane_index()
    for f in range(SENT):
        left = right = None
        for g in range(8):
            part = fields[f, 8 * g : 8 * g + 8]
            inside = (lane >= 16 * g) & (lane < 16 * g + 16)
            a = turned(part, 16 * g)
            b = turned(part, 16 * g - 112)
            left = a if g == 0 else jnp.where(inside, a, left)
            right = b if g == 0 else jnp.where(inside, b, right)
        to_west[8 * f : 8 * f + 8] = left
        to_east[8 * f : 8 * f + 8] = right


def rows_kernel(fields, from_west, from_east, outer, inner):
    lane = lane_index()
    odd = lax.axis_index("row") % 2 == 1

    def fill(to_north, to_south):
        for f in range(SENT):
            to_north[HALO * f : HALO * f + HALO] = fields[f, ROWS - HALO : ROWS]
            to_south[HALO * f : HALO * f + HALO] = fields[f, 0:HALO]
        for pair in range(SENT // 2):
            north = south = None
            for member in range(2):
                f = 2 * pair + member
                base = 64 * member
                a = from_west[8 * f : 8 * f + 8]
                b = from_east[8 * f : 8 * f + 8]
                here = lane >= base
                there = lane >= base + 32
                n = jnp.where(there, turned(b, base + 32 - 96), turned(a, base - 96))
                s = jnp.where(there, turned(b, base + 32), turned(a, base))
                north = n if member == 0 else jnp.where(here, n, north)
                south = s if member == 0 else jnp.where(here, s, south)
            at = SENT * HALO + 8 * pair
            to_north[at : at + 8] = north
            to_south[at : at + 8] = south

    @pl.when(odd)
    def _():
        fill(outer, inner)

    @pl.when(jnp.logical_not(odd))
    def _():
        fill(inner, outer)


def stencil_masks():
    lane, row = lane_index(), row_index()
    is_top = lax.axis_index("row") == 7
    top_rows = (jnp.where(is_top, 1, 0) + jnp.zeros((8, LANES), jnp.int32)) == 1
    return lane == 0, lane == LANES - 1, row, top_rows


def assemble(fields, from_west, from_east, from_outer, from_inner, held):
    is_top = lax.axis_index("row") == 7
    odd = lax.axis_index("row") % 2 + jnp.zeros((8, LANES), jnp.int32) == 1
    lane = lane_index()
    row = row_index()
    first, last, low = lane == 0, lane == LANES - 1, lane < 64

    bottom = lax.axis_index("row") + jnp.zeros((8, LANES), jnp.int32) == 0

    def south(at):
        value = jnp.where(odd, from_inner[at : at + 8], from_outer[at : at + 8])
        return jnp.where(bottom, 0.0, value)

    def north(at):
        return jnp.where(odd, from_outer[at : at + 8], from_inner[at : at + 8])

    def side_rows(message, f, a):
        base = 64 * (f % 2)
        corner = message(SENT * HALO + 8 * (f // 2))
        return jnp.where(low, turned(corner, -(base + 32 + 16 * a)), turned(corner, 112 - base - 16 * a))

    for f in range(SENT):
        a, b = from_west[8 * f : 8 * f + 8], from_east[8 * f : 8 * f + 8]
        for g in range(8):
            at = PAD + HALO + 8 * g
            held[f, 0, at : at + 8] = fields[f, 8 * g : 8 * g + 8]
            held[f, 1, at : at + 8] = jnp.where(low, turned(b, -16 * g), turned(a, 112 - 16 * g))
        for g in range(2):
            at = PAD + 8 * g
            held[f, 0, at : at + 8] = south(HALO * f + 8 * g)
            held[f, 1, at : at + 8] = side_rows(south, f, g)

    @pl.when(jnp.logical_not(is_top))
    def _():
        for f in range(SENT):
            for g in range(2):
                at = TOP + 8 * g
                held[f, 0, at : at + 8] = north(HALO * f + 8 * g)
                held[f, 1, at : at + 8] = side_rows(north, f, g)

    @pl.when(is_top)
    def _():
        def rotated(value):
            value = jnp.take_along_axis(value, LANES - 1 - lane, axis=1)
            return jnp.take_along_axis(value, 7 - row, axis=0)

        for f in range(SENT):
            for g in range(2):
                source = 1 - g
                main = rotated(north(HALO * f + 8 * source))
                side = rotated(side_rows(north, f, source))
                if f in MOVING:
                    main, side = east(main, side, last)
                    if f in NEGATED:
                        main, side = -main, -side
                    at = TOP + 8 * g
                else:
                    at = TOP + 1 + 8 * g
                held[f, 0, at : at + 8] = main
                held[f, 1, at : at + 8] = side
                if f in (HW, HH):
                    main, side = east(main, side, last)
                    own = HWV if f == HW else HHV
                    held[own, 0, TOP + 8 * g : TOP + 8 * g + 8] = main
                    held[own, 1, TOP + 8 * g : TOP + 8 * g + 8] = side

    for g in range(12):
        at = PAD + 8 * g
        for t in range(2):
            scale = held[AA, t, at : at + 8]
            inertia = held[INE, t, at : at + 8]
            held[AA, t, at : at + 8] = (inertia + 1.0) * scale
            held[BB, t, at : at + 8] = (inertia * (1.0 / 32.0)) * scale
            if g < 10:
                held[HWV, t, at : at + 8] = held[HW, t, at : at + 8]
                held[HHV, t, at : at + 8] = held[HH, t, at : at + 8]
        velocity_sums(
            held,
            at,
            held[U, 0, at : at + 8],
            held[U, 1, at : at + 8],
            held[V, 0, at : at + 8],
            held[V, 1, at : at + 8],
            first,
        )

    @pl.when(jnp.logical_not(is_top))
    def _():
        for t in range(2):
            held[HWV, t, TOP : TOP + HALO] = held[HW, t, TOP : TOP + HALO]
            held[HHV, t, TOP : TOP + HALO] = held[HH, t, TOP : TOP + HALO]


def velocity_sums(held, at, um, us, vm, vs, first):
    wum, wus = west(um, us, first)
    wvm, wvs = west(vm, vs, first)
    for t, (x, wx, y, wy) in enumerate(((um, wum, vm, wvm), (us, wus, vs, wvs))):
        held[DU, t, at : at + 8] = x - wx
        held[SU, t, at : at + 8] = x + wx
        held[DV, t, at : at + 8] = y - wy
        held[SV, t, at : at + 8] = y + wy


def stress_rows(held, at, last):
    fresh = []
    for t in range(2):
        here = lambda f: held[f, t, at : at + 8]
        below = lambda f: held[f, t, at - 1 : at + 7]
        hw, hh = here(HW), here(HH)
        gux = hw * (here(DU) + below(DU))
        guy = hh * (here(SU) - below(SU))
        gvx = hw * (here(DV) + below(DV))
        gvy = hh * (here(SV) - below(SV))
        divergence = gux + gvy
        tension = gux - gvy
        shearing = guy + gvx
        deform = jnp.sqrt(
            divergence * divergence + 0.25 * (tension * tension + shearing * shearing)
        )
        viscous = here(STR) / (deform + 0.5)
        quarter = 0.25 * viscous
        s1 = here(S1) * (2.0 / 3.0) + viscous * (divergence - deform)
        s2 = here(S2) * (2.0 / 3.0) + quarter * tension
        s12 = here(S12) * (2.0 / 3.0) + quarter * shearing
        held[S1, t, at : at + 8] = s1
        held[S2, t, at : at + 8] = s2
        held[S12, t, at : at + 8] = s12
        fresh.append((s1 + s2, s1 - s2, s12))
    (pm, mm, qm), (ps, ms, qs) = fresh
    epm, eps = east(pm, ps, last)
    emm, ems = east(mm, ms, last)
    eqm, eqs = east(qm, qs, last)
    for t, (p, ep, m, em, q, eq) in enumerate(
        ((pm, epm, mm, emm, qm, eqm), (ps, eps, ms, ems, qs, eqs))
    ):
        held[DP, t, at : at + 8] = ep - p
        held[AM, t, at : at + 8] = em + m
        held[DS, t, at : at + 8] = eq - q
        held[AS, t, at : at + 8] = eq + q


def velocity_rows(held, at, first, row, top_rows):
    fresh = []
    for t in range(2):
        here = lambda f: held[f, t, at : at + 8]

        def pair(f):
            own, above = here(f), held[f, t, at + 1 : at + 9]
            if at == TOP - 8:
                above = jnp.where((row == 7) & top_rows, held[f, t, at + 2 : at + 10], above)
            if at == TOP:
                own = jnp.where((row == 0) & top_rows, held[f, t, at - 1 : at + 7], own)
            return own, above

        hw, hh = here(HWV), here(HHV)
        dp, ndp = pair(DP)
        ds, nds = pair(DS)
        as_, nas = pair(AS)
        am, nam = pair(AM)
        inertia, a, b = here(INE), here(AA), here(BB)
        x = inertia * here(U) + (hw * (dp + ndp) + hh * (nas - as_))
        y = inertia * here(V) + (hw * (ds + nds) + hh * (nam - am))
        u = a * x + b * y + here(KU)
        v = a * y - b * x + here(KV)
        held[U, t, at : at + 8] = u
        held[V, t, at : at + 8] = v
        fresh.append((u, v))
    (um, vm), (us, vs) = fresh
    velocity_sums(held, at, um, us, vm, vs, first)


def subcycles(held, start, stop, lo, hi):
    first, last, row, top_rows = stencil_masks()

    def body(_, carry):
        for g in range(lo, hi):
            stress_rows(held, PAD + 8 * g, last)
        for g in range(lo, hi):
            velocity_rows(held, PAD + 8 * g, first, row, top_rows)
        return carry

    lax.fori_loop(start, stop, body, 0)


def place_of(me, which):
    chip, core = me // 2, me % 2
    step = 1 - 2 * core
    if which >= 4:
        core = 1 - core
        which -= 4
        step = -step
    chips = (chip, lax.rem(chip - step + 4, 4), lax.rem(chip + step + 4, 4), lax.rem(chip + 2, 4))
    return (2 * chips[which] + core) * ROWS


def into(out, ref, place, sem):
    return pltpu.make_async_copy(ref, out.at[0, :, pl.ds(place, ROWS), :], sem)


def first_half_kernel(
    fields, from_west, from_east, from_outer, from_inner, snap, flag, zero, held, out, sems
):
    me = lax.axis_index("row")
    mine = jnp.max(flag[...]) == 1
    zeros = [into(out, zero, n * ROWS, sems.at[n]) for n in range(8)]
    own = into(out, snap, place_of(me, 0), sems.at[0])

    @pl.when(mine)
    def _():
        own.start()

    @pl.when(jnp.logical_not(mine))
    def _():
        for copy in zeros:
            copy.start()

    assemble(fields, from_west, from_east, from_outer, from_inner, held)
    subcycles(held, 0, 5, 0, 12)
    subcycles(held, 5, SPLIT, 1, 11)

    @pl.when(mine)
    def _():
        own.wait()

    @pl.when(jnp.logical_not(mine))
    def _():
        for copy in zeros:
            copy.wait()


def second_half_kernel(state, out_in, flag, near, near_back, vel, stress, held, out, sems):
    me = lax.axis_index("row")
    mine = jnp.max(flag[...]) == 1
    copies = [
        into(out, near, place_of(me, 1), sems.at[0]),
        into(out, near_back, place_of(me, 2), sems.at[1]),
    ]

    @pl.when(mine)
    def _():
        for copy in copies:
            copy.start()

    subcycles(held, SPLIT, SUB, 1, 11)
    at = PAD + HALO
    vel[0] = held[U, 0, at : at + ROWS]
    vel[1] = held[V, 0, at : at + ROWS]
    stress[0] = 2.0 * held[S1, 0, at : at + ROWS]
    stress[1] = 2.0 * held[S2, 0, at : at + ROWS]
    stress[2] = held[S12, 0, at : at + ROWS]

    @pl.when(mine)
    def _():
        for copy in copies:
            copy.wait()


def last_kernel(
    out_in, flag, vel, stress, far, partner, partner_far, out, vel_out, stress_out, sems
):
    me = lax.axis_index("row")
    fields_out = [
        pltpu.make_async_copy(vel, vel_out, sems.at[5]),
        pltpu.make_async_copy(stress, stress_out, sems.at[6]),
    ]
    for copy in fields_out:
        copy.start()
    mine = jnp.max(flag[...]) == 1

    @pl.when(mine)
    def _():
        copies = [into(out, partner.at[n], place_of(me, 4 + n), sems.at[n]) for n in range(3)]
        copies.append(into(out, partner_far, place_of(me, 7), sems.at[3]))
        copies.append(into(out, far, place_of(me, 3), sems.at[4]))
        for copy in copies:
            copy.start()
        for copy in copies:
            copy.wait()

    for copy in fields_out:
        copy.wait()


def join_kernel(own, near, near_back, joined):
    for n, block in enumerate((own, near, near_back)):
        joined[n] = block[...]


def vmem():
    return pl.BlockSpec(memory_space=pltpu.VMEM)


def shape(*dims):
    return jax.ShapeDtypeStruct(dims, jnp.float32)


def grant(mebibytes):
    return pltpu.CompilerParams(vmem_limit_bytes=mebibytes << 20)


def step(
    velocity_start,
    stress_start,
    wind_stress,
    ocean_current,
    ice_area,
    ice_volume,
    inverse_width,
    inverse_height,
    land_block,
    ice_block,
    writer,
):
    fields, to_west, to_east, snap, flag, blank = pl.pallas_call(
        prepare_kernel,
        out_shape=(
            shape(SENT, ROWS, LANES),
            shape(SENT * 8, LANES),
            shape(SENT * 8, LANES),
            shape(10, ROWS, LANES),
            jax.ShapeDtypeStruct((8, LANES), jnp.int32),
            shape(10, ROWS, LANES),
        ),
        in_specs=[pl.BlockSpec(memory_space=pltpu.HBM)] * 11,
        out_specs=(vmem(),) * 6,
        scratch_shapes=[
            pltpu.VMEM((2, ROWS, LANES), jnp.float32),
            pltpu.VMEM((3, ROWS, LANES), jnp.float32),
            pltpu.VMEM((2, ROWS, LANES), jnp.float32),
            pltpu.VMEM((2, ROWS, LANES), jnp.float32),
            pltpu.VMEM((ROWS, LANES), jnp.float32),
            pltpu.VMEM((ROWS, LANES), jnp.float32),
            pltpu.VMEM((4, 16), jnp.int32),
            pltpu.VMEM((4, 16), jnp.int32),
            pltpu.SMEM((32,), jnp.int32),
            pltpu.SemaphoreType.DMA((11,)),
        ],
        compiler_params=grant(8),
        name="prepare",
    )(
        *(
            pltpu.with_memory_space_constraint(value, pltpu.HBM)
            for value in (
                velocity_start,
                stress_start,
                wind_stress,
                ocean_current,
                ice_area,
                ice_volume,
                inverse_width,
                inverse_height,
                land_block.T,
                ice_block.T,
                writer,
            )
        )
    )
    along = [(r, (r + 2 - 4 * (r % 2)) % 8) for r in range(8)]
    against = [(r, (r - 2 + 4 * (r % 2)) % 8) for r in range(8)]
    partner = [(r, r ^ 1) for r in range(8)]
    eastward = [(c, (c + 1) % 32) for c in range(32)]
    westward = [(c, (c - 1) % 32) for c in range(32)]
    across = [(7 * 32 + c, 7 * 32 + 31 - c) for c in range(32)]
    across += [(c, c ^ 1) for c in range(32)]
    for c in range(32):
        for r in (1, 3, 5):
            across += [(32 * r + c, 32 * r + 32 + c), (32 * r + 32 + c, 32 * r + c)]

    near = lax.ppermute(snap, "row", along)
    from_west = lax.ppermute(to_east, "col", eastward)
    from_east = lax.ppermute(to_west, "col", westward)
    near_back = lax.ppermute(snap, "row", against)

    outer, inner = pl.pallas_call(
        rows_kernel,
        out_shape=(shape(MESSAGE, LANES),) * 2,
        in_specs=[vmem()] * 3,
        out_specs=(vmem(),) * 2,
        compiler_params=grant(8),
        cost_estimate=pl.CostEstimate(flops=1000000, bytes_accessed=1000000, transcendentals=0),
        name="rows",
    )(fields, from_west, from_east)
    from_outer = lax.ppermute(outer, ("row", "col"), across)
    from_inner = lax.ppermute(inner, "row", partner)
    far = lax.ppermute(near, "row", along)

    hbm = lambda: pl.BlockSpec(memory_space=pl.ANY)
    state, restart = pl.pallas_call(
        first_half_kernel,
        out_shape=(shape(HELD, 2, TALL, LANES), shape(1, 10, 8 * ROWS, LANES)),
        in_specs=[vmem()] * 5 + [hbm(), vmem(), hbm()],
        out_specs=(vmem(), hbm()),
        scratch_shapes=[pltpu.SemaphoreType.DMA((8,))],
        compiler_params=grant(16),
        cost_estimate=pl.CostEstimate(flops=20000000, bytes_accessed=2000000, transcendentals=0),
        name="first_half",
    )(fields, from_west, from_east, from_outer, from_inner, snap, flag, blank)

    joined = pl.pallas_call(
        join_kernel,
        out_shape=shape(3, 10, ROWS, LANES),
        in_specs=[vmem()] * 3,
        out_specs=vmem(),
        compiler_params=grant(8),
        name="join",
    )(snap, near, near_back)
    partner_blocks = lax.ppermute(joined, "row", partner)

    velocity, stress, _, restart = pl.pallas_call(
        second_half_kernel,
        out_shape=(
            shape(2, ROWS, LANES),
            shape(3, ROWS, LANES),
            shape(HELD, 2, TALL, LANES),
            shape(1, 10, 8 * ROWS, LANES),
        ),
        in_specs=[vmem(), hbm(), vmem(), hbm(), hbm()],
        out_specs=(vmem(), vmem(), vmem(), hbm()),
        input_output_aliases={0: 2, 1: 3},
        scratch_shapes=[pltpu.SemaphoreType.DMA((2,))],
        compiler_params=grant(8),
        cost_estimate=pl.CostEstimate(flops=20000000, bytes_accessed=2000000, transcendentals=0),
        name="second_half",
    )(state, restart, flag, near, near_back)
    partner_far = lax.ppermute(far, "row", partner)

    restart, velocity, stress = pl.pallas_call(
        last_kernel,
        out_shape=(
            shape(1, 10, 8 * ROWS, LANES),
            shape(2, ROWS, LANES),
            shape(3, ROWS, LANES),
        ),
        in_specs=[hbm(), vmem()] + [hbm()] * 5,
        out_specs=(hbm(), hbm(), hbm()),
        input_output_aliases={0: 0},
        scratch_shapes=[pltpu.SemaphoreType.DMA((7,))],
        compiler_params=grant(4),
        name="last",
    )(restart, flag, velocity, stress, far, partner_blocks, partner_far)
    return (velocity, stress, restart)


def solution(mesh):
    return jax.shard_map(
        step,
        mesh=mesh,
        in_specs=(
            P(None, "row", "col"),
            P(None, "row", "col"),
            P(None, "row", "col"),
            P(None, "row", "col"),
            P(None, "row", "col"),
            P(None, "row", "col"),
            P("row", "col"),
            P("row", "col"),
            P("row", "col"),
            P("row", "col"),
            P(),
        ),
        out_specs=(P(None, "row", "col"), P(None, "row", "col"), P("row", None, None, "col")),
        check_vma=False,
    )
```

```python
import jax
import jax.numpy as jnp
from jax import lax
from jax.experimental import pallas as pl
from jax.experimental.pallas import tpu as pltpu
from jax.sharding import PartitionSpec as P


SUB = 12
SPLIT = 7
ROWS = 64
LANES = 128
HALO = 16
PAD = 8
TALL = PAD + HALO + ROWS + HALO + PAD
TOP = PAD + HALO + ROWS

U, V, S1, S2, S12, STR, HW, HH, INE, AA, KU, KV = range(12)
SENT = 12
BB, HWV, HHV, DU, SU, DV, SV, DP, DS, AS, AM = range(12, 23)
HELD = 23
MOVING = (U, V, INE, AA, KU, KV)
NEGATED = (U, V, KU, KV)
MESSAGE = SENT * HALO + SENT // 2 * 8


def lane_index():
    return lax.broadcasted_iota(jnp.int32, (8, LANES), 1)


def row_index():
    return lax.broadcasted_iota(jnp.int32, (8, LANES), 0)


def turned(value, steps):
    steps = steps % LANES
    return value if steps == 0 else pltpu.roll(value, steps, 1)


def west(main, side, first):
    a, b = turned(main, 1), turned(side, 1)
    return jnp.where(first, b, a), jnp.where(first, a, b)


def east(main, side, last):
    a, b = turned(main, -1), turned(side, -1)
    return jnp.where(last, b, a), jnp.where(last, a, b)


def expanded(blocks_t):
    rows = lax.broadcasted_iota(jnp.int32, (ROWS, 16), 0) // 4
    pick_rows = (rows == lax.broadcasted_iota(jnp.int32, (ROWS, 16), 1)).astype(jnp.float32)
    lanes = lax.broadcasted_iota(jnp.int32, (4, LANES), 1) // 32
    pick_lanes = (lanes == lax.broadcasted_iota(jnp.int32, (4, LANES), 0)).astype(jnp.float32)
    half = lax.dot_general(
        pick_rows, blocks_t, (((1,), (1,)), ((), ())), preferred_element_type=jnp.float32
    )
    return lax.dot_general(
        half, pick_lanes, (((1,), (0,)), ((), ())), preferred_element_type=jnp.float32
    )


def prepare_kernel(
    vel_hbm,
    stress_hbm,
    wind_hbm,
    ocean_hbm,
    area_hbm,
    volume_hbm,
    wide_hbm,
    high_hbm,
    land_hbm,
    ice_hbm,
    writer_hbm,
    fields,
    to_west,
    to_east,
    snap,
    flag,
    blank,
    vel,
    stress,
    wind,
    ocean,
    wide,
    high,
    land_t,
    ice_t,
    writer,
    sems,
):
    area, volume = snap.at[0:5], snap.at[5:10]
    moves = (
        (area_hbm, area),
        (volume_hbm, volume),
        (land_hbm, land_t),
        (ice_hbm, ice_t),
        (ocean_hbm, ocean),
        (wind_hbm, wind),
        (stress_hbm, stress),
        (vel_hbm, vel),
        (wide_hbm, wide),
        (high_hbm, high),
        (writer_hbm, writer),
    )
    copies = [pltpu.make_async_copy(a, b, sems.at[n]) for n, (a, b) in enumerate(moves)]
    for copy in copies:
        copy.start()
    blank[...] = jnp.zeros_like(blank)
    for copy in copies:
        copy.wait()
    mine = writer[lax.axis_index("col")] == lax.axis_index("row")
    flag[...] = jnp.where(mine, 1, 0) + jnp.zeros((8, LANES), jnp.int32)
    land = expanded(land_t[...].astype(jnp.float32))
    ice = expanded(ice_t[...].astype(jnp.float32))
    area_total = area[0] + area[1] + area[2] + area[3] + area[4]
    volume_total = volume[0] + volume[1] + volume[2] + volume[3] + volume[4]
    fields[U] = vel[0]
    fields[V] = vel[1]
    fields[S1] = 0.5 * stress[0]
    fields[S2] = 0.5 * stress[1]
    fields[S12] = stress[2]
    fields[STR] = (4.0 / 6.0) * volume_total * jnp.exp(-20.0 * (1.0 - area_total)) * land
    fields[HW] = 0.5 * wide[...]
    fields[HH] = 0.5 * high[...]
    inertia = 16.0 * (1.0 + volume_total)
    turning = 0.5 * (1.0 + volume_total)
    damped = inertia + 1.0
    scale = land * ice / (damped * damped + turning * turning)
    still = land * (1.0 - ice)
    fx = wind[0] + ocean[0]
    fy = wind[1] + ocean[1]
    fields[INE] = inertia
    fields[AA] = scale
    fields[KU] = scale * (damped * fx + turning * fy) + still * ocean[0]
    fields[KV] = scale * (damped * fy - turning * fx) + still * ocean[1]
    lane = lane_index()
    for f in range(SENT):
        left = right = None
        for g in range(8):
            part = fields[f, 8 * g : 8 * g + 8]
            inside = (lane >= 16 * g) & (lane < 16 * g + 16)
            a = turned(part, 16 * g)
            b = turned(part, 16 * g - 112)
            left = a if g == 0 else jnp.where(inside, a, left)
            right = b if g == 0 else jnp.where(inside, b, right)
        to_west[8 * f : 8 * f + 8] = left
        to_east[8 * f : 8 * f + 8] = right


def rows_kernel(fields, from_west, from_east, outer, inner):
    lane = lane_index()
    odd = lax.axis_index("row") % 2 == 1

    def fill(to_north, to_south):
        for f in range(SENT):
            to_north[HALO * f : HALO * f + HALO] = fields[f, ROWS - HALO : ROWS]
            to_south[HALO * f : HALO * f + HALO] = fields[f, 0:HALO]
        for pair in range(SENT // 2):
            north = south = None
            for member in range(2):
                f = 2 * pair + member
                base = 64 * member
                a = from_west[8 * f : 8 * f + 8]
                b = from_east[8 * f : 8 * f + 8]
                here = lane >= base
                there = lane >= base + 32
                n = jnp.where(there, turned(b, base + 32 - 96), turned(a, base - 96))
                s = jnp.where(there, turned(b, base + 32), turned(a, base))
                north = n if member == 0 else jnp.where(here, n, north)
                south = s if member == 0 else jnp.where(here, s, south)
            at = SENT * HALO + 8 * pair
            to_north[at : at + 8] = north
            to_south[at : at + 8] = south

    @pl.when(odd)
    def _():
        fill(outer, inner)

    @pl.when(jnp.logical_not(odd))
    def _():
        fill(inner, outer)


def stencil_masks():
    lane, row = lane_index(), row_index()
    is_top = lax.axis_index("row") == 7
    top_rows = (jnp.where(is_top, 1, 0) + jnp.zeros((8, LANES), jnp.int32)) == 1
    return lane == 0, lane == LANES - 1, row, top_rows


def assemble(fields, from_west, from_east, from_outer, from_inner, held):
    is_top = lax.axis_index("row") == 7
    odd = lax.axis_index("row") % 2 + jnp.zeros((8, LANES), jnp.int32) == 1
    lane = lane_index()
    row = row_index()
    first, last, low = lane == 0, lane == LANES - 1, lane < 64

    bottom = lax.axis_index("row") + jnp.zeros((8, LANES), jnp.int32) == 0

    def south(at):
        value = jnp.where(odd, from_inner[at : at + 8], from_outer[at : at + 8])
        return jnp.where(bottom, 0.0, value)

    def north(at):
        return jnp.where(odd, from_outer[at : at + 8], from_inner[at : at + 8])

    def side_rows(message, f, a):
        base = 64 * (f % 2)
        corner = message(SENT * HALO + 8 * (f // 2))
        return jnp.where(low, turned(corner, -(base + 32 + 16 * a)), turned(corner, 112 - base - 16 * a))

    for f in range(SENT):
        a, b = from_west[8 * f : 8 * f + 8], from_east[8 * f : 8 * f + 8]
        for g in range(8):
            at = PAD + HALO + 8 * g
            held[f, 0, at : at + 8] = fields[f, 8 * g : 8 * g + 8]
            held[f, 1, at : at + 8] = jnp.where(low, turned(b, -16 * g), turned(a, 112 - 16 * g))
        for g in range(2):
            at = PAD + 8 * g
            held[f, 0, at : at + 8] = south(HALO * f + 8 * g)
            held[f, 1, at : at + 8] = side_rows(south, f, g)

    @pl.when(jnp.logical_not(is_top))
    def _():
        for f in range(SENT):
            for g in range(2):
                at = TOP + 8 * g
                held[f, 0, at : at + 8] = north(HALO * f + 8 * g)
                held[f, 1, at : at + 8] = side_rows(north, f, g)

    @pl.when(is_top)
    def _():
        def rotated(value):
            value = jnp.take_along_axis(value, LANES - 1 - lane, axis=1)
            return jnp.take_along_axis(value, 7 - row, axis=0)

        for f in range(SENT):
            for g in range(2):
                source = 1 - g
                main = rotated(north(HALO * f + 8 * source))
                side = rotated(side_rows(north, f, source))
                if f in MOVING:
                    main, side = east(main, side, last)
                    if f in NEGATED:
                        main, side = -main, -side
                    at = TOP + 8 * g
                else:
                    at = TOP + 1 + 8 * g
                held[f, 0, at : at + 8] = main
                held[f, 1, at : at + 8] = side
                if f in (HW, HH):
                    main, side = east(main, side, last)
                    own = HWV if f == HW else HHV
                    held[own, 0, TOP + 8 * g : TOP + 8 * g + 8] = main
                    held[own, 1, TOP + 8 * g : TOP + 8 * g + 8] = side

    for g in range(12):
        at = PAD + 8 * g
        for t in range(2):
            scale = held[AA, t, at : at + 8]
            inertia = held[INE, t, at : at + 8]
            held[AA, t, at : at + 8] = (inertia + 1.0) * scale
            held[BB, t, at : at + 8] = (inertia * (1.0 / 32.0)) * scale
            if g < 10:
                held[HWV, t, at : at + 8] = held[HW, t, at : at + 8]
                held[HHV, t, at : at + 8] = held[HH, t, at : at + 8]
        velocity_sums(
            held,
            at,
            held[U, 0, at : at + 8],
            held[U, 1, at : at + 8],
            held[V, 0, at : at + 8],
            held[V, 1, at : at + 8],
            first,
        )

    @pl.when(jnp.logical_not(is_top))
    def _():
        for t in range(2):
            held[HWV, t, TOP : TOP + HALO] = held[HW, t, TOP : TOP + HALO]
            held[HHV, t, TOP : TOP + HALO] = held[HH, t, TOP : TOP + HALO]


def velocity_sums(held, at, um, us, vm, vs, first):
    wum, wus = west(um, us, first)
    wvm, wvs = west(vm, vs, first)
    for t, (x, wx, y, wy) in enumerate(((um, wum, vm, wvm), (us, wus, vs, wvs))):
        held[DU, t, at : at + 8] = x - wx
        held[SU, t, at : at + 8] = x + wx
        held[DV, t, at : at + 8] = y - wy
        held[SV, t, at : at + 8] = y + wy


def stress_rows(held, at, last):
    fresh = []
    for t in range(2):
        here = lambda f: held[f, t, at : at + 8]
        below = lambda f: held[f, t, at - 1 : at + 7]
        hw, hh = here(HW), here(HH)
        gux = hw * (here(DU) + below(DU))
        guy = hh * (here(SU) - below(SU))
        gvx = hw * (here(DV) + below(DV))
        gvy = hh * (here(SV) - below(SV))
        divergence = gux + gvy
        tension = gux - gvy
        shearing = guy + gvx
        deform = jnp.sqrt(
            divergence * divergence + 0.25 * (tension * tension + shearing * shearing)
        )
        viscous = here(STR) / (deform + 0.5)
        quarter = 0.25 * viscous
        s1 = here(S1) * (2.0 / 3.0) + viscous * (divergence - deform)
        s2 = here(S2) * (2.0 / 3.0) + quarter * tension
        s12 = here(S12) * (2.0 / 3.0) + quarter * shearing
        held[S1, t, at : at + 8] = s1
        held[S2, t, at : at + 8] = s2
        held[S12, t, at : at + 8] = s12
        fresh.append((s1 + s2, s1 - s2, s12))
    (pm, mm, qm), (ps, ms, qs) = fresh
    epm, eps = east(pm, ps, last)
    emm, ems = east(mm, ms, last)
    eqm, eqs = east(qm, qs, last)
    for t, (p, ep, m, em, q, eq) in enumerate(
        ((pm, epm, mm, emm, qm, eqm), (ps, eps, ms, ems, qs, eqs))
    ):
        held[DP, t, at : at + 8] = ep - p
        held[AM, t, at : at + 8] = em + m
        held[DS, t, at : at + 8] = eq - q
        held[AS, t, at : at + 8] = eq + q


def velocity_rows(held, at, first, row, top_rows):
    fresh = []
    for t in range(2):
        here = lambda f: held[f, t, at : at + 8]

        def pair(f):
            own, above = here(f), held[f, t, at + 1 : at + 9]
            if at == TOP - 8:
                above = jnp.where((row == 7) & top_rows, held[f, t, at + 2 : at + 10], above)
            if at == TOP:
                own = jnp.where((row == 0) & top_rows, held[f, t, at - 1 : at + 7], own)
            return own, above

        hw, hh = here(HWV), here(HHV)
        dp, ndp = pair(DP)
        ds, nds = pair(DS)
        as_, nas = pair(AS)
        am, nam = pair(AM)
        inertia, a, b = here(INE), here(AA), here(BB)
        x = inertia * here(U) + (hw * (dp + ndp) + hh * (nas - as_))
        y = inertia * here(V) + (hw * (ds + nds) + hh * (nam - am))
        u = a * x + b * y + here(KU)
        v = a * y - b * x + here(KV)
        held[U, t, at : at + 8] = u
        held[V, t, at : at + 8] = v
        fresh.append((u, v))
    (um, vm), (us, vs) = fresh
    velocity_sums(held, at, um, us, vm, vs, first)


def subcycles(held, start, stop, lo, hi):
    first, last, row, top_rows = stencil_masks()

    def body(_, carry):
        for g in range(lo, hi):
            stress_rows(held, PAD + 8 * g, last)
        for g in range(lo, hi):
            velocity_rows(held, PAD + 8 * g, first, row, top_rows)
        return carry

    lax.fori_loop(start, stop, body, 0)


def place_of(me, which):
    chip, core = me // 2, me % 2
    step = 2 * core - 1
    if which >= 4:
        core = 1 - core
        which -= 4
        step = -step
    chips = (chip, lax.rem(chip - step + 4, 4), lax.rem(chip + step + 4, 4), lax.rem(chip + 2, 4))
    return (2 * chips[which] + core) * ROWS


def into(out, ref, place, sem):
    return pltpu.make_async_copy(ref, out.at[0, :, pl.ds(place, ROWS), :], sem)


def first_half_kernel(
    fields, from_west, from_east, from_outer, from_inner, snap, flag, zero, held, out, sems
):
    me = lax.axis_index("row")
    mine = jnp.max(flag[...]) == 1
    zeros = [into(out, zero, n * ROWS, sems.at[n]) for n in range(8)]
    own = into(out, snap, place_of(me, 0), sems.at[0])

    @pl.when(mine)
    def _():
        own.start()

    @pl.when(jnp.logical_not(mine))
    def _():
        for copy in zeros:
            copy.start()

    assemble(fields, from_west, from_east, from_outer, from_inner, held)
    subcycles(held, 0, 5, 0, 12)
    subcycles(held, 5, SPLIT, 1, 11)

    @pl.when(mine)
    def _():
        own.wait()

    @pl.when(jnp.logical_not(mine))
    def _():
        for copy in zeros:
            copy.wait()


def second_half_kernel(state, out_in, flag, near, near_back, vel, stress, held, out, sems):
    me = lax.axis_index("row")
    mine = jnp.max(flag[...]) == 1
    copies = [
        into(out, near, place_of(me, 1), sems.at[0]),
        into(out, near_back, place_of(me, 2), sems.at[1]),
    ]

    @pl.when(mine)
    def _():
        for copy in copies:
            copy.start()

    subcycles(held, SPLIT, SUB, 1, 11)
    at = PAD + HALO
    vel[0] = held[U, 0, at : at + ROWS]
    vel[1] = held[V, 0, at : at + ROWS]
    stress[0] = 2.0 * held[S1, 0, at : at + ROWS]
    stress[1] = 2.0 * held[S2, 0, at : at + ROWS]
    stress[2] = held[S12, 0, at : at + ROWS]

    @pl.when(mine)
    def _():
        for copy in copies:
            copy.wait()


def last_kernel(
    out_in, flag, vel, stress, far, partner, partner_far, out, vel_out, stress_out, sems
):
    me = lax.axis_index("row")
    fields_out = [
        pltpu.make_async_copy(vel, vel_out, sems.at[5]),
        pltpu.make_async_copy(stress, stress_out, sems.at[6]),
    ]
    for copy in fields_out:
        copy.start()
    mine = jnp.max(flag[...]) == 1

    @pl.when(mine)
    def _():
        copies = [into(out, partner.at[n], place_of(me, 4 + n), sems.at[n]) for n in range(3)]
        copies.append(into(out, partner_far, place_of(me, 7), sems.at[3]))
        copies.append(into(out, far, place_of(me, 3), sems.at[4]))
        for copy in copies:
            copy.start()
        for copy in copies:
            copy.wait()

    for copy in fields_out:
        copy.wait()


def join_kernel(own, near, near_back, joined):
    for n, block in enumerate((own, near, near_back)):
        joined[n] = block[...]


def vmem():
    return pl.BlockSpec(memory_space=pltpu.VMEM)


def shape(*dims):
    return jax.ShapeDtypeStruct(dims, jnp.float32)


def grant(mebibytes):
    return pltpu.CompilerParams(vmem_limit_bytes=mebibytes << 20)


def step(
    velocity_start,
    stress_start,
    wind_stress,
    ocean_current,
    ice_area,
    ice_volume,
    inverse_width,
    inverse_height,
    land_block,
    ice_block,
    writer,
):
    fields, to_west, to_east, snap, flag, blank = pl.pallas_call(
        prepare_kernel,
        out_shape=(
            shape(SENT, ROWS, LANES),
            shape(SENT * 8, LANES),
            shape(SENT * 8, LANES),
            shape(10, ROWS, LANES),
            jax.ShapeDtypeStruct((8, LANES), jnp.int32),
            shape(10, ROWS, LANES),
        ),
        in_specs=[pl.BlockSpec(memory_space=pltpu.HBM)] * 11,
        out_specs=(vmem(),) * 6,
        scratch_shapes=[
            pltpu.VMEM((2, ROWS, LANES), jnp.float32),
            pltpu.VMEM((3, ROWS, LANES), jnp.float32),
            pltpu.VMEM((2, ROWS, LANES), jnp.float32),
            pltpu.VMEM((2, ROWS, LANES), jnp.float32),
            pltpu.VMEM((ROWS, LANES), jnp.float32),
            pltpu.VMEM((ROWS, LANES), jnp.float32),
            pltpu.VMEM((4, 16), jnp.int32),
            pltpu.VMEM((4, 16), jnp.int32),
            pltpu.SMEM((32,), jnp.int32),
            pltpu.SemaphoreType.DMA((11,)),
        ],
        compiler_params=grant(8),
        name="prepare",
    )(
        *(
            pltpu.with_memory_space_constraint(value, pltpu.HBM)
            for value in (
                velocity_start,
                stress_start,
                wind_stress,
                ocean_current,
                ice_area,
                ice_volume,
                inverse_width,
                inverse_height,
                land_block.T,
                ice_block.T,
                writer,
            )
        )
    )
    along = [(r, (r - 2 + 4 * (r % 2)) % 8) for r in range(8)]
    against = [(r, (r + 2 - 4 * (r % 2)) % 8) for r in range(8)]
    partner = [(r, r ^ 1) for r in range(8)]
    eastward = [(c, (c + 1) % 32) for c in range(32)]
    westward = [(c, (c - 1) % 32) for c in range(32)]
    across = [(7 * 32 + c, 7 * 32 + 31 - c) for c in range(32)]
    across += [(c, c ^ 1) for c in range(32)]
    for c in range(32):
        for r in (1, 3, 5):
            across += [(32 * r + c, 32 * r + 32 + c), (32 * r + 32 + c, 32 * r + c)]

    near = lax.ppermute(snap, "row", along)
    from_west = lax.ppermute(to_east, "col", eastward)
    from_east = lax.ppermute(to_west, "col", westward)
    near_back = lax.ppermute(snap, "row", against)

    outer, inner = pl.pallas_call(
        rows_kernel,
        out_shape=(shape(MESSAGE, LANES),) * 2,
        in_specs=[vmem()] * 3,
        out_specs=(vmem(),) * 2,
        compiler_params=grant(8),
        cost_estimate=pl.CostEstimate(flops=1000000, bytes_accessed=1000000, transcendentals=0),
        name="rows",
    )(fields, from_west, from_east)
    from_outer = lax.ppermute(outer, ("row", "col"), across)
    from_inner = lax.ppermute(inner, "row", partner)
    far = lax.ppermute(near, "row", along)

    hbm = lambda: pl.BlockSpec(memory_space=pl.ANY)
    state, restart = pl.pallas_call(
        first_half_kernel,
        out_shape=(shape(HELD, 2, TALL, LANES), shape(1, 10, 8 * ROWS, LANES)),
        in_specs=[vmem()] * 5 + [hbm(), vmem(), hbm()],
        out_specs=(vmem(), hbm()),
        scratch_shapes=[pltpu.SemaphoreType.DMA((8,))],
        compiler_params=grant(16),
        cost_estimate=pl.CostEstimate(flops=20000000, bytes_accessed=2000000, transcendentals=0),
        name="first_half",
    )(fields, from_west, from_east, from_outer, from_inner, snap, flag, blank)

    joined = pl.pallas_call(
        join_kernel,
        out_shape=shape(3, 10, ROWS, LANES),
        in_specs=[vmem()] * 3,
        out_specs=vmem(),
        compiler_params=grant(8),
        name="join",
    )(snap, near, near_back)
    partner_blocks = lax.ppermute(joined, "row", partner)

    velocity, stress, _, restart = pl.pallas_call(
        second_half_kernel,
        out_shape=(
            shape(2, ROWS, LANES),
            shape(3, ROWS, LANES),
            shape(HELD, 2, TALL, LANES),
            shape(1, 10, 8 * ROWS, LANES),
        ),
        in_specs=[vmem(), hbm(), vmem(), hbm(), hbm()],
        out_specs=(vmem(), vmem(), vmem(), hbm()),
        input_output_aliases={0: 2, 1: 3},
        scratch_shapes=[pltpu.SemaphoreType.DMA((2,))],
        compiler_params=grant(8),
        cost_estimate=pl.CostEstimate(flops=20000000, bytes_accessed=2000000, transcendentals=0),
        name="second_half",
    )(state, restart, flag, near, near_back)
    partner_far = lax.ppermute(far, "row", partner)

    restart, velocity, stress = pl.pallas_call(
        last_kernel,
        out_shape=(
            shape(1, 10, 8 * ROWS, LANES),
            shape(2, ROWS, LANES),
            shape(3, ROWS, LANES),
        ),
        in_specs=[hbm(), vmem()] + [hbm()] * 5,
        out_specs=(hbm(), hbm(), hbm()),
        input_output_aliases={0: 0},
        scratch_shapes=[pltpu.SemaphoreType.DMA((7,))],
        compiler_params=grant(4),
        name="last",
    )(restart, flag, velocity, stress, far, partner_blocks, partner_far)
    return (velocity, stress, restart)


def solution(mesh):
    return jax.shard_map(
        step,
        mesh=mesh,
        in_specs=(
            P(None, "row", "col"),
            P(None, "row", "col"),
            P(None, "row", "col"),
            P(None, "row", "col"),
            P(None, "row", "col"),
            P(None, "row", "col"),
            P("row", "col"),
            P("row", "col"),
            P("row", "col"),
            P("row", "col"),
            P(),
        ),
        out_specs=(P(None, "row", "col"), P(None, "row", "col"), P("row", None, None, "col")),
        check_vma=False,
    )
```

```python
import jax
import jax.numpy as jnp
from jax import lax
from jax.experimental import pallas as pl
from jax.experimental.pallas import tpu as pltpu
from jax.sharding import PartitionSpec as P


SUB = 12
SPLIT = 7
ROWS = 64
LANES = 128
HALO = 16
PAD = 8
TALL = PAD + HALO + ROWS + HALO + PAD
TOP = PAD + HALO + ROWS

U, V, S1, S2, S12, STR, HW, HH, INE, AA, KU, KV = range(12)
SENT = 12
BB, HWV, HHV, DU, SU, DV, SV, DP, DS, AS, AM = range(12, 23)
HELD = 23
MOVING = (U, V, INE, AA, KU, KV)
NEGATED = (U, V, KU, KV)
MESSAGE = SENT * HALO + SENT // 2 * 8


def lane_index():
    return lax.broadcasted_iota(jnp.int32, (8, LANES), 1)


def row_index():
    return lax.broadcasted_iota(jnp.int32, (8, LANES), 0)


def turned(value, steps):
    steps = steps % LANES
    return value if steps == 0 else pltpu.roll(value, steps, 1)


def west(main, side, first):
    a, b = turned(main, 1), turned(side, 1)
    return jnp.where(first, b, a), jnp.where(first, a, b)


def east(main, side, last):
    a, b = turned(main, -1), turned(side, -1)
    return jnp.where(last, b, a), jnp.where(last, a, b)


def expanded(blocks_t):
    rows = lax.broadcasted_iota(jnp.int32, (ROWS, 16), 0) // 4
    pick_rows = (rows == lax.broadcasted_iota(jnp.int32, (ROWS, 16), 1)).astype(jnp.float32)
    lanes = lax.broadcasted_iota(jnp.int32, (4, LANES), 1) // 32
    pick_lanes = (lanes == lax.broadcasted_iota(jnp.int32, (4, LANES), 0)).astype(jnp.float32)
    half = lax.dot_general(
        pick_rows, blocks_t, (((1,), (1,)), ((), ())), preferred_element_type=jnp.float32
    )
    return lax.dot_general(
        half, pick_lanes, (((1,), (0,)), ((), ())), preferred_element_type=jnp.float32
    )


def prepare_kernel(
    vel_hbm,
    stress_hbm,
    wind_hbm,
    ocean_hbm,
    area_hbm,
    volume_hbm,
    wide_hbm,
    high_hbm,
    land_hbm,
    ice_hbm,
    writer_hbm,
    fields,
    to_west,
    to_east,
    snap,
    flag,
    blank,
    vel,
    stress,
    wind,
    ocean,
    wide,
    high,
    land_t,
    ice_t,
    writer,
    sems,
):
    area, volume = snap.at[0:5], snap.at[5:10]
    moves = (
        (area_hbm, area),
        (volume_hbm, volume),
        (land_hbm, land_t),
        (ice_hbm, ice_t),
        (ocean_hbm, ocean),
        (wind_hbm, wind),
        (stress_hbm, stress),
        (vel_hbm, vel),
        (wide_hbm, wide),
        (high_hbm, high),
        (writer_hbm, writer),
    )
    copies = [pltpu.make_async_copy(a, b, sems.at[n]) for n, (a, b) in enumerate(moves)]
    for copy in copies:
        copy.start()
    blank[...] = jnp.zeros_like(blank)
    for copy in copies:
        copy.wait()
    mine = writer[lax.axis_index("col")] == lax.axis_index("row")
    flag[...] = jnp.where(mine, 1, 0) + jnp.zeros((8, LANES), jnp.int32)
    land = expanded(land_t[...].astype(jnp.float32))
    ice = expanded(ice_t[...].astype(jnp.float32))
    area_total = area[0] + area[1] + area[2] + area[3] + area[4]
    volume_total = volume[0] + volume[1] + volume[2] + volume[3] + volume[4]
    fields[U] = vel[0]
    fields[V] = vel[1]
    fields[S1] = 0.5 * stress[0]
    fields[S2] = 0.5 * stress[1]
    fields[S12] = stress[2]
    fields[STR] = (4.0 / 6.0) * volume_total * jnp.exp(-20.0 * (1.0 - area_total)) * land
    fields[HW] = 0.5 * wide[...]
    fields[HH] = 0.5 * high[...]
    inertia = 16.0 * (1.0 + volume_total)
    turning = 0.5 * (1.0 + volume_total)
    damped = inertia + 1.0
    scale = land * ice / (damped * damped + turning * turning)
    still = land * (1.0 - ice)
    fx = wind[0] + ocean[0]
    fy = wind[1] + ocean[1]
    fields[INE] = inertia
    fields[AA] = scale
    fields[KU] = scale * (damped * fx + turning * fy) + still * ocean[0]
    fields[KV] = scale * (damped * fy - turning * fx) + still * ocean[1]
    lane = lane_index()
    for f in range(SENT):
        left = right = None
        for g in range(8):
            part = fields[f, 8 * g : 8 * g + 8]
            inside = (lane >= 16 * g) & (lane < 16 * g + 16)
            a = turned(part, 16 * g)
            b = turned(part, 16 * g - 112)
            left = a if g == 0 else jnp.where(inside, a, left)
            right = b if g == 0 else jnp.where(inside, b, right)
        to_west[8 * f : 8 * f + 8] = left
        to_east[8 * f : 8 * f + 8] = right


def rows_kernel(fields, from_west, from_east, outer, inner):
    lane = lane_index()
    odd = lax.axis_index("row") % 2 == 1

    def fill(to_north, to_south):
        for f in range(SENT):
            to_north[HALO * f : HALO * f + HALO] = fields[f, ROWS - HALO : ROWS]
            to_south[HALO * f : HALO * f + HALO] = fields[f, 0:HALO]
        for pair in range(SENT // 2):
            north = south = None
            for member in range(2):
                f = 2 * pair + member
                base = 64 * member
                a = from_west[8 * f : 8 * f + 8]
                b = from_east[8 * f : 8 * f + 8]
                here = lane >= base
                there = lane >= base + 32
                n = jnp.where(there, turned(b, base + 32 - 96), turned(a, base - 96))
                s = jnp.where(there, turned(b, base + 32), turned(a, base))
                north = n if member == 0 else jnp.where(here, n, north)
                south = s if member == 0 else jnp.where(here, s, south)
            at = SENT * HALO + 8 * pair
            to_north[at : at + 8] = north
            to_south[at : at + 8] = south

    @pl.when(odd)
    def _():
        fill(outer, inner)

    @pl.when(jnp.logical_not(odd))
    def _():
        fill(inner, outer)


def stencil_masks():
    lane, row = lane_index(), row_index()
    is_top = lax.axis_index("row") == 7
    top_rows = (jnp.where(is_top, 1, 0) + jnp.zeros((8, LANES), jnp.int32)) == 1
    return lane == 0, lane == LANES - 1, row, top_rows


def own_kernel(fields, from_west, from_east, held):
    lane = lane_index()
    for f in range(SENT):
        a, b = from_west[8 * f : 8 * f + 8], from_east[8 * f : 8 * f + 8]
        for g in range(8):
            at = PAD + HALO + 8 * g
            held[f, 0, at : at + 8] = fields[f, 8 * g : 8 * g + 8]
            held[f, 1, at : at + 8] = jnp.where(lane < 64, turned(b, -16 * g), turned(a, 112 - 16 * g))
    for g in range(2, 10):
        derive(held, g, lane == 0)
        same_sizes(held, g)


def same_sizes(held, g):
    rows = slice(PAD + 8 * g, PAD + 8 * g + 8)
    for t in range(2):
        held[HWV, t, rows] = held[HW, t, rows]
        held[HHV, t, rows] = held[HH, t, rows]


def derive(held, g, first):
    at = PAD + 8 * g
    rows = slice(at, at + 8)
    for t in range(2):
        scale = held[AA, t, rows]
        inertia = held[INE, t, rows]
        held[AA, t, rows] = (inertia + 1.0) * scale
        held[BB, t, rows] = (inertia * (1.0 / 32.0)) * scale
    velocity_sums(
        held, at, held[U, 0, rows], held[U, 1, rows], held[V, 0, rows], held[V, 1, rows], first
    )


def assemble(from_outer, from_inner, held):
    is_top = lax.axis_index("row") == 7
    odd = lax.axis_index("row") % 2 + jnp.zeros((8, LANES), jnp.int32) == 1
    lane = lane_index()
    row = row_index()
    first, last, low = lane == 0, lane == LANES - 1, lane < 64

    bottom = lax.axis_index("row") + jnp.zeros((8, LANES), jnp.int32) == 0

    def south(at):
        value = jnp.where(odd, from_inner[at : at + 8], from_outer[at : at + 8])
        return jnp.where(bottom, 0.0, value)

    def north(at):
        return jnp.where(odd, from_outer[at : at + 8], from_inner[at : at + 8])

    def side_rows(message, f, a):
        base = 64 * (f % 2)
        corner = message(SENT * HALO + 8 * (f // 2))
        return jnp.where(low, turned(corner, -(base + 32 + 16 * a)), turned(corner, 112 - base - 16 * a))

    for f in range(SENT):
        for g in range(2):
            at = PAD + 8 * g
            held[f, 0, at : at + 8] = south(HALO * f + 8 * g)
            held[f, 1, at : at + 8] = side_rows(south, f, g)

    @pl.when(jnp.logical_not(is_top))
    def _():
        for f in range(SENT):
            for g in range(2):
                at = TOP + 8 * g
                held[f, 0, at : at + 8] = north(HALO * f + 8 * g)
                held[f, 1, at : at + 8] = side_rows(north, f, g)

    @pl.when(is_top)
    def _():
        def rotated(value):
            value = jnp.take_along_axis(value, LANES - 1 - lane, axis=1)
            return jnp.take_along_axis(value, 7 - row, axis=0)

        for f in range(SENT):
            for g in range(2):
                source = 1 - g
                main = rotated(north(HALO * f + 8 * source))
                side = rotated(side_rows(north, f, source))
                if f in MOVING:
                    main, side = east(main, side, last)
                    if f in NEGATED:
                        main, side = -main, -side
                    at = TOP + 8 * g
                else:
                    at = TOP + 1 + 8 * g
                held[f, 0, at : at + 8] = main
                held[f, 1, at : at + 8] = side
                if f in (HW, HH):
                    main, side = east(main, side, last)
                    own = HWV if f == HW else HHV
                    held[own, 0, TOP + 8 * g : TOP + 8 * g + 8] = main
                    held[own, 1, TOP + 8 * g : TOP + 8 * g + 8] = side

    for g in (0, 1):
        derive(held, g, first)
        same_sizes(held, g)
    for g in (10, 11):
        derive(held, g, first)

    @pl.when(jnp.logical_not(is_top))
    def _():
        for g in (10, 11):
            same_sizes(held, g)


def velocity_sums(held, at, um, us, vm, vs, first):
    wum, wus = west(um, us, first)
    wvm, wvs = west(vm, vs, first)
    for t, (x, wx, y, wy) in enumerate(((um, wum, vm, wvm), (us, wus, vs, wvs))):
        held[DU, t, at : at + 8] = x - wx
        held[SU, t, at : at + 8] = x + wx
        held[DV, t, at : at + 8] = y - wy
        held[SV, t, at : at + 8] = y + wy


def stress_rows(held, at, last):
    fresh = []
    for t in range(2):
        here = lambda f: held[f, t, at : at + 8]
        below = lambda f: held[f, t, at - 1 : at + 7]
        hw, hh = here(HW), here(HH)
        gux = hw * (here(DU) + below(DU))
        guy = hh * (here(SU) - below(SU))
        gvx = hw * (here(DV) + below(DV))
        gvy = hh * (here(SV) - below(SV))
        divergence = gux + gvy
        tension = gux - gvy
        shearing = guy + gvx
        deform = jnp.sqrt(
            divergence * divergence + 0.25 * (tension * tension + shearing * shearing)
        )
        viscous = here(STR) / (deform + 0.5)
        quarter = 0.25 * viscous
        s1 = here(S1) * (2.0 / 3.0) + viscous * (divergence - deform)
        s2 = here(S2) * (2.0 / 3.0) + quarter * tension
        s12 = here(S12) * (2.0 / 3.0) + quarter * shearing
        held[S1, t, at : at + 8] = s1
        held[S2, t, at : at + 8] = s2
        held[S12, t, at : at + 8] = s12
        fresh.append((s1 + s2, s1 - s2, s12))
    (pm, mm, qm), (ps, ms, qs) = fresh
    epm, eps = east(pm, ps, last)
    emm, ems = east(mm, ms, last)
    eqm, eqs = east(qm, qs, last)
    for t, (p, ep, m, em, q, eq) in enumerate(
        ((pm, epm, mm, emm, qm, eqm), (ps, eps, ms, ems, qs, eqs))
    ):
        held[DP, t, at : at + 8] = ep - p
        held[AM, t, at : at + 8] = em + m
        held[DS, t, at : at + 8] = eq - q
        held[AS, t, at : at + 8] = eq + q


def velocity_rows(held, at, first, row, top_rows):
    fresh = []
    for t in range(2):
        here = lambda f: held[f, t, at : at + 8]

        def pair(f):
            own, above = here(f), held[f, t, at + 1 : at + 9]
            if at == TOP - 8:
                above = jnp.where((row == 7) & top_rows, held[f, t, at + 2 : at + 10], above)
            if at == TOP:
                own = jnp.where((row == 0) & top_rows, held[f, t, at - 1 : at + 7], own)
            return own, above

        hw, hh = here(HWV), here(HHV)
        dp, ndp = pair(DP)
        ds, nds = pair(DS)
        as_, nas = pair(AS)
        am, nam = pair(AM)
        inertia, a, b = here(INE), here(AA), here(BB)
        x = inertia * here(U) + (hw * (dp + ndp) + hh * (nas - as_))
        y = inertia * here(V) + (hw * (ds + nds) + hh * (nam - am))
        u = a * x + b * y + here(KU)
        v = a * y - b * x + here(KV)
        held[U, t, at : at + 8] = u
        held[V, t, at : at + 8] = v
        fresh.append((u, v))
    (um, vm), (us, vs) = fresh
    velocity_sums(held, at, um, us, vm, vs, first)


def subcycles(held, start, stop, lo, hi):
    first, last, row, top_rows = stencil_masks()

    def body(_, carry):
        for g in range(lo, hi):
            stress_rows(held, PAD + 8 * g, last)
        for g in range(lo, hi):
            velocity_rows(held, PAD + 8 * g, first, row, top_rows)
        return carry

    lax.fori_loop(start, stop, body, 0)


def place_of(me, which):
    chip, core = me // 2, me % 2
    step = 2 * core - 1
    if which >= 4:
        core = 1 - core
        which -= 4
        step = -step
    chips = (chip, lax.rem(chip - step + 4, 4), lax.rem(chip + step + 4, 4), lax.rem(chip + 2, 4))
    return (2 * chips[which] + core) * ROWS


def into(out, ref, place, sem):
    return pltpu.make_async_copy(ref, out.at[0, :, pl.ds(place, ROWS), :], sem)


def first_half_kernel(
    state, from_outer, from_inner, snap, flag, zero, held, out, sems
):
    me = lax.axis_index("row")
    mine = jnp.max(flag[...]) == 1
    zeros = [into(out, zero, n * ROWS, sems.at[n]) for n in range(8)]
    own = into(out, snap, place_of(me, 0), sems.at[0])

    @pl.when(mine)
    def _():
        own.start()

    @pl.when(jnp.logical_not(mine))
    def _():
        for copy in zeros:
            copy.start()

    assemble(from_outer, from_inner, held)
    subcycles(held, 0, 5, 0, 12)
    subcycles(held, 5, SPLIT, 1, 11)

    @pl.when(mine)
    def _():
        own.wait()

    @pl.when(jnp.logical_not(mine))
    def _():
        for copy in zeros:
            copy.wait()


def second_half_kernel(state, out_in, flag, near, near_back, vel, stress, held, out, sems):
    me = lax.axis_index("row")
    mine = jnp.max(flag[...]) == 1
    copies = [
        into(out, near, place_of(me, 1), sems.at[0]),
        into(out, near_back, place_of(me, 2), sems.at[1]),
    ]

    @pl.when(mine)
    def _():
        for copy in copies:
            copy.start()

    subcycles(held, SPLIT, SUB, 1, 11)
    at = PAD + HALO
    vel[0] = held[U, 0, at : at + ROWS]
    vel[1] = held[V, 0, at : at + ROWS]
    stress[0] = 2.0 * held[S1, 0, at : at + ROWS]
    stress[1] = 2.0 * held[S2, 0, at : at + ROWS]
    stress[2] = held[S12, 0, at : at + ROWS]

    @pl.when(mine)
    def _():
        for copy in copies:
            copy.wait()


def late_kernel(out_in, flag, vel, stress, far, partner, out, vel_out, stress_out, sems):
    me = lax.axis_index("row")
    fields_out = [
        pltpu.make_async_copy(vel, vel_out, sems.at[4]),
        pltpu.make_async_copy(stress, stress_out, sems.at[5]),
    ]
    for copy in fields_out:
        copy.start()
    mine = jnp.max(flag[...]) == 1

    @pl.when(mine)
    def _():
        copies = [into(out, partner.at[n], place_of(me, 4 + n), sems.at[n]) for n in range(3)]
        copies.append(into(out, far, place_of(me, 3), sems.at[3]))
        for copy in copies:
            copy.start()
        for copy in copies:
            copy.wait()

    for copy in fields_out:
        copy.wait()


def last_kernel(out_in, flag, partner_far, out, sem):
    mine = jnp.max(flag[...]) == 1

    @pl.when(mine)
    def _():
        copy = into(out, partner_far, place_of(lax.axis_index("row"), 7), sem)
        copy.start()
        copy.wait()


def join_kernel(own, near, near_back, joined):
    for n, block in enumerate((own, near, near_back)):
        joined[n] = block[...]


def vmem():
    return pl.BlockSpec(memory_space=pltpu.VMEM)


def shape(*dims):
    return jax.ShapeDtypeStruct(dims, jnp.float32)


def grant(mebibytes):
    return pltpu.CompilerParams(vmem_limit_bytes=mebibytes << 20)


def step(
    velocity_start,
    stress_start,
    wind_stress,
    ocean_current,
    ice_area,
    ice_volume,
    inverse_width,
    inverse_height,
    land_block,
    ice_block,
    writer,
):
    fields, to_west, to_east, snap, flag, blank = pl.pallas_call(
        prepare_kernel,
        out_shape=(
            shape(SENT, ROWS, LANES),
            shape(SENT * 8, LANES),
            shape(SENT * 8, LANES),
            shape(10, ROWS, LANES),
            jax.ShapeDtypeStruct((8, LANES), jnp.int32),
            shape(10, ROWS, LANES),
        ),
        in_specs=[pl.BlockSpec(memory_space=pltpu.HBM)] * 11,
        out_specs=(vmem(),) * 6,
        scratch_shapes=[
            pltpu.VMEM((2, ROWS, LANES), jnp.float32),
            pltpu.VMEM((3, ROWS, LANES), jnp.float32),
            pltpu.VMEM((2, ROWS, LANES), jnp.float32),
            pltpu.VMEM((2, ROWS, LANES), jnp.float32),
            pltpu.VMEM((ROWS, LANES), jnp.float32),
            pltpu.VMEM((ROWS, LANES), jnp.float32),
            pltpu.VMEM((4, 16), jnp.int32),
            pltpu.VMEM((4, 16), jnp.int32),
            pltpu.SMEM((32,), jnp.int32),
            pltpu.SemaphoreType.DMA((11,)),
        ],
        compiler_params=grant(8),
        name="prepare",
    )(
        *(
            pltpu.with_memory_space_constraint(value, pltpu.HBM)
            for value in (
                velocity_start,
                stress_start,
                wind_stress,
                ocean_current,
                ice_area,
                ice_volume,
                inverse_width,
                inverse_height,
                land_block.T,
                ice_block.T,
                writer,
            )
        )
    )
    along = [(r, (r - 2 + 4 * (r % 2)) % 8) for r in range(8)]
    against = [(r, (r + 2 - 4 * (r % 2)) % 8) for r in range(8)]
    partner = [(r, r ^ 1) for r in range(8)]
    eastward = [(c, (c + 1) % 32) for c in range(32)]
    westward = [(c, (c - 1) % 32) for c in range(32)]
    across = [(7 * 32 + c, 7 * 32 + 31 - c) for c in range(32)]
    across += [(c, c ^ 1) for c in range(32)]
    for c in range(32):
        for r in (1, 3, 5):
            across += [(32 * r + c, 32 * r + 32 + c), (32 * r + 32 + c, 32 * r + c)]

    near = lax.ppermute(snap, "row", along)
    from_west = lax.ppermute(to_east, "col", eastward)
    from_east = lax.ppermute(to_west, "col", westward)
    near_back = lax.ppermute(snap, "row", against)

    outer, inner = pl.pallas_call(
        rows_kernel,
        out_shape=(shape(MESSAGE, LANES),) * 2,
        in_specs=[vmem()] * 3,
        out_specs=(vmem(),) * 2,
        compiler_params=grant(8),
        cost_estimate=pl.CostEstimate(flops=1000000, bytes_accessed=1000000, transcendentals=0),
        name="rows",
    )(fields, from_west, from_east)
    from_outer = lax.ppermute(outer, ("row", "col"), across)
    from_inner = lax.ppermute(inner, "row", partner)
    far = lax.ppermute(near, "row", along)

    hbm = lambda: pl.BlockSpec(memory_space=pl.ANY)
    state = pl.pallas_call(
        own_kernel,
        out_shape=shape(HELD, 2, TALL, LANES),
        in_specs=[vmem()] * 3,
        out_specs=vmem(),
        compiler_params=grant(8),
        cost_estimate=pl.CostEstimate(flops=1000000, bytes_accessed=1000000, transcendentals=0),
        name="own",
    )(fields, from_west, from_east)
    state, restart = pl.pallas_call(
        first_half_kernel,
        out_shape=(shape(HELD, 2, TALL, LANES), shape(1, 10, 8 * ROWS, LANES)),
        in_specs=[vmem()] * 3 + [hbm(), vmem(), hbm()],
        out_specs=(vmem(), hbm()),
        input_output_aliases={0: 0},
        scratch_shapes=[pltpu.SemaphoreType.DMA((8,))],
        compiler_params=grant(16),
        cost_estimate=pl.CostEstimate(flops=20000000, bytes_accessed=2000000, transcendentals=0),
        name="first_half",
    )(state, from_outer, from_inner, snap, flag, blank)

    joined = pl.pallas_call(
        join_kernel,
        out_shape=shape(3, 10, ROWS, LANES),
        in_specs=[vmem()] * 3,
        out_specs=vmem(),
        compiler_params=grant(8),
        name="join",
    )(snap, near, near_back)
    partner_blocks = lax.ppermute(joined, "row", partner)

    velocity, stress, _, restart = pl.pallas_call(
        second_half_kernel,
        out_shape=(
            shape(2, ROWS, LANES),
            shape(3, ROWS, LANES),
            shape(HELD, 2, TALL, LANES),
            shape(1, 10, 8 * ROWS, LANES),
        ),
        in_specs=[vmem(), hbm(), vmem(), hbm(), hbm()],
        out_specs=(vmem(), vmem(), vmem(), hbm()),
        input_output_aliases={0: 2, 1: 3},
        scratch_shapes=[pltpu.SemaphoreType.DMA((2,))],
        compiler_params=grant(8),
        cost_estimate=pl.CostEstimate(flops=20000000, bytes_accessed=2000000, transcendentals=0),
        name="second_half",
    )(state, restart, flag, near, near_back)
    partner_far = lax.ppermute(far, "row", partner)

    restart, velocity, stress = pl.pallas_call(
        late_kernel,
        out_shape=(
            shape(1, 10, 8 * ROWS, LANES),
            shape(2, ROWS, LANES),
            shape(3, ROWS, LANES),
        ),
        in_specs=[hbm(), vmem()] + [hbm()] * 4,
        out_specs=(hbm(), hbm(), hbm()),
        input_output_aliases={0: 0},
        scratch_shapes=[pltpu.SemaphoreType.DMA((6,))],
        compiler_params=grant(4),
        cost_estimate=pl.CostEstimate(flops=1000000, bytes_accessed=1000000, transcendentals=0),
        name="late",
    )(restart, flag, velocity, stress, far, partner_blocks)
    restart = pl.pallas_call(
        last_kernel,
        out_shape=shape(1, 10, 8 * ROWS, LANES),
        in_specs=[hbm(), vmem(), hbm()],
        out_specs=hbm(),
        input_output_aliases={0: 0},
        scratch_shapes=[pltpu.SemaphoreType.DMA],
        compiler_params=grant(4),
        name="last",
    )(restart, flag, partner_far)
    return (velocity, stress, restart)


def solution(mesh):
    return jax.shard_map(
        step,
        mesh=mesh,
        in_specs=(
            P(None, "row", "col"),
            P(None, "row", "col"),
            P(None, "row", "col"),
            P(None, "row", "col"),
            P(None, "row", "col"),
            P(None, "row", "col"),
            P("row", "col"),
            P("row", "col"),
            P("row", "col"),
            P("row", "col"),
            P(),
        ),
        out_specs=(P(None, "row", "col"), P(None, "row", "col"), P("row", None, None, "col")),
        check_vma=False,
    )
```

```python
import jax
import jax.numpy as jnp
from jax import lax
from jax.experimental import pallas as pl
from jax.experimental.pallas import tpu as pltpu
from jax.sharding import PartitionSpec as P


SUB = 12
SPLIT = 5
ROWS = 64
LANES = 128
HALO = 16
PAD = 8
TALL = PAD + HALO + ROWS + HALO + PAD
TOP = PAD + HALO + ROWS

U, V, S1, S2, S12, STR, HW, HH, INE, AA, KU, KV = range(12)
SENT = 12
BB, HWV, HHV, DU, SU, DV, SV, DP, DS, AS, AM = range(12, 23)
HELD = 23
MOVING = (U, V, INE, AA, KU, KV)
NEGATED = (U, V, KU, KV)
MESSAGE = SENT * HALO + SENT // 2 * 8


def lane_index():
    return lax.broadcasted_iota(jnp.int32, (8, LANES), 1)


def row_index():
    return lax.broadcasted_iota(jnp.int32, (8, LANES), 0)


def turned(value, steps):
    steps = steps % LANES
    return value if steps == 0 else pltpu.roll(value, steps, 1)


def west(main, side, first):
    a, b = turned(main, 1), turned(side, 1)
    return jnp.where(first, b, a), jnp.where(first, a, b)


def east(main, side, last):
    a, b = turned(main, -1), turned(side, -1)
    return jnp.where(last, b, a), jnp.where(last, a, b)


def expanded(blocks_t):
    rows = lax.broadcasted_iota(jnp.int32, (ROWS, 16), 0) // 4
    pick_rows = (rows == lax.broadcasted_iota(jnp.int32, (ROWS, 16), 1)).astype(jnp.float32)
    lanes = lax.broadcasted_iota(jnp.int32, (4, LANES), 1) // 32
    pick_lanes = (lanes == lax.broadcasted_iota(jnp.int32, (4, LANES), 0)).astype(jnp.float32)
    half = lax.dot_general(
        pick_rows, blocks_t, (((1,), (1,)), ((), ())), preferred_element_type=jnp.float32
    )
    return lax.dot_general(
        half, pick_lanes, (((1,), (0,)), ((), ())), preferred_element_type=jnp.float32
    )


def prepare_kernel(
    vel_hbm,
    stress_hbm,
    wind_hbm,
    ocean_hbm,
    area_hbm,
    volume_hbm,
    wide_hbm,
    high_hbm,
    land_hbm,
    ice_hbm,
    writer_hbm,
    fields,
    to_west,
    to_east,
    snap,
    flag,
    blank,
    vel,
    stress,
    wind,
    ocean,
    wide,
    high,
    land_t,
    ice_t,
    writer,
    sems,
):
    area, volume = snap.at[0:5], snap.at[5:10]
    moves = (
        (area_hbm, area),
        (volume_hbm, volume),
        (land_hbm, land_t),
        (ice_hbm, ice_t),
        (ocean_hbm, ocean),
        (wind_hbm, wind),
        (stress_hbm, stress),
        (vel_hbm, vel),
        (wide_hbm, wide),
        (high_hbm, high),
        (writer_hbm, writer),
    )
    copies = [pltpu.make_async_copy(a, b, sems.at[n]) for n, (a, b) in enumerate(moves)]
    for copy in copies:
        copy.start()
    blank[...] = jnp.zeros_like(blank)
    for copy in copies:
        copy.wait()
    mine = writer[lax.axis_index("col")] == lax.axis_index("row")
    flag[...] = jnp.where(mine, 1, 0) + jnp.zeros((8, LANES), jnp.int32)
    land = expanded(land_t[...].astype(jnp.float32))
    ice = expanded(ice_t[...].astype(jnp.float32))
    area_total = area[0] + area[1] + area[2] + area[3] + area[4]
    volume_total = volume[0] + volume[1] + volume[2] + volume[3] + volume[4]
    fields[U] = vel[0]
    fields[V] = vel[1]
    fields[S1] = 0.5 * stress[0]
    fields[S2] = 0.5 * stress[1]
    fields[S12] = stress[2]
    fields[STR] = (4.0 / 6.0) * volume_total * jnp.exp(-20.0 * (1.0 - area_total)) * land
    fields[HW] = 0.5 * wide[...]
    fields[HH] = 0.5 * high[...]
    inertia = 16.0 * (1.0 + volume_total)
    turning = 0.5 * (1.0 + volume_total)
    damped = inertia + 1.0
    scale = land * ice / (damped * damped + turning * turning)
    still = land * (1.0 - ice)
    fx = wind[0] + ocean[0]
    fy = wind[1] + ocean[1]
    fields[INE] = inertia
    fields[AA] = scale
    fields[KU] = scale * (damped * fx + turning * fy) + still * ocean[0]
    fields[KV] = scale * (damped * fy - turning * fx) + still * ocean[1]
    lane = lane_index()
    for f in range(SENT):
        left = right = None
        for g in range(8):
            part = fields[f, 8 * g : 8 * g + 8]
            inside = (lane >= 16 * g) & (lane < 16 * g + 16)
            a = turned(part, 16 * g)
            b = turned(part, 16 * g - 112)
            left = a if g == 0 else jnp.where(inside, a, left)
            right = b if g == 0 else jnp.where(inside, b, right)
        to_west[8 * f : 8 * f + 8] = left
        to_east[8 * f : 8 * f + 8] = right


def rows_kernel(fields, from_west, from_east, outer, inner):
    lane = lane_index()
    odd = lax.axis_index("row") % 2 == 1

    def fill(to_north, to_south):
        for f in range(SENT):
            to_north[HALO * f : HALO * f + HALO] = fields[f, ROWS - HALO : ROWS]
            to_south[HALO * f : HALO * f + HALO] = fields[f, 0:HALO]
        for pair in range(SENT // 2):
            north = south = None
            for member in range(2):
                f = 2 * pair + member
                base = 64 * member
                a = from_west[8 * f : 8 * f + 8]
                b = from_east[8 * f : 8 * f + 8]
                here = lane >= base
                there = lane >= base + 32
                n = jnp.where(there, turned(b, base + 32 - 96), turned(a, base - 96))
                s = jnp.where(there, turned(b, base + 32), turned(a, base))
                north = n if member == 0 else jnp.where(here, n, north)
                south = s if member == 0 else jnp.where(here, s, south)
            at = SENT * HALO + 8 * pair
            to_north[at : at + 8] = north
            to_south[at : at + 8] = south

    @pl.when(odd)
    def _():
        fill(outer, inner)

    @pl.when(jnp.logical_not(odd))
    def _():
        fill(inner, outer)


def stencil_masks():
    lane, row = lane_index(), row_index()
    is_top = lax.axis_index("row") == 7
    top_rows = (jnp.where(is_top, 1, 0) + jnp.zeros((8, LANES), jnp.int32)) == 1
    return lane == 0, lane == LANES - 1, row, top_rows


def own_kernel(fields, from_west, from_east, held):
    lane = lane_index()
    for f in range(SENT):
        a, b = from_west[8 * f : 8 * f + 8], from_east[8 * f : 8 * f + 8]
        for g in range(8):
            at = PAD + HALO + 8 * g
            held[f, 0, at : at + 8] = fields[f, 8 * g : 8 * g + 8]
            held[f, 1, at : at + 8] = jnp.where(lane < 64, turned(b, -16 * g), turned(a, 112 - 16 * g))
    for g in range(2, 10):
        derive(held, g, lane == 0)
        same_sizes(held, g)


def same_sizes(held, g):
    rows = slice(PAD + 8 * g, PAD + 8 * g + 8)
    for t in range(2):
        held[HWV, t, rows] = held[HW, t, rows]
        held[HHV, t, rows] = held[HH, t, rows]


def derive(held, g, first):
    at = PAD + 8 * g
    rows = slice(at, at + 8)
    for t in range(2):
        scale = held[AA, t, rows]
        inertia = held[INE, t, rows]
        held[AA, t, rows] = (inertia + 1.0) * scale
        held[BB, t, rows] = (inertia * (1.0 / 32.0)) * scale
    velocity_sums(
        held, at, held[U, 0, rows], held[U, 1, rows], held[V, 0, rows], held[V, 1, rows], first
    )


def assemble(from_outer, from_inner, held):
    is_top = lax.axis_index("row") == 7
    odd = lax.axis_index("row") % 2 + jnp.zeros((8, LANES), jnp.int32) == 1
    lane = lane_index()
    row = row_index()
    first, last, low = lane == 0, lane == LANES - 1, lane < 64

    bottom = lax.axis_index("row") + jnp.zeros((8, LANES), jnp.int32) == 0

    def south(at):
        value = jnp.where(odd, from_inner[at : at + 8], from_outer[at : at + 8])
        return jnp.where(bottom, 0.0, value)

    def north(at):
        return jnp.where(odd, from_outer[at : at + 8], from_inner[at : at + 8])

    def side_rows(message, f, a):
        base = 64 * (f % 2)
        corner = message(SENT * HALO + 8 * (f // 2))
        return jnp.where(low, turned(corner, -(base + 32 + 16 * a)), turned(corner, 112 - base - 16 * a))

    for f in range(SENT):
        for g in range(2):
            at = PAD + 8 * g
            held[f, 0, at : at + 8] = south(HALO * f + 8 * g)
            held[f, 1, at : at + 8] = side_rows(south, f, g)

    @pl.when(jnp.logical_not(is_top))
    def _():
        for f in range(SENT):
            for g in range(2):
                at = TOP + 8 * g
                held[f, 0, at : at + 8] = north(HALO * f + 8 * g)
                held[f, 1, at : at + 8] = side_rows(north, f, g)

    @pl.when(is_top)
    def _():
        def rotated(value):
            value = jnp.take_along_axis(value, LANES - 1 - lane, axis=1)
            return jnp.take_along_axis(value, 7 - row, axis=0)

        for f in range(SENT):
            for g in range(2):
                source = 1 - g
                main = rotated(north(HALO * f + 8 * source))
                side = rotated(side_rows(north, f, source))
                if f in MOVING:
                    main, side = east(main, side, last)
                    if f in NEGATED:
                        main, side = -main, -side
                    at = TOP + 8 * g
                else:
                    at = TOP + 1 + 8 * g
                held[f, 0, at : at + 8] = main
                held[f, 1, at : at + 8] = side
                if f in (HW, HH):
                    main, side = east(main, side, last)
                    own = HWV if f == HW else HHV
                    held[own, 0, TOP + 8 * g : TOP + 8 * g + 8] = main
                    held[own, 1, TOP + 8 * g : TOP + 8 * g + 8] = side

    for g in (0, 1):
        derive(held, g, first)
        same_sizes(held, g)
    for g in (10, 11):
        derive(held, g, first)

    @pl.when(jnp.logical_not(is_top))
    def _():
        for g in (10, 11):
            same_sizes(held, g)


def velocity_sums(held, at, um, us, vm, vs, first):
    wum, wus = west(um, us, first)
    wvm, wvs = west(vm, vs, first)
    for t, (x, wx, y, wy) in enumerate(((um, wum, vm, wvm), (us, wus, vs, wvs))):
        held[DU, t, at : at + 8] = x - wx
        held[SU, t, at : at + 8] = x + wx
        held[DV, t, at : at + 8] = y - wy
        held[SV, t, at : at + 8] = y + wy


def stress_rows(held, at, last):
    fresh = []
    for t in range(2):
        here = lambda f: held[f, t, at : at + 8]
        below = lambda f: held[f, t, at - 1 : at + 7]
        hw, hh = here(HW), here(HH)
        gux = hw * (here(DU) + below(DU))
        guy = hh * (here(SU) - below(SU))
        gvx = hw * (here(DV) + below(DV))
        gvy = hh * (here(SV) - below(SV))
        divergence = gux + gvy
        tension = gux - gvy
        shearing = guy + gvx
        deform = jnp.sqrt(
            divergence * divergence + 0.25 * (tension * tension + shearing * shearing)
        )
        viscous = here(STR) / (deform + 0.5)
        quarter = 0.25 * viscous
        s1 = here(S1) * (2.0 / 3.0) + viscous * (divergence - deform)
        s2 = here(S2) * (2.0 / 3.0) + quarter * tension
        s12 = here(S12) * (2.0 / 3.0) + quarter * shearing
        held[S1, t, at : at + 8] = s1
        held[S2, t, at : at + 8] = s2
        held[S12, t, at : at + 8] = s12
        fresh.append((s1 + s2, s1 - s2, s12))
    (pm, mm, qm), (ps, ms, qs) = fresh
    epm, eps = east(pm, ps, last)
    emm, ems = east(mm, ms, last)
    eqm, eqs = east(qm, qs, last)
    for t, (p, ep, m, em, q, eq) in enumerate(
        ((pm, epm, mm, emm, qm, eqm), (ps, eps, ms, ems, qs, eqs))
    ):
        held[DP, t, at : at + 8] = ep - p
        held[AM, t, at : at + 8] = em + m
        held[DS, t, at : at + 8] = eq - q
        held[AS, t, at : at + 8] = eq + q


def velocity_rows(held, at, first, row, top_rows):
    fresh = []
    for t in range(2):
        here = lambda f: held[f, t, at : at + 8]

        def pair(f):
            own, above = here(f), held[f, t, at + 1 : at + 9]
            if at == TOP - 8:
                above = jnp.where((row == 7) & top_rows, held[f, t, at + 2 : at + 10], above)
            if at == TOP:
                own = jnp.where((row == 0) & top_rows, held[f, t, at - 1 : at + 7], own)
            return own, above

        hw, hh = here(HWV), here(HHV)
        dp, ndp = pair(DP)
        ds, nds = pair(DS)
        as_, nas = pair(AS)
        am, nam = pair(AM)
        inertia, a, b = here(INE), here(AA), here(BB)
        x = inertia * here(U) + (hw * (dp + ndp) + hh * (nas - as_))
        y = inertia * here(V) + (hw * (ds + nds) + hh * (nam - am))
        u = a * x + b * y + here(KU)
        v = a * y - b * x + here(KV)
        held[U, t, at : at + 8] = u
        held[V, t, at : at + 8] = v
        fresh.append((u, v))
    (um, vm), (us, vs) = fresh
    velocity_sums(held, at, um, us, vm, vs, first)


def subcycles(held, start, stop, lo, hi):
    first, last, row, top_rows = stencil_masks()

    def body(_, carry):
        for g in range(lo, hi):
            stress_rows(held, PAD + 8 * g, last)
        for g in range(lo, hi):
            velocity_rows(held, PAD + 8 * g, first, row, top_rows)
        return carry

    lax.fori_loop(start, stop, body, 0)


def place_of(me, which):
    chip, core = me // 2, me % 2
    step = 2 * core - 1
    if which >= 4:
        core = 1 - core
        which -= 4
        step = -step
    chips = (chip, lax.rem(chip - step + 4, 4), lax.rem(chip + step + 4, 4), lax.rem(chip + 2, 4))
    return (2 * chips[which] + core) * ROWS


def into(out, ref, place, sem):
    return pltpu.make_async_copy(ref, out.at[0, :, pl.ds(place, ROWS), :], sem)


def first_half_kernel(
    state, from_outer, from_inner, snap, flag, zero, held, out, sems
):
    me = lax.axis_index("row")
    mine = jnp.max(flag[...]) == 1
    zeros = [into(out, zero, n * ROWS, sems.at[n]) for n in range(8)]
    own = into(out, snap, place_of(me, 0), sems.at[0])

    @pl.when(mine)
    def _():
        own.start()

    @pl.when(jnp.logical_not(mine))
    def _():
        for copy in zeros:
            copy.start()

    assemble(from_outer, from_inner, held)
    subcycles(held, 0, 5, 0, 12)

    @pl.when(mine)
    def _():
        own.wait()

    @pl.when(jnp.logical_not(mine))
    def _():
        for copy in zeros:
            copy.wait()


def second_half_kernel(state, out_in, flag, near, near_back, far, vel, stress, held, out, sems):
    me = lax.axis_index("row")
    mine = jnp.max(flag[...]) == 1
    copies = [
        into(out, near, place_of(me, 1), sems.at[0]),
        into(out, near_back, place_of(me, 2), sems.at[1]),
        into(out, far, place_of(me, 3), sems.at[2]),
    ]

    @pl.when(mine)
    def _():
        for copy in copies:
            copy.start()

    subcycles(held, SPLIT, SUB, 1, 11)
    at = PAD + HALO
    vel[0] = held[U, 0, at : at + ROWS]
    vel[1] = held[V, 0, at : at + ROWS]
    stress[0] = 2.0 * held[S1, 0, at : at + ROWS]
    stress[1] = 2.0 * held[S2, 0, at : at + ROWS]
    stress[2] = held[S12, 0, at : at + ROWS]

    @pl.when(mine)
    def _():
        for copy in copies:
            copy.wait()


def late_kernel(vel, stress, vel_out, stress_out, sems):
    copies = [
        pltpu.make_async_copy(vel, vel_out, sems.at[0]),
        pltpu.make_async_copy(stress, stress_out, sems.at[1]),
    ]
    for copy in copies:
        copy.start()
    for copy in copies:
        copy.wait()


def last_kernel(out_in, flag, partner, out, sems):
    me = lax.axis_index("row")
    mine = jnp.max(flag[...]) == 1

    @pl.when(mine)
    def _():
        copies = [into(out, partner.at[n], place_of(me, 4 + n), sems.at[n]) for n in range(4)]
        for copy in copies:
            copy.start()
        for copy in copies:
            copy.wait()


def join_kernel(own, near, near_back, far, joined):
    for n, block in enumerate((own, near, near_back, far)):
        joined[n] = block[...]


def vmem():
    return pl.BlockSpec(memory_space=pltpu.VMEM)


def shape(*dims):
    return jax.ShapeDtypeStruct(dims, jnp.float32)


def grant(mebibytes):
    return pltpu.CompilerParams(vmem_limit_bytes=mebibytes << 20)


def step(
    velocity_start,
    stress_start,
    wind_stress,
    ocean_current,
    ice_area,
    ice_volume,
    inverse_width,
    inverse_height,
    land_block,
    ice_block,
    writer,
):
    fields, to_west, to_east, snap, flag, blank = pl.pallas_call(
        prepare_kernel,
        out_shape=(
            shape(SENT, ROWS, LANES),
            shape(SENT * 8, LANES),
            shape(SENT * 8, LANES),
            shape(10, ROWS, LANES),
            jax.ShapeDtypeStruct((8, LANES), jnp.int32),
            shape(10, ROWS, LANES),
        ),
        in_specs=[pl.BlockSpec(memory_space=pltpu.HBM)] * 11,
        out_specs=(vmem(),) * 6,
        scratch_shapes=[
            pltpu.VMEM((2, ROWS, LANES), jnp.float32),
            pltpu.VMEM((3, ROWS, LANES), jnp.float32),
            pltpu.VMEM((2, ROWS, LANES), jnp.float32),
            pltpu.VMEM((2, ROWS, LANES), jnp.float32),
            pltpu.VMEM((ROWS, LANES), jnp.float32),
            pltpu.VMEM((ROWS, LANES), jnp.float32),
            pltpu.VMEM((4, 16), jnp.int32),
            pltpu.VMEM((4, 16), jnp.int32),
            pltpu.SMEM((32,), jnp.int32),
            pltpu.SemaphoreType.DMA((11,)),
        ],
        compiler_params=grant(8),
        name="prepare",
    )(
        *(
            pltpu.with_memory_space_constraint(value, pltpu.HBM)
            for value in (
                velocity_start,
                stress_start,
                wind_stress,
                ocean_current,
                ice_area,
                ice_volume,
                inverse_width,
                inverse_height,
                land_block.T,
                ice_block.T,
                writer,
            )
        )
    )
    along = [(r, (r - 2 + 4 * (r % 2)) % 8) for r in range(8)]
    against = [(r, (r + 2 - 4 * (r % 2)) % 8) for r in range(8)]
    partner = [(r, r ^ 1) for r in range(8)]
    eastward = [(c, (c + 1) % 32) for c in range(32)]
    westward = [(c, (c - 1) % 32) for c in range(32)]
    across = [(7 * 32 + c, 7 * 32 + 31 - c) for c in range(32)]
    across += [(c, c ^ 1) for c in range(32)]
    for c in range(32):
        for r in (1, 3, 5):
            across += [(32 * r + c, 32 * r + 32 + c), (32 * r + 32 + c, 32 * r + c)]

    near = lax.ppermute(snap, "row", along)
    from_west = lax.ppermute(to_east, "col", eastward)
    from_east = lax.ppermute(to_west, "col", westward)
    near_back = lax.ppermute(snap, "row", against)

    outer, inner = pl.pallas_call(
        rows_kernel,
        out_shape=(shape(MESSAGE, LANES),) * 2,
        in_specs=[vmem()] * 3,
        out_specs=(vmem(),) * 2,
        compiler_params=grant(8),
        cost_estimate=pl.CostEstimate(flops=1000000, bytes_accessed=1000000, transcendentals=0),
        name="rows",
    )(fields, from_west, from_east)
    from_outer = lax.ppermute(outer, ("row", "col"), across)
    from_inner = lax.ppermute(inner, "row", partner)
    far = lax.ppermute(near, "row", along)

    hbm = lambda: pl.BlockSpec(memory_space=pl.ANY)
    state = pl.pallas_call(
        own_kernel,
        out_shape=shape(HELD, 2, TALL, LANES),
        in_specs=[vmem()] * 3,
        out_specs=vmem(),
        compiler_params=grant(8),
        cost_estimate=pl.CostEstimate(flops=1000000, bytes_accessed=1000000, transcendentals=0),
        name="own",
    )(fields, from_west, from_east)
    state, restart = pl.pallas_call(
        first_half_kernel,
        out_shape=(shape(HELD, 2, TALL, LANES), shape(1, 10, 8 * ROWS, LANES)),
        in_specs=[vmem()] * 3 + [hbm(), vmem(), hbm()],
        out_specs=(vmem(), hbm()),
        input_output_aliases={0: 0},
        scratch_shapes=[pltpu.SemaphoreType.DMA((8,))],
        compiler_params=grant(16),
        cost_estimate=pl.CostEstimate(flops=20000000, bytes_accessed=2000000, transcendentals=0),
        name="first_half",
    )(state, from_outer, from_inner, snap, flag, blank)

    joined = pl.pallas_call(
        join_kernel,
        out_shape=shape(4, 10, ROWS, LANES),
        in_specs=[vmem()] * 4,
        out_specs=vmem(),
        compiler_params=grant(8),
        name="join",
    )(snap, near, near_back, far)
    partner_blocks = lax.ppermute(joined, "row", partner)

    velocity, stress, _, restart = pl.pallas_call(
        second_half_kernel,
        out_shape=(
            shape(2, ROWS, LANES),
            shape(3, ROWS, LANES),
            shape(HELD, 2, TALL, LANES),
            shape(1, 10, 8 * ROWS, LANES),
        ),
        in_specs=[vmem(), hbm(), vmem(), hbm(), hbm(), hbm()],
        out_specs=(vmem(), vmem(), vmem(), hbm()),
        input_output_aliases={0: 2, 1: 3},
        scratch_shapes=[pltpu.SemaphoreType.DMA((3,))],
        compiler_params=grant(8),
        cost_estimate=pl.CostEstimate(flops=20000000, bytes_accessed=2000000, transcendentals=0),
        name="second_half",
    )(state, restart, flag, near, near_back, far)

    velocity, stress = pl.pallas_call(
        late_kernel,
        out_shape=(shape(2, ROWS, LANES), shape(3, ROWS, LANES)),
        in_specs=[hbm(), hbm()],
        out_specs=(hbm(), hbm()),
        scratch_shapes=[pltpu.SemaphoreType.DMA((2,))],
        compiler_params=grant(4),
        cost_estimate=pl.CostEstimate(flops=1000000, bytes_accessed=1000000, transcendentals=0),
        name="late",
    )(velocity, stress)
    restart = pl.pallas_call(
        last_kernel,
        out_shape=shape(1, 10, 8 * ROWS, LANES),
        in_specs=[hbm(), vmem(), hbm()],
        out_specs=hbm(),
        input_output_aliases={0: 0},
        scratch_shapes=[pltpu.SemaphoreType.DMA((4,))],
        compiler_params=grant(4),
        name="last",
    )(restart, flag, partner_blocks)
    return (velocity, stress, restart)


def solution(mesh):
    return jax.shard_map(
        step,
        mesh=mesh,
        in_specs=(
            P(None, "row", "col"),
            P(None, "row", "col"),
            P(None, "row", "col"),
            P(None, "row", "col"),
            P(None, "row", "col"),
            P(None, "row", "col"),
            P("row", "col"),
            P("row", "col"),
            P("row", "col"),
            P("row", "col"),
            P(),
        ),
        out_specs=(P(None, "row", "col"), P(None, "row", "col"), P("row", None, None, "col")),
        check_vma=False,
    )
```

```python
import jax
import jax.numpy as jnp
from jax import lax
from jax.experimental import pallas as pl
from jax.experimental.pallas import tpu as pltpu
from jax.sharding import PartitionSpec as P


SUB = 12
ROWS = 64
LANES = 128
HALO = 16
PAD = 8
TALL = PAD + HALO + ROWS + HALO + PAD
TOP = PAD + HALO + ROWS

U, V, S1, S2, S12, STR, HW, HH, INE, AA, KU, KV = range(12)
SENT = 12
BB, HWV, HHV, DU, SU, DV, SV, DP, DS, AS, AM = range(12, 23)
HELD = 23
MOVING = (U, V, INE, AA, KU, KV)
NEGATED = (U, V, KU, KV)
MESSAGE = SENT * HALO + SENT // 2 * 8


def lane_index():
    return lax.broadcasted_iota(jnp.int32, (8, LANES), 1)


def row_index():
    return lax.broadcasted_iota(jnp.int32, (8, LANES), 0)


def turned(value, steps):
    steps = steps % LANES
    return value if steps == 0 else pltpu.roll(value, steps, 1)


def west(main, side, first):
    a, b = turned(main, 1), turned(side, 1)
    return jnp.where(first, b, a), jnp.where(first, a, b)


def east(main, side, last):
    a, b = turned(main, -1), turned(side, -1)
    return jnp.where(last, b, a), jnp.where(last, a, b)


def expanded(blocks_t):
    rows = lax.broadcasted_iota(jnp.int32, (ROWS, 16), 0) // 4
    pick_rows = (rows == lax.broadcasted_iota(jnp.int32, (ROWS, 16), 1)).astype(jnp.float32)
    lanes = lax.broadcasted_iota(jnp.int32, (4, LANES), 1) // 32
    pick_lanes = (lanes == lax.broadcasted_iota(jnp.int32, (4, LANES), 0)).astype(jnp.float32)
    half = lax.dot_general(
        pick_rows, blocks_t, (((1,), (1,)), ((), ())), preferred_element_type=jnp.float32
    )
    return lax.dot_general(
        half, pick_lanes, (((1,), (0,)), ((), ())), preferred_element_type=jnp.float32
    )


def prepare_kernel(
    vel_hbm,
    stress_hbm,
    wind_hbm,
    ocean_hbm,
    area_hbm,
    volume_hbm,
    wide_hbm,
    high_hbm,
    land_hbm,
    ice_hbm,
    writer_hbm,
    fields,
    to_west,
    to_east,
    snap,
    flag,
    blank,
    vel,
    stress,
    wind,
    ocean,
    wide,
    high,
    land_t,
    ice_t,
    writer,
    sems,
):
    area, volume = snap.at[0:5], snap.at[5:10]
    moves = (
        (area_hbm, area),
        (volume_hbm, volume),
        (land_hbm, land_t),
        (ice_hbm, ice_t),
        (ocean_hbm, ocean),
        (wind_hbm, wind),
        (stress_hbm, stress),
        (vel_hbm, vel),
        (wide_hbm, wide),
        (high_hbm, high),
        (writer_hbm, writer),
    )
    copies = [pltpu.make_async_copy(a, b, sems.at[n]) for n, (a, b) in enumerate(moves)]
    for copy in copies:
        copy.start()
    blank[...] = jnp.zeros_like(blank)
    for copy in copies:
        copy.wait()
    mine = writer[lax.axis_index("col")] == lax.axis_index("row")
    flag[...] = jnp.where(mine, 1, 0) + jnp.zeros((8, LANES), jnp.int32)
    land = expanded(land_t[...].astype(jnp.float32))
    ice = expanded(ice_t[...].astype(jnp.float32))
    area_total = area[0] + area[1] + area[2] + area[3] + area[4]
    volume_total = volume[0] + volume[1] + volume[2] + volume[3] + volume[4]
    fields[U] = vel[0]
    fields[V] = vel[1]
    fields[S1] = 0.5 * stress[0]
    fields[S2] = 0.5 * stress[1]
    fields[S12] = stress[2]
    fields[STR] = (4.0 / 6.0) * volume_total * jnp.exp(-20.0 * (1.0 - area_total)) * land
    fields[HW] = 0.5 * wide[...]
    fields[HH] = 0.5 * high[...]
    inertia = 16.0 * (1.0 + volume_total)
    turning = 0.5 * (1.0 + volume_total)
    damped = inertia + 1.0
    scale = land * ice / (damped * damped + turning * turning)
    still = land * (1.0 - ice)
    fx = wind[0] + ocean[0]
    fy = wind[1] + ocean[1]
    fields[INE] = inertia
    fields[AA] = scale
    fields[KU] = scale * (damped * fx + turning * fy) + still * ocean[0]
    fields[KV] = scale * (damped * fy - turning * fx) + still * ocean[1]
    lane = lane_index()
    for f in range(SENT):
        left = right = None
        for g in range(8):
            part = fields[f, 8 * g : 8 * g + 8]
            inside = (lane >= 16 * g) & (lane < 16 * g + 16)
            a = turned(part, 16 * g)
            b = turned(part, 16 * g - 112)
            left = a if g == 0 else jnp.where(inside, a, left)
            right = b if g == 0 else jnp.where(inside, b, right)
        to_west[8 * f : 8 * f + 8] = left
        to_east[8 * f : 8 * f + 8] = right


def rows_kernel(fields, from_west, from_east, outer, inner):
    lane = lane_index()
    odd = lax.axis_index("row") % 2 == 1

    def fill(to_north, to_south):
        for f in range(SENT):
            to_north[HALO * f : HALO * f + HALO] = fields[f, ROWS - HALO : ROWS]
            to_south[HALO * f : HALO * f + HALO] = fields[f, 0:HALO]
        for pair in range(SENT // 2):
            north = south = None
            for member in range(2):
                f = 2 * pair + member
                base = 64 * member
                a = from_west[8 * f : 8 * f + 8]
                b = from_east[8 * f : 8 * f + 8]
                here = lane >= base
                there = lane >= base + 32
                n = jnp.where(there, turned(b, base + 32 - 96), turned(a, base - 96))
                s = jnp.where(there, turned(b, base + 32), turned(a, base))
                north = n if member == 0 else jnp.where(here, n, north)
                south = s if member == 0 else jnp.where(here, s, south)
            at = SENT * HALO + 8 * pair
            to_north[at : at + 8] = north
            to_south[at : at + 8] = south

    @pl.when(odd)
    def _():
        fill(outer, inner)

    @pl.when(jnp.logical_not(odd))
    def _():
        fill(inner, outer)


def stencil_masks():
    lane, row = lane_index(), row_index()
    is_top = lax.axis_index("row") == 7
    top_rows = (jnp.where(is_top, 1, 0) + jnp.zeros((8, LANES), jnp.int32)) == 1
    return lane == 0, lane == LANES - 1, row, top_rows


def own_kernel(fields, from_west, from_east, held):
    lane = lane_index()
    for f in range(SENT):
        a, b = from_west[8 * f : 8 * f + 8], from_east[8 * f : 8 * f + 8]
        for g in range(8):
            at = PAD + HALO + 8 * g
            held[f, 0, at : at + 8] = fields[f, 8 * g : 8 * g + 8]
            held[f, 1, at : at + 8] = jnp.where(lane < 64, turned(b, -16 * g), turned(a, 112 - 16 * g))
    for g in range(2, 10):
        derive(held, g, lane == 0)
        same_sizes(held, g)


def same_sizes(held, g):
    rows = slice(PAD + 8 * g, PAD + 8 * g + 8)
    for t in range(2):
        held[HWV, t, rows] = held[HW, t, rows]
        held[HHV, t, rows] = held[HH, t, rows]


def derive(held, g, first):
    at = PAD + 8 * g
    rows = slice(at, at + 8)
    for t in range(2):
        scale = held[AA, t, rows]
        inertia = held[INE, t, rows]
        held[AA, t, rows] = (inertia + 1.0) * scale
        held[BB, t, rows] = (inertia * (1.0 / 32.0)) * scale
    velocity_sums(
        held, at, held[U, 0, rows], held[U, 1, rows], held[V, 0, rows], held[V, 1, rows], first
    )


def assemble(from_outer, from_inner, held):
    is_top = lax.axis_index("row") == 7
    odd = lax.axis_index("row") % 2 + jnp.zeros((8, LANES), jnp.int32) == 1
    lane = lane_index()
    row = row_index()
    first, last, low = lane == 0, lane == LANES - 1, lane < 64

    bottom = lax.axis_index("row") + jnp.zeros((8, LANES), jnp.int32) == 0

    def south(at):
        value = jnp.where(odd, from_inner[at : at + 8], from_outer[at : at + 8])
        return jnp.where(bottom, 0.0, value)

    def north(at):
        return jnp.where(odd, from_outer[at : at + 8], from_inner[at : at + 8])

    def side_rows(message, f, a):
        base = 64 * (f % 2)
        corner = message(SENT * HALO + 8 * (f // 2))
        return jnp.where(low, turned(corner, -(base + 32 + 16 * a)), turned(corner, 112 - base - 16 * a))

    for f in range(SENT):
        for g in range(2):
            at = PAD + 8 * g
            held[f, 0, at : at + 8] = south(HALO * f + 8 * g)
            held[f, 1, at : at + 8] = side_rows(south, f, g)

    @pl.when(jnp.logical_not(is_top))
    def _():
        for f in range(SENT):
            for g in range(2):
                at = TOP + 8 * g
                held[f, 0, at : at + 8] = north(HALO * f + 8 * g)
                held[f, 1, at : at + 8] = side_rows(north, f, g)

    @pl.when(is_top)
    def _():
        def rotated(value):
            value = jnp.take_along_axis(value, LANES - 1 - lane, axis=1)
            return jnp.take_along_axis(value, 7 - row, axis=0)

        for f in range(SENT):
            for g in range(2):
                source = 1 - g
                main = rotated(north(HALO * f + 8 * source))
                side = rotated(side_rows(north, f, source))
                if f in MOVING:
                    main, side = east(main, side, last)
                    if f in NEGATED:
                        main, side = -main, -side
                    at = TOP + 8 * g
                else:
                    at = TOP + 1 + 8 * g
                held[f, 0, at : at + 8] = main
                held[f, 1, at : at + 8] = side
                if f in (HW, HH):
                    main, side = east(main, side, last)
                    own = HWV if f == HW else HHV
                    held[own, 0, TOP + 8 * g : TOP + 8 * g + 8] = main
                    held[own, 1, TOP + 8 * g : TOP + 8 * g + 8] = side

    for g in (0, 1):
        derive(held, g, first)
        same_sizes(held, g)
    for g in (10, 11):
        derive(held, g, first)

    @pl.when(jnp.logical_not(is_top))
    def _():
        for g in (10, 11):
            same_sizes(held, g)


def velocity_sums(held, at, um, us, vm, vs, first):
    wum, wus = west(um, us, first)
    wvm, wvs = west(vm, vs, first)
    for t, (x, wx, y, wy) in enumerate(((um, wum, vm, wvm), (us, wus, vs, wvs))):
        held[DU, t, at : at + 8] = x - wx
        held[SU, t, at : at + 8] = x + wx
        held[DV, t, at : at + 8] = y - wy
        held[SV, t, at : at + 8] = y + wy


def stress_rows(held, at, last):
    fresh = []
    for t in range(2):
        here = lambda f: held[f, t, at : at + 8]
        below = lambda f: held[f, t, at - 1 : at + 7]
        hw, hh = here(HW), here(HH)
        gux = hw * (here(DU) + below(DU))
        guy = hh * (here(SU) - below(SU))
        gvx = hw * (here(DV) + below(DV))
        gvy = hh * (here(SV) - below(SV))
        divergence = gux + gvy
        tension = gux - gvy
        shearing = guy + gvx
        deform = jnp.sqrt(
            divergence * divergence + 0.25 * (tension * tension + shearing * shearing)
        )
        viscous = here(STR) / (deform + 0.5)
        quarter = 0.25 * viscous
        s1 = here(S1) * (2.0 / 3.0) + viscous * (divergence - deform)
        s2 = here(S2) * (2.0 / 3.0) + quarter * tension
        s12 = here(S12) * (2.0 / 3.0) + quarter * shearing
        held[S1, t, at : at + 8] = s1
        held[S2, t, at : at + 8] = s2
        held[S12, t, at : at + 8] = s12
        fresh.append((s1 + s2, s1 - s2, s12))
    (pm, mm, qm), (ps, ms, qs) = fresh
    epm, eps = east(pm, ps, last)
    emm, ems = east(mm, ms, last)
    eqm, eqs = east(qm, qs, last)
    for t, (p, ep, m, em, q, eq) in enumerate(
        ((pm, epm, mm, emm, qm, eqm), (ps, eps, ms, ems, qs, eqs))
    ):
        held[DP, t, at : at + 8] = ep - p
        held[AM, t, at : at + 8] = em + m
        held[DS, t, at : at + 8] = eq - q
        held[AS, t, at : at + 8] = eq + q


def velocity_rows(held, at, first, row, top_rows):
    fresh = []
    for t in range(2):
        here = lambda f: held[f, t, at : at + 8]

        def pair(f):
            own, above = here(f), held[f, t, at + 1 : at + 9]
            if at == TOP - 8:
                above = jnp.where((row == 7) & top_rows, held[f, t, at + 2 : at + 10], above)
            if at == TOP:
                own = jnp.where((row == 0) & top_rows, held[f, t, at - 1 : at + 7], own)
            return own, above

        hw, hh = here(HWV), here(HHV)
        dp, ndp = pair(DP)
        ds, nds = pair(DS)
        as_, nas = pair(AS)
        am, nam = pair(AM)
        inertia, a, b = here(INE), here(AA), here(BB)
        x = inertia * here(U) + (hw * (dp + ndp) + hh * (nas - as_))
        y = inertia * here(V) + (hw * (ds + nds) + hh * (nam - am))
        u = a * x + b * y + here(KU)
        v = a * y - b * x + here(KV)
        held[U, t, at : at + 8] = u
        held[V, t, at : at + 8] = v
        fresh.append((u, v))
    (um, vm), (us, vs) = fresh
    velocity_sums(held, at, um, us, vm, vs, first)


def subcycles(held, start, stop, lo, hi):
    first, last, row, top_rows = stencil_masks()

    def body(_, carry):
        for g in range(lo, hi):
            stress_rows(held, PAD + 8 * g, last)
        for g in range(lo, hi):
            velocity_rows(held, PAD + 8 * g, first, row, top_rows)
        return carry

    lax.fori_loop(start, stop, body, 0)


def place_of(me, which):
    chip, core = me // 2, me % 2
    step = 2 * core - 1
    if which >= 4:
        core = 1 - core
        which -= 4
        step = -step
    chips = (chip, lax.rem(chip - step + 4, 4), lax.rem(chip + step + 4, 4), lax.rem(chip + 2, 4))
    return (2 * chips[which] + core) * ROWS


def into(out, ref, place, sem):
    return pltpu.make_async_copy(ref, out.at[0, :, pl.ds(place, ROWS), :], sem)


def stencil_kernel(
    state, from_outer, from_inner, snap, near, near_back, flag, zero, vel, stress, held, out, sems
):
    me = lax.axis_index("row")
    mine = jnp.max(flag[...]) == 1
    zeros = [into(out, zero, n * ROWS, sems.at[n]) for n in range(8)]
    own = [into(out, ref, place_of(me, n), sems.at[n]) for n, ref in enumerate((snap, near, near_back))]

    @pl.when(mine)
    def _():
        for copy in own:
            copy.start()

    @pl.when(jnp.logical_not(mine))
    def _():
        for copy in zeros:
            copy.start()

    assemble(from_outer, from_inner, held)
    subcycles(held, 0, 5, 0, 12)
    subcycles(held, 5, SUB, 1, 11)
    at = PAD + HALO
    vel[0] = held[U, 0, at : at + ROWS]
    vel[1] = held[V, 0, at : at + ROWS]
    stress[0] = 2.0 * held[S1, 0, at : at + ROWS]
    stress[1] = 2.0 * held[S2, 0, at : at + ROWS]
    stress[2] = held[S12, 0, at : at + ROWS]

    @pl.when(mine)
    def _():
        for copy in own:
            copy.wait()

    @pl.when(jnp.logical_not(mine))
    def _():
        for copy in zeros:
            copy.wait()


def late_kernel(out_in, flag, vel, stress, far, partner, out, vel_out, stress_out, sems):
    me = lax.axis_index("row")
    fields_out = [
        pltpu.make_async_copy(vel, vel_out, sems.at[4]),
        pltpu.make_async_copy(stress, stress_out, sems.at[5]),
    ]
    for copy in fields_out:
        copy.start()
    mine = jnp.max(flag[...]) == 1

    @pl.when(mine)
    def _():
        copies = [into(out, partner.at[n], place_of(me, 4 + n), sems.at[n]) for n in range(3)]
        copies.append(into(out, far, place_of(me, 3), sems.at[3]))
        for copy in copies:
            copy.start()
        for copy in copies:
            copy.wait()

    for copy in fields_out:
        copy.wait()


def last_kernel(out_in, flag, partner_far, out, sem):
    mine = jnp.max(flag[...]) == 1

    @pl.when(mine)
    def _():
        copy = into(out, partner_far, place_of(lax.axis_index("row"), 7), sem)
        copy.start()
        copy.wait()


def join_kernel(own, near, near_back, joined):
    for n, block in enumerate((own, near, near_back)):
        joined[n] = block[...]


def vmem():
    return pl.BlockSpec(memory_space=pltpu.VMEM)


def shape(*dims):
    return jax.ShapeDtypeStruct(dims, jnp.float32)


def grant(mebibytes):
    return pltpu.CompilerParams(vmem_limit_bytes=mebibytes << 20)


def step(
    velocity_start,
    stress_start,
    wind_stress,
    ocean_current,
    ice_area,
    ice_volume,
    inverse_width,
    inverse_height,
    land_block,
    ice_block,
    writer,
):
    fields, to_west, to_east, snap, flag, blank = pl.pallas_call(
        prepare_kernel,
        out_shape=(
            shape(SENT, ROWS, LANES),
            shape(SENT * 8, LANES),
            shape(SENT * 8, LANES),
            shape(10, ROWS, LANES),
            jax.ShapeDtypeStruct((8, LANES), jnp.int32),
            shape(10, ROWS, LANES),
        ),
        in_specs=[pl.BlockSpec(memory_space=pltpu.HBM)] * 11,
        out_specs=(vmem(),) * 6,
        scratch_shapes=[
            pltpu.VMEM((2, ROWS, LANES), jnp.float32),
            pltpu.VMEM((3, ROWS, LANES), jnp.float32),
            pltpu.VMEM((2, ROWS, LANES), jnp.float32),
            pltpu.VMEM((2, ROWS, LANES), jnp.float32),
            pltpu.VMEM((ROWS, LANES), jnp.float32),
            pltpu.VMEM((ROWS, LANES), jnp.float32),
            pltpu.VMEM((4, 16), jnp.int32),
            pltpu.VMEM((4, 16), jnp.int32),
            pltpu.SMEM((32,), jnp.int32),
            pltpu.SemaphoreType.DMA((11,)),
        ],
        compiler_params=grant(8),
        name="prepare",
    )(
        *(
            pltpu.with_memory_space_constraint(value, pltpu.HBM)
            for value in (
                velocity_start,
                stress_start,
                wind_stress,
                ocean_current,
                ice_area,
                ice_volume,
                inverse_width,
                inverse_height,
                land_block.T,
                ice_block.T,
                writer,
            )
        )
    )
    along = [(r, (r - 2 + 4 * (r % 2)) % 8) for r in range(8)]
    against = [(r, (r + 2 - 4 * (r % 2)) % 8) for r in range(8)]
    partner = [(r, r ^ 1) for r in range(8)]
    eastward = [(c, (c + 1) % 32) for c in range(32)]
    westward = [(c, (c - 1) % 32) for c in range(32)]
    across = [(7 * 32 + c, 7 * 32 + 31 - c) for c in range(32)]
    across += [(c, c ^ 1) for c in range(32)]
    for c in range(32):
        for r in (1, 3, 5):
            across += [(32 * r + c, 32 * r + 32 + c), (32 * r + 32 + c, 32 * r + c)]

    near = lax.ppermute(snap, "row", along)
    from_west = lax.ppermute(to_east, "col", eastward)
    from_east = lax.ppermute(to_west, "col", westward)
    near_back = lax.ppermute(snap, "row", against)

    outer, inner = pl.pallas_call(
        rows_kernel,
        out_shape=(shape(MESSAGE, LANES),) * 2,
        in_specs=[vmem()] * 3,
        out_specs=(vmem(),) * 2,
        compiler_params=grant(8),
        cost_estimate=pl.CostEstimate(flops=1000000, bytes_accessed=1000000, transcendentals=0),
        name="rows",
    )(fields, from_west, from_east)
    from_outer = lax.ppermute(outer, ("row", "col"), across)
    from_inner = lax.ppermute(inner, "row", partner)
    far = lax.ppermute(near, "row", along)

    hbm = lambda: pl.BlockSpec(memory_space=pl.ANY)
    state = pl.pallas_call(
        own_kernel,
        out_shape=shape(HELD, 2, TALL, LANES),
        in_specs=[vmem()] * 3,
        out_specs=vmem(),
        compiler_params=grant(8),
        cost_estimate=pl.CostEstimate(flops=1000000, bytes_accessed=1000000, transcendentals=0),
        name="own",
    )(fields, from_west, from_east)
    joined = pl.pallas_call(
        join_kernel,
        out_shape=shape(3, 10, ROWS, LANES),
        in_specs=[vmem()] * 3,
        out_specs=vmem(),
        compiler_params=grant(8),
        name="join",
    )(snap, near, near_back)
    partner_blocks = lax.ppermute(joined, "row", partner)

    velocity, stress, _, restart = pl.pallas_call(
        stencil_kernel,
        out_shape=(
            shape(2, ROWS, LANES),
            shape(3, ROWS, LANES),
            shape(HELD, 2, TALL, LANES),
            shape(1, 10, 8 * ROWS, LANES),
        ),
        in_specs=[vmem()] * 3 + [hbm()] * 3 + [vmem(), hbm()],
        out_specs=(vmem(), vmem(), vmem(), hbm()),
        input_output_aliases={0: 2},
        scratch_shapes=[pltpu.SemaphoreType.DMA((8,))],
        compiler_params=grant(16),
        cost_estimate=pl.CostEstimate(flops=40000000, bytes_accessed=2000000, transcendentals=0),
        name="stencil",
    )(state, from_outer, from_inner, snap, near, near_back, flag, blank)
    partner_far = lax.ppermute(far, "row", partner)

    restart, velocity, stress = pl.pallas_call(
        late_kernel,
        out_shape=(
            shape(1, 10, 8 * ROWS, LANES),
            shape(2, ROWS, LANES),
            shape(3, ROWS, LANES),
        ),
        in_specs=[hbm(), vmem()] + [hbm()] * 4,
        out_specs=(hbm(), hbm(), hbm()),
        input_output_aliases={0: 0},
        scratch_shapes=[pltpu.SemaphoreType.DMA((6,))],
        compiler_params=grant(4),
        cost_estimate=pl.CostEstimate(flops=1000000, bytes_accessed=1000000, transcendentals=0),
        name="late",
    )(restart, flag, velocity, stress, far, partner_blocks)
    restart = pl.pallas_call(
        last_kernel,
        out_shape=shape(1, 10, 8 * ROWS, LANES),
        in_specs=[hbm(), vmem(), hbm()],
        out_specs=hbm(),
        input_output_aliases={0: 0},
        scratch_shapes=[pltpu.SemaphoreType.DMA],
        compiler_params=grant(4),
        name="last",
    )(restart, flag, partner_far)
    return (velocity, stress, restart)


def solution(mesh):
    return jax.shard_map(
        step,
        mesh=mesh,
        in_specs=(
            P(None, "row", "col"),
            P(None, "row", "col"),
            P(None, "row", "col"),
            P(None, "row", "col"),
            P(None, "row", "col"),
            P(None, "row", "col"),
            P("row", "col"),
            P("row", "col"),
            P("row", "col"),
            P("row", "col"),
            P(),
        ),
        out_specs=(P(None, "row", "col"), P(None, "row", "col"), P("row", None, None, "col")),
        check_vma=False,
    )
```
